32 devices in a mesh: dp: 16 (over z, y, x), group: 2 (over core).
Axes of the slice: x: 2, y: 2, z: 4, core: 2. Of those that a mesh axis runs over, the one named last changes fastest.
Arguments:
- tokens: bfloat16 [25088, 512], P(('dp', 'group')), may hold values from -6 to 6
- cotangent: bfloat16 [25088, 512], P(('dp', 'group')), may hold values from -6 to 6
- counts: int32 [32], P(('dp', 'group')), may hold values from 2 to 16, as said below
- regions: int32 [25088], P(('dp', 'group')), may hold values from 0 to 8, as said below
- square_weights: float32 [4, 512, 512], P('group'), may hold values from -0.70710678 to 0.70710678
- wide_weights: float32 [2, 512, 2048], P('group'), may hold values from -0.25 to 0.25
- vectors: float32 [12, 512], replicated, may hold values from -1.2 to 1.4
- bias_table: float32 [169, 16], replicated, may hold values from -4 to 400
- square_moment: float32 [4, 512, 512], P('group'), may hold values from -64 to 64
- wide_moment: float32 [2, 512, 2048], P('group'), may hold values from -64 to 64
- vector_moment: float32 [12, 512], replicated, may hold values from -64 to 64
- table_moment: float32 [169, 16], replicated, may hold values from -7 to 7
Outputs:
- block_out: bfloat16 [25088, 512], P(('dp', 'group'))
- grad_tokens: bfloat16 [25088, 512], P(('dp', 'group'))
- grad_square: float32 [4, 512, 512], P('group')
- grad_wide: float32 [2, 512, 2048], P('group')
- grad_vectors: float32 [12, 512], replicated
- grad_table: float32 [169, 16], replicated
- new_square: float32 [4, 512, 512], P('group')
- new_wide: float32 [2, 512, 2048], P('group')
- new_vectors: float32 [12, 512], replicated
- new_table: float32 [169, 16], replicated
- new_square_moment: float32 [4, 512, 512], P('group')
- new_wide_moment: float32 [2, 512, 2048], P('group')
- new_vector_moment: float32 [12, 512], replicated
- new_table_moment: float32 [169, 16], replicated
The draws below stay inside these ranges and needn't reach their ends.
Inputs may be any that keep to these rules, and one draw needn't show every extreme that they name: Entries 2 k and 2 k + 1 belong to the two devices of one group; their counts add to at most 20. Some device holds 16 windows beside a partner with 4. `regions`: each window's ids are one of the four layouts that a cyclic shift by 3 leaves in a 2 x 2 block of windows: all 0; 1 in local columns below 4 and 2 beyond; 3 in local rows below 4 and 6 beyond; 4, 5, 7, 8 by both.
All inputs are finite; a program needn't handle non-finite values.
Results may differ from the reference program's by a relative error of at most 0.012.
Values may be sent and summed in bfloat16 or wider, within the bound.
A program may use at most 128 MiB of HBM per device.

```python
import jax
import jax.numpy as jnp
from jax import lax

D = 512
HEADS = 16
HEAD_DIM = 32
FF = 2048
WIN = 7
SHIFT = 3
WIN_DEV = 16
TOKW = 49
TABLE_ROWS = 169
VEC_ROWS = 12
PAIR_MOST = 20
SLOTS = 512
ROWS = 25088


def draw_counts(key, part):
    pair_count = SLOTS // WIN_DEV // 2
    streams = jax.random.split(key, 4)
    first_count = jax.random.randint(streams[0], (pair_count,), 2, WIN_DEV + 1)
    headroom = jnp.minimum(WIN_DEV, PAIR_MOST - first_count)
    spread_bits = jax.random.randint(streams[1], (pair_count,), 0, 1 << 20)
    second_count = 2 + spread_bits % (headroom - 1)
    forced = jax.random.randint(streams[2], (), 0, pair_count)
    chosen = jnp.arange(pair_count) == forced
    first_count = jnp.where(chosen, WIN_DEV, first_count)
    second_count = jnp.where(chosen, PAIR_MOST - WIN_DEV, second_count)
    flipped = jax.random.randint(streams[3], (pair_count,), 0, 2) == 1
    core_zero = jnp.where(flipped, second_count, first_count)
    core_one = jnp.where(flipped, first_count, second_count)
    return jnp.stack([core_zero, core_one], axis=1).reshape(-1).astype(jnp.int32)


def draw_regions(key, part):
    layout_ids = jax.random.randint(key, (SLOTS,), 0, 4)
    places = jnp.arange(TOKW)
    lower_rows = (places // WIN >= WIN - SHIFT).astype(jnp.int32)
    right_cols = (places % WIN >= WIN - SHIFT).astype(jnp.int32)
    layouts = jnp.stack([0 * places, 1 + right_cols, 3 + 3 * lower_rows, 4 + 3 * lower_rows + right_cols])
    return layouts[layout_ids].reshape(-1).astype(jnp.int32)


def draw_square_weights(key, part):
    base_draw = jnp.clip(jax.random.normal(key, (4, D, D), jnp.float32), -4.0, 4.0)
    scales = jnp.where(jnp.arange(4) == 3, (D // HEADS) ** (-0.5), D ** (-0.5))
    return (base_draw * scales[:, None, None]).astype(jnp.float32)


def draw_vectors(key, part):
    base_draw = jnp.clip(jax.random.normal(key, (VEC_ROWS, D), jnp.float32), -4.0, 4.0)
    row_ids = jnp.arange(VEC_ROWS)[:, None]
    return jnp.where(row_ids < 2, 1.0 + 0.1 * base_draw, 0.3 * base_draw).astype(jnp.float32)


def draw_bias_table(key, part):
    streams = jax.random.split(key, 1)
    return jnp.clip(jax.random.normal(streams[0], (TABLE_ROWS, HEADS), jnp.float32), -4.0, 4.0)


def block_levels(stream_key, dims, shards, smallest, top_value):
    def one(dim, parts):
        steps = jax.random.uniform(jax.random.fold_in(jax.random.fold_in(stream_key, 6), dim), (parts,), jnp.float32, smallest / len(shards), top_value / len(shards))
        return jnp.repeat(jnp.exp(steps), dims[dim] // parts).reshape((-1,) + (1,) * (len(dims) - dim - 1))

    loudness = one(*shards[0])
    for cut in shards[1:]:
        loudness = loudness * one(*cut)
    return loudness


def gaussian(stream_key, dims, scale, limit, shards=(), held_as=jnp.bfloat16):
    array = jax.random.normal(stream_key, dims, jnp.float32) * scale
    if len(shards) > 0:
        array = block_levels(stream_key, dims, shards, -0.22, 0.18) * array
    return jnp.clip(array, min=-limit, max=limit).astype(held_as)


def setup_inputs(seed: int = 0) -> dict:
    splits = jax.random.split(jax.random.key(seed), 13)
    tokens = gaussian(splits[0], (ROWS, D), 1.0, 6.0, ((0, 32),))
    cotangent = gaussian(splits[1], (ROWS, D), 1.0, 6.0, ((0, 32),))
    counts = draw_counts(jax.random.fold_in(splits[12], 71), 0)
    regions = draw_regions(jax.random.fold_in(splits[12], 71), 0)
    square_weights = draw_square_weights(jax.random.fold_in(splits[12], 71), 0)
    wide_weights = gaussian(splits[5], (2, D, FF), D ** -0.5, 0.25, ((0, 2),), jnp.float32)
    vectors = draw_vectors(jax.random.fold_in(splits[12], 71), 0)
    bias_table = draw_bias_table(jax.random.fold_in(splits[12], 71), 0)
    square_moment = gaussian(splits[8], (4, D, D), (0.5 * SLOTS ** 0.5), 64.0, ((0, 2),), jnp.float32)
    wide_moment = gaussian(splits[9], (2, D, FF), (0.5 * SLOTS ** 0.5), 64.0, ((0, 2),), jnp.float32)
    vector_moment = gaussian(splits[10], (VEC_ROWS, D), (0.5 * SLOTS ** 0.5), 64.0, (), jnp.float32)
    table_moment = gaussian(splits[11], (TABLE_ROWS, HEADS), (0.05 * SLOTS ** 0.5), 7.0, (), jnp.float32)
    return {"tokens": tokens, "cotangent": cotangent, "counts": counts, "regions": regions, "square_weights": square_weights, "wide_weights": wide_weights, "vectors": vectors, "bias_table": bias_table, "square_moment": square_moment, "wide_moment": wide_moment, "vector_moment": vector_moment, "table_moment": table_moment}


@jax.custom_vjp
def low(v):
    return lax.optimization_barrier(v.astype(jnp.bfloat16)).astype(jnp.float32)

@jax.custom_vjp
def low_back(v):
    return v

def low_keep(v):
    return (low(v), None)

def low_pass(kept, grad):
    return (grad,)

def back_keep(v):
    return (v, None)

def back_low(kept, grad):
    return (low(grad),)
low.defvjp(low_keep, low_pass)
low_back.defvjp(back_keep, back_low)
HIGHEST = lax.Precision.HIGHEST
MOMENTUM = 0.9
MATRIX_RATE = 0.4
VECTOR_RATE = 0.05
TABLE_RATE = 1.0
NEWTON_ONE = 3.4445
NEWTON_TWO = -4.775
NEWTON_THREE = 2.0315

def relative_index():
    places = jnp.arange(TOKW)
    rowpos = places // WIN
    colpos = places % WIN
    offsets = (rowpos[:, None] - rowpos[None, :] + WIN - 1) * (2 * WIN - 1) + colpos[:, None] - colpos[None, :] + WIN - 1
    return offsets.astype(jnp.int32)

def layer_norm(values, norm_gain, norm_shift):
    center = values - lax.optimization_barrier(jnp.mean(values, axis=-1, keepdims=True))
    spread = lax.optimization_barrier(jnp.mean(center * center, axis=-1, keepdims=True))
    return center * lax.rsqrt(spread + 1e-05) * norm_gain + norm_shift

def window_block(weights, vector_rows, bias_heads, inputs, region_ids):
    w_query, w_key, w_value, w_proj, w_first, w_second = weights
    window_count = inputs.shape[0]

    def split_heads(matrix):
        return matrix.reshape(window_count, TOKW, HEADS, HEAD_DIM)
    normed = low(layer_norm(inputs, vector_rows[0], vector_rows[2]))
    queries = low(low_back(jnp.einsum('btd,de->bte', normed, w_query, precision=HIGHEST) + vector_rows[4]))
    key_rows = low(low_back(jnp.einsum('btd,de->bte', normed, w_key, precision=HIGHEST)))
    value_rows = low(low_back(jnp.einsum('btd,de->bte', normed, w_value, precision=HIGHEST) + vector_rows[5]))
    scores = jnp.einsum('bihc,bjhc->bhij', split_heads(queries), split_heads(key_rows), precision=HIGHEST) * HEAD_DIM ** (-0.5) + bias_heads[None]
    scores = low_back(scores)
    allowed = (region_ids[:, :, None] == region_ids[:, None, :])[:, None]
    masked = jnp.where(allowed, scores, -1e+30)
    row_max = lax.optimization_barrier(jnp.max(masked, axis=-1, keepdims=True))
    exponent = jnp.exp(masked - row_max)
    prob_rows = low(exponent / lax.optimization_barrier(jnp.sum(exponent, axis=-1, keepdims=True)))
    mixed_heads = jnp.einsum('bhij,bjhc->bihc', prob_rows, split_heads(value_rows), precision=HIGHEST).reshape(window_count, TOKW, D)
    mixed_heads = low(low_back(mixed_heads))
    branch = low_back(jnp.einsum('btd,de->bte', mixed_heads, w_proj, precision=HIGHEST) + vector_rows[6])
    middle = inputs + branch
    normed_two = low(layer_norm(middle, vector_rows[1], vector_rows[3]))
    hidden = low_back(jnp.einsum('btd,df->btf', normed_two, w_first, precision=HIGHEST) + vector_rows[8:].reshape(FF))
    active = low(jax.nn.gelu(hidden, approximate=False))
    result = low_back(jnp.einsum('btf,df->btd', active, w_second, precision=HIGHEST) + vector_rows[7])
    return middle + result

def orthogonalize(matrix):
    current = (matrix / (jnp.sqrt(jnp.sum(matrix * matrix)) + 1e-07)).astype(jnp.bfloat16)
    for iteration in range(5):
        gram_matrix = jnp.dot(current, current.T, preferred_element_type=jnp.float32).astype(jnp.bfloat16)
        gram_square = jnp.dot(gram_matrix, gram_matrix, preferred_element_type=jnp.float32)
        mixing = (NEWTON_TWO * gram_matrix.astype(jnp.float32) + NEWTON_THREE * gram_square).astype(jnp.bfloat16)
        current = (NEWTON_ONE * current.astype(jnp.float32) + jnp.dot(mixing, current, preferred_element_type=jnp.float32)).astype(jnp.bfloat16)
    return current.astype(jnp.float32)

def reference(tokens, cotangent, counts, regions, square_weights, wide_weights, vectors, bias_table, square_moment, wide_moment, vector_moment, table_moment):
    slot_ids = jnp.arange(SLOTS)
    live_slots = (slot_ids % WIN_DEV < counts[slot_ids // WIN_DEV]).astype(jnp.float32)[:, None, None]
    inputs = tokens.astype(jnp.float32).reshape(SLOTS, TOKW, D)
    region_ids = regions.reshape(SLOTS, TOKW)
    blocks = SLOTS // (8 * WIN_DEV)
    positions = relative_index()

    def forward_pass(block_inputs, square_stack, wide_stack, vector_rows, table_rows):
        weights = (low(square_stack[0]), low(square_stack[1]), low(square_stack[2]), low(square_stack[3]), low(wide_stack[0]), low(wide_stack[1]))
        bias_heads = jnp.transpose(table_rows[positions], (2, 0, 1))

        def one_block(block_pair):
            return window_block(weights, vector_rows, bias_heads, block_pair[0], block_pair[1])
        outputs = lax.map(jax.checkpoint(one_block), (block_inputs.reshape(blocks, 8 * WIN_DEV, TOKW, D), region_ids.reshape(blocks, 8 * WIN_DEV, TOKW)))
        return outputs.reshape(SLOTS, TOKW, D)
    result, pullback = jax.vjp(forward_pass, inputs, square_weights, wide_weights, vectors, bias_table)
    seed_grad = cotangent.astype(jnp.float32).reshape(SLOTS, TOKW, D) * live_slots
    grad_inputs, grad_square, grad_wide, grad_vectors, grad_table = pullback(seed_grad)
    block_out = (result * live_slots).astype(jnp.bfloat16).reshape(ROWS, D)
    grad_tokens = grad_inputs.astype(jnp.bfloat16).reshape(ROWS, D)
    new_square_moment = MOMENTUM * square_moment + grad_square
    new_wide_moment = MOMENTUM * wide_moment + grad_wide
    new_square = jnp.stack([square_weights[matrix_index] - MATRIX_RATE * orthogonalize(new_square_moment[matrix_index]) for matrix_index in range(4)])
    new_wide = jnp.stack([wide_weights[matrix_index] - MATRIX_RATE * orthogonalize(new_wide_moment[matrix_index]) for matrix_index in range(2)])
    slot_root = jnp.sqrt(jnp.float32(SLOTS))
    new_vector_moment = MOMENTUM * vector_moment + grad_vectors
    new_vectors = vectors - VECTOR_RATE / slot_root * new_vector_moment
    new_table_moment = MOMENTUM * table_moment + grad_table
    new_table = bias_table - TABLE_RATE / slot_root * new_table_moment
    return (block_out, grad_tokens, grad_square, grad_wide, grad_vectors, grad_table, new_square, new_wide, new_vectors, new_table, new_square_moment, new_wide_moment, new_vector_moment, new_table_moment)
```

```python
import functools
import math

import jax
import jax.numpy as jnp
from jax import lax
from jax.experimental import pallas as pl
from jax.experimental.pallas import tpu as pltpu
from jax.sharding import PartitionSpec as P

D = 512
HEADS = 16
HEAD_DIM = 32
WIN = 7
WIN_DEV = 16
TOKW = 49
TABLE_ROWS = 169


HIGHEST = lax.Precision.HIGHEST
MOMENTUM = 0.9
MATRIX_RATE = 0.4
VECTOR_RATE = 0.05
TABLE_RATE = 1.0
NEWTON_ONE = 3.4445
NEWTON_TWO = -4.775
NEWTON_THREE = 2.0315
MASKED = -1e30
EPSILON = 1e-05


def norm_forward(values, norm_gain, norm_shift):
    center = values - jnp.mean(values, axis=-1, keepdims=True)
    spread = jnp.mean(center * center, axis=-1, keepdims=True)
    inverse = lax.rsqrt(spread + EPSILON)
    normed = center * inverse
    return (normed * norm_gain + norm_shift, normed, inverse)


def norm_backward(grad_out, normed, inverse, norm_gain):
    grad_normed = grad_out * norm_gain
    inner_mean = jnp.mean(grad_normed, axis=-1, keepdims=True)
    cross_mean = jnp.mean(grad_normed * normed, axis=-1, keepdims=True)
    grad_in = inverse * (grad_normed - inner_mean - normed * cross_mean)
    return (grad_in, jnp.sum(grad_out * normed, axis=0), jnp.sum(grad_out, axis=0))


def relative_onehot():
    places = jnp.arange(TOKW)
    rowpos = places // WIN
    colpos = places % WIN
    offsets = (
        (rowpos[:, None] - rowpos[None, :] + WIN - 1) * (2 * WIN - 1)
        + colpos[:, None]
        - colpos[None, :]
        + WIN
        - 1
    )
    return (offsets.reshape(-1)[:, None] == jnp.arange(TABLE_ROWS)[None, :]).astype(jnp.float32)


def head_scores(query_rows, key_rows, bias_heads, allowed):
    scores = jnp.einsum("sihc,sjhc->shij", query_rows, key_rows, preferred_element_type=jnp.float32)
    scores = scores * HEAD_DIM ** (-0.5) + bias_heads[None]
    return jnp.where(allowed, scores, MASKED)


MESH = pl.DeviceIdType.MESH
BLK = 512
HALF = 6
ORDER = (2, 3, 4, 5, 0, 1)
SMALL = 40


def chip_grid(dp):
    side = max(1, math.isqrt(dp // 4))
    if side * side * 4 == dp:
        return (side, side, 4)
    return (1, 1, dp)


class Lane:
    def __init__(self, size, pos, stride, dp, group):
        self.n, self.i, self.stride, self.dp, self.group = size, pos, stride, dp, group

    def peer(self, delta):
        return (self.dp + delta * self.stride, self.group)


class Ids:
    def __init__(self):
        self.count = 0

    def take(self, number=1):
        first = self.count
        self.count += number
        return first


def lanes(sizes):
    dp, group = lax.axis_index("dp"), lax.axis_index("group")
    nx, ny, nz = sizes
    x, y, z = lax.rem(dp, nx), lax.rem(lax.div(dp, nx), ny), lax.div(dp, nx * ny)
    return (
        Lane(nx, x, 1, dp, group),
        Lane(ny, y, nx, dp, group),
        Lane(nz, z, nx * ny, dp, group),
    )


class Plan:
    def __init__(self, sizes, pieces):
        nx, ny, nz = sizes
        self.orders = ((0, 2, 1), (1, 2, 0))
        self.rs, self.ag = Ids(), Ids()
        self.rows = 0
        self.slots = {}
        half = BLK // 2
        for piece in range(pieces):
            color = piece % 2
            rows = half
            for stage, dim in enumerate(self.orders[color]):
                n = sizes[dim]
                if stage < 2:
                    rows = rows // n
                land = {}
                for way in ("R", "L"):
                    for j in range(n):
                        if (way == "R" and j > 0) or (way == "L" and j < n - 1):
                            land[way, j] = (self.rs.take(), self.rows)
                            self.rows += rows
                ag_recv = self.ag.take(n)
                self.slots[piece, stage] = (land, ag_recv)


def make_comm(sizes):
    pieces = 2 * HALF
    plan = Plan(sizes, pieces)

    def tasks_for(piece, env):
        (lane_all, own_ref, core_land, acc, out_ref, land_ref, rs_send, rs_recv, ag_sl, ag_sr, ag_recv,
         core_send_sem, core_recv_sem, partner, ends, grads_ref) = env
        color = piece % 2
        block = ORDER[piece // 2]
        base = color * (BLK // 2)
        half = BLK // 2
        order = plan.orders[color]
        dims = [lane_all[d] for d in order]
        tasks = []

        def add_into(dst, dst_rows, dst_cols, src_row, rows, cols_w, col0=0):
            step = min(rows, 32)

            def body(k, carry):
                r = pl.multiple_of(dst_rows + k * step, 16)
                s = pl.multiple_of(src_row + k * step, 16)
                here = acc[block, pl.ds(r, step), dst_cols].astype(jnp.float32)
                there = land_ref[pl.ds(s, step), pl.ds(0, cols_w)].astype(jnp.float32)
                dst[block, pl.ds(r, step), dst_cols] = (here + there).astype(jnp.bfloat16)
                return carry

            if rows == step:
                body(0, 0)
            else:
                lax.fori_loop(0, rows // step, body, 0)

        all_cols = pl.ds(0, BLK)

        r_sizes = [half // dims[0].n, half // dims[0].n // dims[1].n]
        off0 = base
        off1 = off0 + dims[0].i * r_sizes[0]
        off2 = off1 + dims[1].i * r_sizes[1]
        cols = BLK // dims[2].n

        def view(stage, j):
            if stage == 0:
                return pl.multiple_of(off0 + j * r_sizes[0], 16), r_sizes[0], pl.ds(0, BLK), BLK
            if stage == 1:
                return pl.multiple_of(off1 + j * r_sizes[1], 16), r_sizes[1], pl.ds(0, BLK), BLK
            start = j * cols if isinstance(j, int) else pl.multiple_of(j * cols, 128)
            return pl.multiple_of(off2, 16), r_sizes[1], pl.ds(start, cols), cols

        def rs_copy(stage, way, j):
            land, _ = plan.slots[piece, stage]
            sem, row = land[way, j]
            lane = dims[stage]
            r, rows, cs, width = view(stage, j)
            return pltpu.make_async_remote_copy(
                src_ref=acc.at[block, pl.ds(r, rows), cs],
                dst_ref=land_ref.at[pl.ds(row, rows), pl.ds(0, width)],
                send_sem=rs_send.at[sem],
                recv_sem=rs_recv.at[sem],
                device_id=lane.peer(1 if way == "R" else -1),
                device_id_type=MESH,
            )

        def rs_tick(stage, h):
            lane = dims[stage]
            n = lane.n
            land, _ = plan.slots[piece, stage]
            last = stage == 2

            @pl.when(lane.i == h)
            def _():
                for j in range(n - 1, h - 1, -1):
                    if h > 0:
                        rs_copy(stage, "R", j).wait_recv()
                        r, rows, cs, width = view(stage, j)
                        add_into(acc, r, cs, land["R", j][1], rows, width)
                    if j > h:
                        rs_copy(stage, "R", j).start()

            @pl.when(lane.i == n - 1 - h)
            def _():
                for j in range(0, n - h):
                    if h > 0:
                        rs_copy(stage, "L", j).wait_recv()
                        r, rows, cs, width = view(stage, j)
                        add_into(acc, r, cs, land["L", j][1], rows, width)
                    if j < n - 1 - h:
                        rs_copy(stage, "L", j).start()

        def rs_end(stage):
            lane = dims[stage]
            n = lane.n
            for j in range(n):
                if j > 0:
                    @pl.when(lane.i < j)
                    def _():
                        rs_copy(stage, "R", j).wait_send()
                if j < n - 1:
                    @pl.when(lane.i > j)
                    def _():
                        rs_copy(stage, "L", j).wait_send()

        def ag_copy(stage, j, way):
            _, first = plan.slots[piece, stage]
            lane = dims[stage]
            r, rows, cs, width = view(stage, j)
            piece_ref = out_ref.at[block, pl.ds(r, rows), cs]
            return pltpu.make_async_remote_copy(
                src_ref=piece_ref,
                dst_ref=piece_ref,
                send_sem=(ag_sr if way > 0 else ag_sl).at[first + j],
                recv_sem=ag_recv.at[first + j],
                device_id=lane.peer(way),
                device_id_type=MESH,
            )

        def ag_tick(stage, h):
            lane = dims[stage]
            n, i = lane.n, lane.i
            if h == 0:
                @pl.when(i < n - 1)
                def _():
                    ag_copy(stage, i, 1).start()

                @pl.when(i > 0)
                def _():
                    ag_copy(stage, i, -1).start()
                return

            @pl.when(i >= h)
            def _():
                ag_copy(stage, i - h, -1).wait_recv()

                @pl.when(i < n - 1)
                def _():
                    ag_copy(stage, i - h, 1).start()

            @pl.when(i + h <= n - 1)
            def _():
                ag_copy(stage, i + h, 1).wait_recv()

                @pl.when(i > 0)
                def _():
                    ag_copy(stage, i + h, -1).start()

        def ag_end(stage):
            lane = dims[stage]
            n, i = lane.n, lane.i
            for h in range(n):
                @pl.when((i >= h) & (i < n - 1))
                def _():
                    ag_copy(stage, i - h, 1).wait_send()

                @pl.when((i + h <= n - 1) & (i > 0))
                def _():
                    ag_copy(stage, i + h, -1).wait_send()

        def core_copy():
            return pltpu.make_async_remote_copy(
                src_ref=grads_ref.at[1 - partner[2], block, pl.ds(base, half)],
                dst_ref=core_land.at[block, pl.ds(base, half)],
                send_sem=core_send_sem.at[piece],
                recv_sem=core_recv_sem.at[piece],
                device_id=partner[:2],
                device_id_type=MESH,
            )

        def first():
            core_copy().wait_recv()

            def body(k, carry):
                r = pl.multiple_of(base + k * 32, 16)
                here = grads_ref[partner[2], block, pl.ds(r, 32)].astype(jnp.float32)
                there = core_land[block, pl.ds(r, 32)].astype(jnp.float32)
                acc[block, pl.ds(r, 32)] = (here + there).astype(jnp.bfloat16)
                return carry

            lax.fori_loop(0, half // 32, body, 0)

        def copy_out():
            r, rows, cs, width = view(2, dims[2].i)
            out_ref[block, pl.ds(r, rows), cs] = acc[block, pl.ds(r, rows), cs]

        flat = [first]
        groups = []
        for stage in range(3):
            for h in range(dims[stage].n):
                groups.append((h == 0, functools.partial(rs_tick, stage, h)))
        groups.append((False, copy_out))
        for stage in (2, 1, 0):
            for h in range(dims[stage].n):
                groups.append((h == 0, functools.partial(ag_tick, stage, h)))
        ticks = [[first]]
        for joined, task in groups:
            if joined or task is copy_out:
                ticks[-1].append(task)
            else:
                ticks.append([task])
        for stage in range(3):
            ends.append(functools.partial(rs_end, stage))
            ends.append(functools.partial(ag_end, stage))
        ends.append(lambda: core_copy().wait_send())
        return core_copy, ticks

    def kernel(grads_ref, small_ref, out_ref, small_out, core_land, acc, land_ref, small_core, small_land,
               rs_send, rs_recv, ag_sl, ag_sr, ag_recv, core_s, core_r, sm_cs, sm_cr, sm_s, sm_r, *, delta):
        lane_all = lanes(sizes)
        dp, group = lax.axis_index("dp"), lax.axis_index("group")
        partner = (dp, 1 - group, group)

        barrier = pltpu.get_barrier_semaphore()
        total = 1
        pl.semaphore_signal(barrier, inc=1, device_id=partner[:2], device_id_type=MESH)
        for lane in lane_all:
            for k in range(1, lane.n):
                to = lax.rem(lane.i + k, lane.n)
                pl.semaphore_signal(barrier, inc=1, device_id=lane.peer(to - lane.i), device_id_type=MESH)
                total += 1
        pl.semaphore_wait(barrier, total)

        ends = []
        env = (lane_all, None, core_land, acc, out_ref, land_ref, rs_send, rs_recv, ag_sl, ag_sr, ag_recv,
               core_s, core_r, partner, ends, grads_ref)

        def sm_core():
            return pltpu.make_async_remote_copy(
                src_ref=small_ref.at[1 - group], dst_ref=small_core, send_sem=sm_cs.at[0], recv_sem=sm_cr.at[0],
                device_id=partner[:2], device_id_type=MESH)

        def sm_back():
            return pltpu.make_async_remote_copy(
                src_ref=small_out.at[group], dst_ref=small_out.at[group], send_sem=sm_cs.at[1], recv_sem=sm_cr.at[1],
                device_id=partner[:2], device_id_type=MESH)

        first_slot = [0, sizes[0], sizes[0] + sizes[1]]

        def sm_copy(d, k):
            lane = lane_all[d]
            to = lax.rem(lane.i + k, lane.n)
            return pltpu.make_async_remote_copy(
                src_ref=small_land.at[first_slot[d] + lane.i],
                dst_ref=small_land.at[first_slot[d] + lane.i],
                send_sem=sm_s.at[first_slot[d] + k],
                recv_sem=sm_r.at[first_slot[d] + lane.i],
                device_id=lane.peer(to - lane.i), device_id_type=MESH)

        def sm_wait(d, k):
            lane = lane_all[d]
            source = lax.rem(lane.i + k, lane.n)
            pltpu.make_async_remote_copy(
                src_ref=small_land.at[first_slot[d] + source],
                dst_ref=small_land.at[first_slot[d] + source],
                send_sem=sm_s.at[first_slot[d] + k],
                recv_sem=sm_r.at[first_slot[d] + source],
                device_id=lane.peer(source - lane.i), device_id_type=MESH).wait_recv()

        def sm_start(d, value):
            lane = lane_all[d]
            small_land[first_slot[d] + lane.i] = value
            for k in range(1, lane.n):
                sm_copy(d, k).start()

        def sm_finish(d):
            lane = lane_all[d]
            for k in range(1, lane.n):
                sm_wait(d, k)
            value = small_land[first_slot[d]]
            for j in range(1, lane.n):
                value = value + small_land[first_slot[d] + j]
            return value

        def sm0():
            sm_core().wait_recv()
            sm_start(0, small_ref[group] + small_core[...])

        def sm1():
            sm_start(1, sm_finish(0))

        def sm2():
            sm_start(2, sm_finish(1))

        def sm3():
            small_out[group] = sm_finish(2)
            sm_back().start()

        def sm4():
            sm_back().wait_recv()

        sm_core().start()
        made = [tasks_for(p, env) for p in range(pieces)]
        for core_copy, _ in made:
            core_copy().start()
        table = {}
        length = max(len(t) for _, t in made)
        for p, (_, ticks) in enumerate(made):
            for k, tick in enumerate(ticks):
                table.setdefault(int(delta * (p // 2)) + k, []).append((p, tick))
        for k, task in enumerate((sm0, sm1, sm2, sm3, sm4)):
            table.setdefault(1 + 2 * k, []).append((-1, [task]))
        for when in sorted(table):
            for p, tick in sorted(table[when], key=lambda e: e[0]):
                for task in tick:
                    task()
        for task in ends:
            task()
        sm_core().wait_send()
        sm_back().wait_send()
        for d in range(3):
            for k in range(1, sizes[d]):
                sm_copy(d, k).wait_send()

    def call(grads, small, delta=1.0):
        dma = pltpu.SemaphoreType.DMA
        vmem = pl.BlockSpec(memory_space=pltpu.VMEM)
        return pl.pallas_call(
            functools.partial(kernel, delta=delta),
            out_shape=(
                jax.ShapeDtypeStruct((HALF, BLK, BLK), jnp.bfloat16),
                jax.ShapeDtypeStruct((2, SMALL, 128), jnp.float32),
            ),
            in_specs=[vmem, vmem],
            out_specs=[vmem, vmem],
            scratch_shapes=[
                pltpu.VMEM((HALF, BLK, BLK), jnp.bfloat16),
                pltpu.VMEM((HALF, BLK, BLK), jnp.bfloat16),
                pltpu.VMEM((plan.rows, BLK), jnp.bfloat16),
                pltpu.VMEM((SMALL, 128), jnp.float32),
                pltpu.VMEM((sum(sizes), SMALL, 128), jnp.float32),
                dma((plan.rs.count,)),
                dma((plan.rs.count,)),
                dma((plan.ag.count,)),
                dma((plan.ag.count,)),
                dma((plan.ag.count,)),
                dma((pieces,)),
                dma((pieces,)),
                dma((2,)),
                dma((2,)),
                dma((sum(sizes),)),
                dma((sum(sizes),)),
            ],
            compiler_params=pltpu.CompilerParams(
                collective_id=1, has_side_effects=True, vmem_limit_bytes=56 * 2**20
            ),
            name="reduce_gradients",
        )(grads, small)

    return call


STEP = 32


def muon_kernel(g_hbm, sw_hbm, ww_hbm, sm_hbm, wm_hbm,
                gs_out, gw_out, ns_out, nw_out, nsm_out, nwm_out,
                g, sw, ww, sm, wm, gs, gw, xs, xw, gram, mix, sem_in, sem_out):
    ff = ww.shape[2]
    cols = ff // D

    def load(src, dst, k):
        return pltpu.make_async_copy(src, dst, sem_in.at[k])

    loads = [load(g_hbm.at[pl.ds(0, 2)], g.at[pl.ds(0, 2)], 0), load(sm_hbm, sm, 1),
             load(g_hbm.at[pl.ds(2, cols)], g.at[pl.ds(2, cols)], 2), load(wm_hbm, wm, 3),
             load(sw_hbm, sw, 4), load(ww_hbm, ww, 5)]
    for c in loads:
        c.start()
    stores = [pltpu.make_async_copy(a, b, sem_out.at[k]) for k, (a, b) in enumerate(
        ((gs, gs_out), (sm, nsm_out), (gw, gw_out), (wm, nwm_out), (sw, ns_out), (ww, nw_out)))]

    def scan(moment, grad, pick):
        def body(k, total):
            r = pl.multiple_of(k * STEP, STEP)
            new = None
            part = jnp.zeros((STEP, D), jnp.float32)
            for c, block in enumerate(pick):
                cs = pl.ds(c * D, D)
                add = g[block, pl.ds(r, STEP)].astype(jnp.float32)
                grad[pl.ds(r, STEP), cs] = add
                new = MOMENTUM * moment[pl.ds(r, STEP), cs] + add
                moment[pl.ds(r, STEP), cs] = new
                part = part + new * new
            return total + part
        total = lax.fori_loop(0, D // STEP, body, jnp.zeros((STEP, D), jnp.float32))
        return jnp.sum(total)

    def scale(moment, x, total, width):
        size = jnp.sqrt(jnp.full((1, D), total, jnp.float32)) + 1e-07

        def body(k, carry):
            r = pl.multiple_of(k * STEP, STEP)
            for c in range(width // D):
                cs = pl.ds(c * D, D)
                x[pl.ds(r, STEP), cs] = (moment[pl.ds(r, STEP), cs] / size).astype(jnp.bfloat16)
            return carry
        lax.fori_loop(0, D // STEP, body, 0)

    dot_t = functools.partial(lax.dot_general, dimension_numbers=(((1,), (1,)), ((), ())),
                              preferred_element_type=jnp.float32)

    def newton(many, width):
        def body(k, carry):
            for m in range(len(many)):
                x = many[m]
                gram[m] = dot_t(x[...], x[...]).astype(jnp.bfloat16)
            for m in range(len(many)):
                a = gram[m]
                square = jnp.dot(a, a, preferred_element_type=jnp.float32)
                mix[m] = (NEWTON_TWO * a.astype(jnp.float32) + NEWTON_THREE * square).astype(jnp.bfloat16)
            for m in range(len(many)):
                x = many[m]
                for c in range(width // D):
                    cs = pl.ds(c * D, D)
                    old = x[:, cs]
                    x[:, cs] = (NEWTON_ONE * old.astype(jnp.float32)
                                + jnp.dot(mix[m], old, preferred_element_type=jnp.float32)).astype(jnp.bfloat16)
            return carry
        lax.fori_loop(0, 5, body, 0)

    def finish(weight, x, width):
        def body(k, carry):
            r = pl.multiple_of(k * STEP, STEP)
            for c in range(width // D):
                cs = pl.ds(c * D, D)
                weight[pl.ds(r, STEP), cs] = weight[pl.ds(r, STEP), cs] - MATRIX_RATE * x[pl.ds(r, STEP), cs].astype(jnp.float32)
            return carry
        lax.fori_loop(0, D // STEP, body, 0)

    loads[0].wait()
    loads[1].wait()
    for m in range(2):
        total = scan(sm.at[m], gs.at[m], (m,))
        scale(sm.at[m], xs.at[m], total, D)
    stores[0].start()
    stores[1].start()
    loads[2].wait()
    loads[3].wait()
    total = scan(wm.at[0], gw.at[0], tuple(range(2, 2 + cols)))
    scale(wm.at[0], xw, total, ff)
    stores[2].start()
    stores[3].start()
    newton([xs.at[0], xs.at[1]], D)
    loads[4].wait()
    for m in range(2):
        finish(sw.at[m], xs.at[m], D)
    stores[4].start()
    newton([xw], ff)
    loads[5].wait()
    finish(ww.at[0], xw, ff)
    stores[5].start()
    for c in stores:
        c.wait()


def muon(g, sw, ww, sm, wm):
    any_ = pl.BlockSpec(memory_space=pl.ANY)
    shapes = [sw, ww, sw, ww, sm, wm]
    f32 = jnp.float32
    return pl.pallas_call(
        muon_kernel,
        out_shape=tuple(jax.ShapeDtypeStruct(a.shape, f32) for a in shapes),
        in_specs=[any_] * 5,
        out_specs=(any_,) * 6,
        scratch_shapes=[
            pltpu.VMEM(g.shape, jnp.bfloat16),
            pltpu.VMEM(sw.shape, f32), pltpu.VMEM(ww.shape, f32),
            pltpu.VMEM(sm.shape, f32), pltpu.VMEM(wm.shape, f32),
            pltpu.VMEM(sw.shape, f32), pltpu.VMEM(ww.shape, f32),
            pltpu.VMEM((2, D, D), jnp.bfloat16), pltpu.VMEM((D, ww.shape[2]), jnp.bfloat16),
            pltpu.VMEM((2, D, D), jnp.bfloat16), pltpu.VMEM((2, D, D), jnp.bfloat16),
            pltpu.SemaphoreType.DMA((6,)), pltpu.SemaphoreType.DMA((6,)),
        ],
        compiler_params=pltpu.CompilerParams(vmem_limit_bytes=58 * 2**20),
        name="muon_step",
    )(g, sw, ww, sm, wm)

def window_pass(
    tokens, cotangent, region_ids, live_rows, full_square, full_wide, vectors, bias_heads, onehot
):
    row_count = tokens.shape[0]
    slot_count = row_count // TOKW
    contract_rows = (((0,), (0,)), ((), ()))
    contract_cols = (((1,), (1,)), ((), ()))
    inputs = tokens.astype(jnp.float32)
    seed_grad = cotangent.astype(jnp.float32) * live_rows[:, None]
    normed_one, unit_one, inverse_one = norm_forward(inputs, vectors[0], vectors[2])
    low_one = normed_one.astype(jnp.bfloat16)
    bias_qkv = jnp.stack([vectors[4], jnp.zeros_like(vectors[4]), vectors[5]])
    projected = (
        jnp.einsum("td,sde->ste", low_one, full_square[:3], preferred_element_type=jnp.float32)
        + bias_qkv[:, None, :]
    )
    low_qkv = projected.astype(jnp.bfloat16).reshape(3, slot_count, TOKW, HEADS, HEAD_DIM)
    query_rows, key_rows, value_rows = (low_qkv[0], low_qkv[1], low_qkv[2])
    windows = region_ids.reshape(slot_count, TOKW)
    allowed = (windows[:, :, None] == windows[:, None, :])[:, None]
    masked = head_scores(query_rows, key_rows, bias_heads, allowed)
    row_max = jnp.max(masked, axis=-1, keepdims=True)
    exponent = jnp.exp(masked - row_max)
    row_sum = jnp.sum(exponent, axis=-1, keepdims=True)
    log_total = row_max + jnp.log(row_sum)
    low_probs = (exponent / row_sum).astype(jnp.bfloat16)
    mixed_heads = jnp.einsum(
        "shij,sjhc->sihc", low_probs, value_rows, preferred_element_type=jnp.float32
    )
    low_mixed = mixed_heads.reshape(row_count, D).astype(jnp.bfloat16)
    middle = inputs + (
        jnp.dot(low_mixed, full_square[3], preferred_element_type=jnp.float32) + vectors[6]
    )
    normed_two, unit_two, inverse_two = norm_forward(middle, vectors[1], vectors[3])
    low_two = normed_two.astype(jnp.bfloat16)
    hidden = jnp.dot(low_two, full_wide[0], preferred_element_type=jnp.float32) + vectors[
        8:
    ].reshape(-1)
    low_active = jax.nn.gelu(hidden, approximate=False).astype(jnp.bfloat16)
    second = lax.dot_general(
        low_active, full_wide[1], contract_cols, preferred_element_type=jnp.float32
    )
    output = middle + (second + vectors[7])
    block_out = (output * live_rows[:, None]).astype(jnp.bfloat16)
    low_seed = seed_grad.astype(jnp.bfloat16)
    grad_second = lax.dot_general(
        low_seed, low_active, contract_rows, preferred_element_type=jnp.float32
    )
    grad_bias_out = jnp.sum(seed_grad, axis=0)
    grad_active = jnp.dot(low_seed, full_wide[1], preferred_element_type=jnp.float32)
    cumulative = 0.5 * (1.0 + lax.erf(hidden * 0.7071067811865476))
    density = jnp.exp(-0.5 * hidden * hidden) * 0.3989422804014327
    low_hidden_grad = (grad_active * (cumulative + hidden * density)).astype(jnp.bfloat16)
    grad_first = lax.dot_general(
        low_two, low_hidden_grad, contract_rows, preferred_element_type=jnp.float32
    )
    grad_bias_hidden = jnp.sum(low_hidden_grad, axis=0, dtype=jnp.float32)
    grad_normed_two = lax.dot_general(
        low_hidden_grad, full_wide[0], contract_cols, preferred_element_type=jnp.float32
    )
    grad_inner_two, grad_gain_two, grad_shift_two = norm_backward(
        grad_normed_two, unit_two, inverse_two, vectors[1]
    )
    grad_middle = seed_grad + grad_inner_two
    low_attn_grad = grad_middle.astype(jnp.bfloat16)
    grad_proj = lax.dot_general(
        low_mixed, low_attn_grad, contract_rows, preferred_element_type=jnp.float32
    )
    grad_bias_proj = jnp.sum(low_attn_grad, axis=0, dtype=jnp.float32)
    low_mixed_grad = (
        lax.dot_general(
            low_attn_grad, full_square[3], contract_cols, preferred_element_type=jnp.float32
        )
        .astype(jnp.bfloat16)
        .reshape(slot_count, TOKW, HEADS, HEAD_DIM)
    )
    prob_rows = jnp.exp(head_scores(query_rows, key_rows, bias_heads, allowed) - log_total)
    low_probs_back = prob_rows.astype(jnp.bfloat16)
    grad_probs = jnp.einsum(
        "sihc,sjhc->shij", low_mixed_grad, value_rows, preferred_element_type=jnp.float32
    )
    grad_values = jnp.einsum(
        "shij,sihc->sjhc", low_probs_back, low_mixed_grad, preferred_element_type=jnp.float32
    )
    inner_sum = jnp.sum(prob_rows * grad_probs, axis=-1, keepdims=True)
    low_score_grad = (prob_rows * (grad_probs - inner_sum)).astype(jnp.bfloat16)
    grad_queries = jnp.einsum(
        "shij,sjhc->sihc", low_score_grad, key_rows, preferred_element_type=jnp.float32
    ) * HEAD_DIM ** (-0.5)
    grad_keys = jnp.einsum(
        "shij,sihc->sjhc", low_score_grad, query_rows, preferred_element_type=jnp.float32
    ) * HEAD_DIM ** (-0.5)
    score_sum = jnp.sum(low_score_grad, axis=0, dtype=jnp.float32).reshape(HEADS, TOKW * TOKW)
    grad_table = lax.dot_general(onehot, score_sum, (((0,), (1,)), ((), ())), precision=HIGHEST)
    low_qkv_grad = (
        jnp.stack([grad_queries, grad_keys, grad_values])
        .astype(jnp.bfloat16)
        .reshape(3, row_count, D)
    )
    grad_qkv = jnp.einsum("td,ste->sde", low_one, low_qkv_grad, preferred_element_type=jnp.float32)
    grad_bias_query = jnp.sum(low_qkv_grad[0], axis=0, dtype=jnp.float32)
    grad_bias_value = jnp.sum(low_qkv_grad[2], axis=0, dtype=jnp.float32)
    grad_normed_one = jnp.einsum(
        "ste,sde->td", low_qkv_grad, full_square[:3], preferred_element_type=jnp.float32
    )
    grad_inner_one, grad_gain_one, grad_shift_one = norm_backward(
        grad_normed_one, unit_one, inverse_one, vectors[0]
    )
    grad_tokens = (grad_middle + grad_inner_one).astype(jnp.bfloat16)
    grad_square = jnp.concatenate([grad_qkv, grad_proj[None]], axis=0)
    grad_wide = jnp.stack([grad_first, grad_second])
    vector_head = jnp.stack(
        [
            grad_gain_one,
            grad_gain_two,
            grad_shift_one,
            grad_shift_two,
            grad_bias_query,
            grad_bias_value,
            grad_bias_proj,
            grad_bias_out,
        ]
    )
    grad_vectors = jnp.concatenate([vector_head, grad_bias_hidden.reshape(-1, D)], axis=0)
    return (block_out, grad_tokens, grad_square, grad_wide, grad_vectors, grad_table)


def shards(
    tokens,
    cotangent,
    counts,
    regions,
    square_weights,
    wide_weights,
    vectors,
    bias_table,
    square_moment,
    wide_moment,
    vector_moment,
    table_moment,
):
    full_square, full_wide = (
        lax.all_gather(square_weights.astype(jnp.bfloat16), "group", axis=0, tiled=True),
        lax.all_gather(wide_weights.astype(jnp.bfloat16), "group", axis=0, tiled=True),
    )
    onehot = relative_onehot()
    bias_heads = (
        jnp.dot(onehot, bias_table, precision=HIGHEST).reshape(TOKW, TOKW, HEADS).transpose(2, 0, 1)
    )
    slot_ids = jnp.arange(WIN_DEV)
    own_count = counts[0]
    live_rows = jnp.repeat(slot_ids < own_count, TOKW).astype(jnp.float32)
    results = window_pass(
        tokens, cotangent, regions, live_rows, full_square, full_wide, vectors, bias_heads, onehot
    )
    block_out = results[0]
    grad_tokens = results[1]
    grad_square, grad_wide, grad_vectors, grad_table = (
        results[2],
        results[3],
        results[4],
        results[5],
    )
    ff = full_wide.shape[2]
    wide_blocks = grad_wide.reshape(2, D, ff // D, D).transpose(0, 2, 1, 3)
    grads = jnp.concatenate([grad_square.reshape(2, 2, D, D), wide_blocks], axis=1).astype(jnp.bfloat16)
    small = jnp.concatenate([grad_vectors.reshape(-1), grad_table.reshape(-1)])
    small = jnp.pad(small, (0, 2 * SMALL * 128 - small.shape[0])).reshape(2, SMALL, 128)
    summed, small_sum = make_comm(chip_grid(lax.axis_size("dp")))(grads, small)
    small_sum = small_sum.reshape(-1)
    vec_size = grad_vectors.size
    summed_vectors = small_sum[:vec_size].reshape(grad_vectors.shape)
    summed_table = small_sum[vec_size : vec_size + grad_table.size].reshape(grad_table.shape)
    owned_square, owned_wide, new_square, new_wide, new_square_moment, new_wide_moment = muon(
        summed, square_weights, wide_weights, square_moment, wide_moment
    )
    slots_total = WIN_DEV * lax.axis_size("dp") * lax.axis_size("group")
    slot_root = jnp.sqrt(jnp.float32(slots_total))
    new_vector_moment = MOMENTUM * vector_moment + summed_vectors
    new_vectors = vectors - VECTOR_RATE / slot_root * new_vector_moment
    new_table_moment = MOMENTUM * table_moment + summed_table
    new_table = bias_table - TABLE_RATE / slot_root * new_table_moment
    return (
        block_out,
        grad_tokens,
        owned_square,
        owned_wide,
        summed_vectors,
        summed_table,
        new_square,
        new_wide,
        new_vectors,
        new_table,
        new_square_moment,
        new_wide_moment,
        new_vector_moment,
        new_table_moment,
    )


def solution(mesh):
    in_specs = (
        P(("dp", "group"), None),
        P(("dp", "group"), None),
        P(("dp", "group")),
        P(("dp", "group")),
        P("group", None, None),
        P("group", None, None),
        P(),
        P(),
        P("group", None, None),
        P("group", None, None),
        P(),
        P(),
    )
    out_specs = (
        P(("dp", "group"), None),
        P(("dp", "group"), None),
        P("group", None, None),
        P("group", None, None),
        P(),
        P(),
        P("group", None, None),
        P("group", None, None),
        P(),
        P(),
        P("group", None, None),
        P("group", None, None),
        P(),
        P(),
    )
    return jax.shard_map(shards, mesh=mesh, in_specs=in_specs, out_specs=out_specs, check_vma=False)
```

```python
import functools
import math

import jax
import jax.numpy as jnp
from jax import lax
from jax.experimental import pallas as pl
from jax.experimental.pallas import tpu as pltpu
from jax.sharding import PartitionSpec as P

HIGHEST = lax.Precision.HIGHEST
VECTOR_RATE = 0.05
TABLE_RATE = 1.0
D = 512
HEADS = 16
HEAD_DIM = 32
WIN = 7
WIN_DEV = 16
TOKW = 49
TABLE_ROWS = 169
MASKED = -1e30
EPSILON = 1e-05
MESH = pl.DeviceIdType.MESH

SLOTS_RUN = 10
TALL = 512
PADR = 528
TAIL0 = 480
TAIL = WIN_DEV * TOKW - TAIL0
JR = 56
IR = 64
GH = 8
GC = GH * HEAD_DIM
GL = GH * IR

f32, bf16 = jnp.float32, jnp.bfloat16


def exchange_kernel(sq_hbm, wide_hbm, tok_ref, cot_ref, meta_ref,
                    sq_out, wide_out, tok_out, cot_out, meta_out,
                    sq_in, wide_in, tok_land, sem_in, send, recv):
    dp, group = lax.axis_index("dp"), lax.axis_index("group")
    partner = (dp, 1 - group)
    ff = wide_hbm.shape[2]
    loads = [pltpu.make_async_copy(sq_hbm.at[m], sq_in.at[m], sem_in.at[m]) for m in range(2)]
    loads += [pltpu.make_async_copy(wide_hbm.at[0, pl.ds(128 * c, 128)], wide_in.at[pl.ds(128 * c, 128)], sem_in.at[2 + c])
              for c in range(4)]
    for c in loads:
        c.start()
    barrier = pltpu.get_barrier_semaphore()
    pl.semaphore_signal(barrier, inc=1, device_id=partner, device_id_type=MESH)
    pl.semaphore_wait(barrier, 1)

    def remote(src, dst, k):
        return pltpu.make_async_remote_copy(src_ref=src, dst_ref=dst, send_sem=send.at[k], recv_sem=recv.at[k],
                                            device_id=partner, device_id_type=MESH)

    copies = [remote(meta_ref, meta_out, 6),
              remote(tok_ref.at[pl.ds(TAIL0, TAIL)], tok_out, 7),
              remote(cot_ref.at[pl.ds(TAIL0, TAIL)], cot_out, 8)]
    for c in copies:
        c.start()
    for m in range(2):
        loads[m].wait()

        def body(k, carry):
            r = pl.multiple_of(k * 32, 32)
            sq_out[group, m, pl.ds(r, 32)] = sq_in[m, pl.ds(r, 32)].astype(bf16)
            return carry
        lax.fori_loop(0, D // 32, body, 0)
        c = remote(sq_out.at[group, m], sq_out.at[group, m], m)
        c.start()
        copies.append(c)
    for q in range(4):
        loads[2 + q].wait()

        def body(k, carry):
            r = pl.multiple_of(q * 128 + k * 16, 16)
            wide_out[group, pl.ds(r, 16)] = wide_in[pl.ds(r, 16)].astype(bf16)
            return carry
        lax.fori_loop(0, 8, body, 0)
        piece = pl.ds(128 * q, 128)
        c = remote(wide_out.at[group, piece], wide_out.at[group, piece], 2 + q)
        c.start()
        copies.append(c)
    for c in copies:
        c.wait()


def exchange(sq, wide, tok, cot, meta):
    vmem, any_ = pl.BlockSpec(memory_space=pltpu.VMEM), pl.BlockSpec(memory_space=pl.ANY)
    ff = wide.shape[2]
    return pl.pallas_call(
        exchange_kernel,
        out_shape=(
            jax.ShapeDtypeStruct((2, 2, D, D), bf16),
            jax.ShapeDtypeStruct((2, D, ff), bf16),
            jax.ShapeDtypeStruct((TAIL, D), bf16),
            jax.ShapeDtypeStruct((TAIL, D), bf16),
            jax.ShapeDtypeStruct(meta.shape, jnp.int32),
        ),
        in_specs=[any_, any_, vmem, vmem, vmem],
        out_specs=(vmem,) * 5,
        scratch_shapes=[pltpu.VMEM((2, D, D), f32), pltpu.VMEM((D, ff), f32), pltpu.VMEM((8, 128), f32),
                        pltpu.SemaphoreType.DMA((6,)), pltpu.SemaphoreType.DMA((9,)), pltpu.SemaphoreType.DMA((9,))],
        compiler_params=pltpu.CompilerParams(collective_id=0, has_side_effects=True, vmem_limit_bytes=32 * 2**20),
        name="exchange_weights",
    )(sq, wide, tok, cot, meta)


def nt(a, b):
    return lax.dot_general(a, b, (((1,), (1,)), ((), ())), preferred_element_type=f32)


def tn(a, b):
    return lax.dot_general(a, b, (((0,), (0,)), ((), ())), preferred_element_type=f32)


def nn(a, b):
    return jnp.dot(a, b, preferred_element_type=f32)


def loop_rows(fn, total=TALL, step=64):
    def body(k, carry):
        fn(pl.ds(pl.multiple_of(k * step, step), step))
        return carry
    lax.fori_loop(0, total // step, body, 0)


def block_kernel(mine, theirs, tok, cot, tok_tail, cot_tail, sq, wide, vec, bias,
                 out, out_tail, gtok, gtok_tail, grads, gvec, gtab,
                 x, e, norm, inv, h1, hT, qkv, mask_bias, probs, o, h2, eb, act, dact, u_s, y, dh, dx, dO, wins, dwin, tail_f):
    count = jnp.minimum(mine[0, 0], SLOTS_RUN)
    extra = jnp.maximum(theirs[0, 0] - SLOTS_RUN, 0)
    ff = wide.shape[2]
    chunks = ff // D
    scale = HEAD_DIM ** (-0.5)

    def fill(src, src_tail, dst, masked):
        def body(rows, own):
            v = own.astype(f32)
            if masked:
                index = rows.start + lax.broadcasted_iota(jnp.int32, (rows.size, 1), 0)
                v = jnp.where(index < count * TOKW, v, 0.0)
            dst[rows] = v
        loop_rows(lambda rows: body(rows, src[rows]), 512, 64)
        dst[pl.ds(SLOTS_RUN * TOKW, PADR - SLOTS_RUN * TOKW)] = jnp.zeros((PADR - SLOTS_RUN * TOKW, D), f32)
        loop_rows(lambda rows: tail_f.__setitem__(rows, src_tail[rows].astype(f32)), TAIL, 16)

        for k in range(WIN_DEV - SLOTS_RUN):
            @pl.when(k < extra)
            def _():
                dst[pl.ds((SLOTS_RUN - 1 - k) * TOKW, TOKW)] = tail_f[pl.ds(SLOTS_RUN * TOKW - TAIL0 + k * TOKW, TOKW)]

    fill(tok, tok_tail, x, False)
    fill(cot, cot_tail, e, True)

    def bias_body(c, carry):
        cs = pl.ds(pl.multiple_of(c * 128, 128), 128)
        j = lax.broadcasted_iota(jnp.int32, (JR, 128), 0)
        i = lax.broadcasted_iota(jnp.int32, (JR, 128), 1) & (IR - 1)
        aj, ai = (j * 37) >> 8, (i * 37) >> 8
        bj, bi = j - 7 * aj, i - 7 * ai
        inside = j < TOKW
        same_row = (aj >= 4) == (ai >= 4)
        same_col = (bj >= 4) == (bi >= 4)
        pad = i >= TOKW
        base = bias[:, cs]
        mask_bias[0, :, cs] = jnp.where(inside, base, MASKED)
        mask_bias[1, :, cs] = jnp.where(inside & (same_col | pad), base, MASKED)
        mask_bias[2, :, cs] = jnp.where(inside & (same_row | pad), base, MASKED)
        mask_bias[3, :, cs] = jnp.where(inside & ((same_row & same_col) | pad), base, MASKED)
        return carry
    lax.fori_loop(0, HEADS * IR // 128, bias_body, 0)

    def norm_rows(src, gain, shift, low, k):
        def body(rows):
            v = src[rows]
            center = v - jnp.mean(v, axis=1, keepdims=True)
            r = lax.rsqrt(jnp.mean(center * center, axis=1, keepdims=True) + EPSILON)
            n = center * r
            norm[k, rows] = n
            inv[k, rows] = jnp.broadcast_to(r, (rows.size, 128))
            low[rows] = (n * gain + shift).astype(bf16)
        loop_rows(body)

    norm_rows(x, vec[0:1], vec[2:3], h1, 0)

    def project(m, carry):
        shift = jnp.where(m == 0, vec[4:5], jnp.where(m == 2, vec[5:6], jnp.zeros((1, D), f32)))
        qkv[m, pl.ds(0, TALL)] = nn(h1[...], sq[m]) + shift
        return carry
    lax.fori_loop(0, 3, project, 0)
    o[pl.ds(TALL - 24, PADR - TALL + 24)] = jnp.zeros((PADR - TALL + 24, D), f32)
    live_i = lax.broadcasted_iota(jnp.int32, (IR, 1), 0) < TOKW

    def spread_windows(src, dst):
        for w in range(SLOTS_RUN):
            def body(c, carry):
                cs = pl.ds(pl.multiple_of(c * 128, 128), 128)
                dst[pl.ds(w * IR, IR), cs] = jnp.where(live_i, src[pl.ds(w * TOKW, IR), cs], 0.0).astype(bf16)
                return carry
            lax.fori_loop(0, D // 128, body, 0)

    def pack_windows(src, dst):
        for w in range(SLOTS_RUN):
            def body(c, carry):
                cs = pl.ds(pl.multiple_of(c * 128, 128), 128)
                dst[pl.ds(w * TOKW, TOKW), cs] = src[pl.ds(w * IR, TOKW), cs]
                return carry
            lax.fori_loop(0, D // 128, body, 0)

    for m in range(3):
        spread_windows(qkv.at[m], wins.at[m])

    lane_head = lax.broadcasted_iota(jnp.int32, (GH, 1, GC), 2) >> 5
    row_head = lax.broadcasted_iota(jnp.int32, (GH, 1, GC), 0)
    pick = lane_head == row_head
    pick_f = pick.astype(f32)
    pick_b = pick_f.astype(bf16)

    def spread(b):
        return (b[None] * pick_b).reshape(GL, GC)

    def gather(result):
        return jnp.sum(result.reshape(GH, IR, GC) * pick_f, axis=0)

    def place(t):
        w, hg = lax.div(t, 2), lax.rem(t, 2)
        return w, pl.multiple_of(w * IR, IR), pl.ds(pl.multiple_of(hg * GC, 128), GC), pl.ds(pl.multiple_of(hg * GL, 128), GL)

    def kind_of(w):
        own = mine[0, 1 + w]
        other = theirs[0, 1 + jnp.maximum(2 * SLOTS_RUN - 1 - w, SLOTS_RUN) % WIN_DEV]
        region = jnp.where(w >= SLOTS_RUN - extra, other, own)
        return jnp.where(region == 1, 1, jnp.where(region == 3, 2, jnp.where(region == 4, 3, 0)))

    def attend(t, carry):
        w, row, cs, ls = place(t)
        qd = spread(wins[0, pl.ds(row, IR), cs])
        kb = wins[1, pl.ds(row, JR), cs]
        vb = wins[2, pl.ds(row, JR), cs]
        s = nt(kb, qd) * scale + mask_bias[kind_of(w), :, ls]
        top = jnp.max(s, axis=0, keepdims=True)
        p = jnp.exp(s - top)
        p = p * (1.0 / jnp.sum(p, axis=0, keepdims=True))
        probs[t] = p
        dwin[0, pl.ds(row, IR), cs] = gather(tn(p.astype(bf16), vb))
        return carry
    lax.fori_loop(0, 2 * SLOTS_RUN, attend, 0)

    pack_windows(dwin.at[0], o)

    ob = h2
    loop_rows(lambda rows: ob.__setitem__(rows, o[rows].astype(bf16)))
    y[...] = x[pl.ds(0, TALL)] + (nn(ob[...], sq[3]) + vec[6:7])
    hT[0] = o[pl.ds(0, TALL)].T.astype(bf16)
    norm_rows(y, vec[1:2], vec[3:4], h2, 1)
    hT[1] = h2[...].astype(f32).T.astype(bf16)
    hT[2] = e[pl.ds(0, TALL)].T.astype(bf16)
    loop_rows(lambda rows: eb.__setitem__(rows, e[rows].astype(bf16)))
    dh[...] = jnp.zeros((TALL, D), f32)

    def feed(c, carry):
        cs = pl.ds(pl.multiple_of(c * D, 128), D)
        u_s[...] = nn(h2[...], wide[0, :, cs]) + vec[pl.ds(8 + c, 1)]
        dh_c = nn(eb[...], wide[1, :, cs])
        dO[pl.ds(0, TALL)] = dh_c

        def body(rows):
            u = u_s[rows]
            cdf = 0.5 * (1.0 + lax.erf(u * 0.7071067811865476))
            density = jnp.exp(-0.5 * u * u) * 0.3989422804014327
            act[rows] = (u * cdf).astype(bf16)
            dact[rows] = (dO[rows] * (cdf + u * density)).astype(bf16)
        loop_rows(body, TALL, 16)
        y[...] += nt(act[...], wide[1, :, cs])
        dh[...] += nt(dact[...], wide[0, :, cs])
        grads[1, 2 + c] = nn(hT[2], act[...]).astype(bf16)
        grads[0, 2 + c] = nn(hT[1], dact[...]).astype(bf16)
        gvec[pl.ds(8 + c, 1)] = jnp.sum(dact[...].astype(f32), axis=0, keepdims=True)
        return carry
    lax.fori_loop(0, chunks, feed, 0)

    def norm_back(grad, gain, k, add, dst):
        zero = jnp.zeros((1, D), f32)

        def body(i, carry):
            rows = pl.ds(pl.multiple_of(i * 64, 64), 64)
            g_gain, g_shift = carry
            g = grad[rows]
            n = norm[k, rows]
            dn = g * gain
            r = inv[k, rows][:, :1]
            dst[rows] = add[rows] + r * (dn - jnp.mean(dn, axis=1, keepdims=True)
                                         - n * jnp.mean(dn * n, axis=1, keepdims=True))
            return (g_gain + jnp.sum(g * n, axis=0, keepdims=True), g_shift + jnp.sum(g, axis=0, keepdims=True))
        return lax.fori_loop(0, TALL // 64, body, (zero, zero))

    gvec[1:2], gvec[3:4] = norm_back(dh, vec[1:2], 1, e, dx)
    gvec[7:8] = jnp.sum(e[pl.ds(0, TALL)], axis=0, keepdims=True)

    def put(src, dst, dst_tail):
        def own(rows):
            index = rows.start + lax.broadcasted_iota(jnp.int32, (rows.size, 1), 0)
            dst[rows] = jnp.where(index < count * TOKW, src[rows], 0.0).astype(bf16)
        loop_rows(own, 512, 64)
        dst[pl.ds(512, WIN_DEV * TOKW - 512)] = jnp.zeros((WIN_DEV * TOKW - 512, D), bf16)
        tail_f[...] = jnp.zeros((TAIL + 16, D), f32)

        for k in range(WIN_DEV - SLOTS_RUN):
            @pl.when(k < extra)
            def _():
                tail_f[pl.ds(SLOTS_RUN * TOKW - TAIL0 + k * TOKW, TOKW)] = src[pl.ds((SLOTS_RUN - 1 - k) * TOKW, TOKW)]
        loop_rows(lambda rows: dst_tail.__setitem__(rows, tail_f[rows].astype(bf16)), TAIL, 16)

    y[...] += vec[7:8]
    put(y, out, out_tail)

    loop_rows(lambda rows: eb.__setitem__(rows, dx[rows].astype(bf16)))
    gvec[6:7] = jnp.sum(eb[...].astype(f32), axis=0, keepdims=True)
    grads[1, 1] = nn(hT[0], eb[...]).astype(bf16)
    dO[pl.ds(0, TALL)] = nt(eb[...], sq[3])
    spread_windows(dO, wins.at[3])
    gtab[...] = jnp.zeros((JR, HEADS * IR), f32)

    def attend_back(t, carry):
        w, row, cs, ls = place(t)
        dd = spread(wins[3, pl.ds(row, IR), cs])
        qd = spread(wins[0, pl.ds(row, IR), cs])
        kb = wins[1, pl.ds(row, JR), cs]
        vb = wins[2, pl.ds(row, JR), cs]
        p = probs[t]
        dp = nt(vb, dd)
        dwin[2, pl.ds(row, JR), cs] = nn(p.astype(bf16), dd)
        ds = p * (dp - jnp.sum(p * dp, axis=0, keepdims=True))
        dsb = ds.astype(bf16)
        gtab[:, ls] += dsb.astype(f32)
        dwin[1, pl.ds(row, JR), cs] = nn(dsb, qd) * scale
        dwin[0, pl.ds(row, IR), cs] = gather(tn(dsb, kb)) * scale
        return carry
    lax.fori_loop(0, 2 * SLOTS_RUN, attend_back, 0)

    for m in range(3):
        qkv[m, pl.ds(TALL - 24, PADR - TALL + 24)] = jnp.zeros((PADR - TALL + 24, D), f32)
        pack_windows(dwin.at[m], qkv.at[m])
    hT[0] = h1[...].astype(f32).T.astype(bf16)
    dh[...] = jnp.zeros((TALL, D), f32)

    def input_grads(m, carry):
        loop_rows(lambda rows: eb.__setitem__(rows, qkv[m, rows].astype(bf16)))
        total = jnp.sum(eb[...].astype(f32), axis=0, keepdims=True)

        @pl.when(m == 0)
        def _():
            gvec[4:5] = total

        @pl.when(m == 2)
        def _():
            gvec[5:6] = total
        dh[...] += nt(eb[...], sq[m])
        grads[lax.div(m, 2), lax.rem(m, 2)] = nn(hT[0], eb[...]).astype(bf16)
        return carry
    lax.fori_loop(0, 3, input_grads, 0)
    gvec[0:1], gvec[2:3] = norm_back(dh, vec[0:1], 0, dx, y)
    put(y, gtok, gtok_tail)


def block(mine, theirs, tok, cot, tok_tail, cot_tail, sq, wide, vec, bias):
    vmem, smem = pl.BlockSpec(memory_space=pltpu.VMEM), pl.BlockSpec(memory_space=pltpu.SMEM)
    ff = wide.shape[2]
    V = pltpu.VMEM
    return pl.pallas_call(
        block_kernel,
        out_shape=(
            jax.ShapeDtypeStruct(tok.shape, bf16), jax.ShapeDtypeStruct((TAIL, D), bf16),
            jax.ShapeDtypeStruct(tok.shape, bf16), jax.ShapeDtypeStruct((TAIL, D), bf16),
            jax.ShapeDtypeStruct((2, 2 + ff // D, D, D), bf16),
            jax.ShapeDtypeStruct(vec.shape, f32),
            jax.ShapeDtypeStruct((JR, HEADS * IR), f32),
        ),
        in_specs=[smem, smem] + [vmem] * 8,
        out_specs=(vmem,) * 7,
        scratch_shapes=[
            V((PADR, D), f32), V((PADR, D), f32), V((2, TALL, D), f32), V((2, TALL, 128), f32),
            V((TALL, D), bf16), V((3, D, TALL), bf16), V((3, PADR, D), f32), V((4, JR, HEADS * IR), f32),
            V((2 * SLOTS_RUN, JR, GL), f32), V((PADR, D), f32), V((TALL, D), bf16), V((TALL, D), bf16),
            V((TALL, D), bf16), V((TALL, D), bf16), V((TALL, D), f32), V((TALL, D), f32), V((TALL, D), f32),
            V((TALL, D), f32), V((PADR, D), f32), V((4, SLOTS_RUN * IR, D), bf16), V((3, SLOTS_RUN * IR, D), f32), V((TAIL + 16, D), f32),
        ],
        compiler_params=pltpu.CompilerParams(vmem_limit_bytes=58 * 2**20),
        name="window_block",
    )(mine, theirs, tok, cot, tok_tail, cot_tail, sq.reshape(4, D, D), wide, vec, bias)


def relative_onehot_t():
    j = jnp.arange(TOKW)[:, None]
    i = jnp.arange(IR)[None, :]
    rel = (i // WIN - j // WIN + WIN - 1) * (2 * WIN - 1) + i % WIN - j % WIN + WIN - 1
    hot = (rel[:, :, None] == jnp.arange(TABLE_ROWS)) & (i < TOKW)[:, :, None]
    return hot.astype(f32)


BLK = 512
HALF = 6
ORDER = (2, 3, 4, 5, 0, 1)
SMALL = 40


def chip_grid(dp):
    side = max(1, math.isqrt(dp // 4))
    if side * side * 4 == dp:
        return (side, side, 4)
    return (1, 1, dp)


class Lane:
    def __init__(self, size, pos, stride, dp, group):
        self.n, self.i, self.stride, self.dp, self.group = size, pos, stride, dp, group

    def peer(self, delta):
        return (self.dp + delta * self.stride, self.group)


class Ids:
    def __init__(self):
        self.count = 0

    def take(self, number=1):
        first = self.count
        self.count += number
        return first


def lanes(sizes):
    dp, group = lax.axis_index("dp"), lax.axis_index("group")
    nx, ny, nz = sizes
    x, y, z = lax.rem(dp, nx), lax.rem(lax.div(dp, nx), ny), lax.div(dp, nx * ny)
    return (
        Lane(nx, x, 1, dp, group),
        Lane(ny, y, nx, dp, group),
        Lane(nz, z, nx * ny, dp, group),
    )


class Plan:
    def __init__(self, sizes, pieces):
        nx, ny, nz = sizes
        self.orders = ((0, 2, 1), (1, 2, 0))
        self.rs, self.ag = Ids(), Ids()
        self.rows = 0
        self.slots = {}
        half = BLK // 2
        for piece in range(pieces):
            color = piece % 2
            rows = half
            for stage, dim in enumerate(self.orders[color]):
                n = sizes[dim]
                if stage < 2:
                    rows = rows // n
                land = {}
                for way in ("R", "L"):
                    for j in range(n):
                        if (way == "R" and j > 0) or (way == "L" and j < n - 1):
                            land[way, j] = (self.rs.take(), self.rows)
                            self.rows += rows
                ag_recv = self.ag.take(n)
                self.slots[piece, stage] = (land, ag_recv)


def make_comm(sizes):
    pieces = 2 * HALF
    plan = Plan(sizes, pieces)

    def tasks_for(piece, env):
        (lane_all, own_ref, core_land, acc, out_ref, land_ref, rs_send, rs_recv, ag_sl, ag_sr, ag_recv,
         core_send_sem, core_recv_sem, partner, ends, grads_ref) = env
        color = piece % 2
        block = ORDER[piece // 2]
        base = color * (BLK // 2)
        half = BLK // 2
        order = plan.orders[color]
        dims = [lane_all[d] for d in order]
        tasks = []

        def add_into(dst, dst_rows, dst_cols, src_row, rows, cols_w, col0=0):
            step = min(rows, 32)

            def body(k, carry):
                r = pl.multiple_of(dst_rows + k * step, 16)
                s = pl.multiple_of(src_row + k * step, 16)
                here = acc[block, pl.ds(r, step), dst_cols].astype(jnp.float32)
                there = land_ref[pl.ds(s, step), pl.ds(0, cols_w)].astype(jnp.float32)
                dst[block, pl.ds(r, step), dst_cols] = (here + there).astype(jnp.bfloat16)
                return carry

            if rows == step:
                body(0, 0)
            else:
                lax.fori_loop(0, rows // step, body, 0)

        all_cols = pl.ds(0, BLK)

        r_sizes = [half // dims[0].n, half // dims[0].n // dims[1].n]
        off0 = base
        off1 = off0 + dims[0].i * r_sizes[0]
        off2 = off1 + dims[1].i * r_sizes[1]
        cols = BLK // dims[2].n

        def view(stage, j):
            if stage == 0:
                return pl.multiple_of(off0 + j * r_sizes[0], 16), r_sizes[0], pl.ds(0, BLK), BLK
            if stage == 1:
                return pl.multiple_of(off1 + j * r_sizes[1], 16), r_sizes[1], pl.ds(0, BLK), BLK
            start = j * cols if isinstance(j, int) else pl.multiple_of(j * cols, 128)
            return pl.multiple_of(off2, 16), r_sizes[1], pl.ds(start, cols), cols

        def rs_copy(stage, way, j):
            land, _ = plan.slots[piece, stage]
            sem, row = land[way, j]
            lane = dims[stage]
            r, rows, cs, width = view(stage, j)
            return pltpu.make_async_remote_copy(
                src_ref=acc.at[block, pl.ds(r, rows), cs],
                dst_ref=land_ref.at[pl.ds(row, rows), pl.ds(0, width)],
                send_sem=rs_send.at[sem],
                recv_sem=rs_recv.at[sem],
                device_id=lane.peer(1 if way == "R" else -1),
                device_id_type=MESH,
            )

        def rs_tick(stage, h):
            lane = dims[stage]
            n = lane.n
            land, _ = plan.slots[piece, stage]
            last = stage == 2

            @pl.when(lane.i == h)
            def _():
                for j in range(n - 1, h - 1, -1):
                    if h > 0:
                        rs_copy(stage, "R", j).wait_recv()
                        r, rows, cs, width = view(stage, j)
                        add_into(acc, r, cs, land["R", j][1], rows, width)
                    if j > h:
                        rs_copy(stage, "R", j).start()

            @pl.when(lane.i == n - 1 - h)
            def _():
                for j in range(0, n - h):
                    if h > 0:
                        rs_copy(stage, "L", j).wait_recv()
                        r, rows, cs, width = view(stage, j)
                        add_into(acc, r, cs, land["L", j][1], rows, width)
                    if j < n - 1 - h:
                        rs_copy(stage, "L", j).start()

        def rs_end(stage):
            lane = dims[stage]
            n = lane.n
            for j in range(n):
                if j > 0:
                    @pl.when(lane.i < j)
                    def _():
                        rs_copy(stage, "R", j).wait_send()
                if j < n - 1:
                    @pl.when(lane.i > j)
                    def _():
                        rs_copy(stage, "L", j).wait_send()

        def ag_copy(stage, j, way):
            _, first = plan.slots[piece, stage]
            lane = dims[stage]
            r, rows, cs, width = view(stage, j)
            piece_ref = out_ref.at[block, pl.ds(r, rows), cs]
            return pltpu.make_async_remote_copy(
                src_ref=piece_ref,
                dst_ref=piece_ref,
                send_sem=(ag_sr if way > 0 else ag_sl).at[first + j],
                recv_sem=ag_recv.at[first + j],
                device_id=lane.peer(way),
                device_id_type=MESH,
            )

        def ag_tick(stage, h):
            lane = dims[stage]
            n, i = lane.n, lane.i
            if h == 0:
                @pl.when(i < n - 1)
                def _():
                    ag_copy(stage, i, 1).start()

                @pl.when(i > 0)
                def _():
                    ag_copy(stage, i, -1).start()
                return

            @pl.when(i >= h)
            def _():
                ag_copy(stage, i - h, -1).wait_recv()

                @pl.when(i < n - 1)
                def _():
                    ag_copy(stage, i - h, 1).start()

            @pl.when(i + h <= n - 1)
            def _():
                ag_copy(stage, i + h, 1).wait_recv()

                @pl.when(i > 0)
                def _():
                    ag_copy(stage, i + h, -1).start()

        def ag_end(stage):
            lane = dims[stage]
            n, i = lane.n, lane.i
            for h in range(n):
                @pl.when((i >= h) & (i < n - 1))
                def _():
                    ag_copy(stage, i - h, 1).wait_send()

                @pl.when((i + h <= n - 1) & (i > 0))
                def _():
                    ag_copy(stage, i + h, -1).wait_send()

        def core_copy():
            return pltpu.make_async_remote_copy(
                src_ref=grads_ref.at[1 - partner[2], block, pl.ds(base, half)],
                dst_ref=core_land.at[block, pl.ds(base, half)],
                send_sem=core_send_sem.at[piece],
                recv_sem=core_recv_sem.at[piece],
                device_id=partner[:2],
                device_id_type=MESH,
            )

        def first():
            core_copy().wait_recv()

            def body(k, carry):
                r = pl.multiple_of(base + k * 32, 16)
                here = grads_ref[partner[2], block, pl.ds(r, 32)].astype(jnp.float32)
                there = core_land[block, pl.ds(r, 32)].astype(jnp.float32)
                acc[block, pl.ds(r, 32)] = (here + there).astype(jnp.bfloat16)
                return carry

            lax.fori_loop(0, half // 32, body, 0)

        def copy_out():
            r, rows, cs, width = view(2, dims[2].i)
            out_ref[block, pl.ds(r, rows), cs] = acc[block, pl.ds(r, rows), cs]

        flat = [first]
        groups = []
        for stage in range(3):
            for h in range(dims[stage].n):
                groups.append((h == 0, functools.partial(rs_tick, stage, h)))
        groups.append((False, copy_out))
        for stage in (2, 1, 0):
            for h in range(dims[stage].n):
                groups.append((h == 0, functools.partial(ag_tick, stage, h)))
        ticks = [[first]]
        for joined, task in groups:
            if joined or task is copy_out:
                ticks[-1].append(task)
            else:
                ticks.append([task])
        for stage in range(3):
            ends.append(functools.partial(rs_end, stage))
            ends.append(functools.partial(ag_end, stage))
        ends.append(lambda: core_copy().wait_send())
        return core_copy, ticks

    def kernel(grads_ref, small_ref, tail_a, tail_b, out_ref, small_out, back_a, back_b, core_land, acc, land_ref, small_core, small_land,
               rs_send, rs_recv, ag_sl, ag_sr, ag_recv, core_s, core_r, sm_cs, sm_cr, sm_s, sm_r, bk_s, bk_r, *, delta):
        lane_all = lanes(sizes)
        dp, group = lax.axis_index("dp"), lax.axis_index("group")
        partner = (dp, 1 - group, group)

        barrier = pltpu.get_barrier_semaphore()
        total = 1
        pl.semaphore_signal(barrier, inc=1, device_id=partner[:2], device_id_type=MESH)
        for lane in lane_all:
            for k in range(1, lane.n):
                to = lax.rem(lane.i + k, lane.n)
                pl.semaphore_signal(barrier, inc=1, device_id=lane.peer(to - lane.i), device_id_type=MESH)
                total += 1
        pl.semaphore_wait(barrier, total)

        ends = []
        env = (lane_all, None, core_land, acc, out_ref, land_ref, rs_send, rs_recv, ag_sl, ag_sr, ag_recv,
               core_s, core_r, partner, ends, grads_ref)

        def sm_core():
            return pltpu.make_async_remote_copy(
                src_ref=small_ref.at[1 - group], dst_ref=small_core, send_sem=sm_cs.at[0], recv_sem=sm_cr.at[0],
                device_id=partner[:2], device_id_type=MESH)

        def sm_back():
            return pltpu.make_async_remote_copy(
                src_ref=small_out.at[group], dst_ref=small_out.at[group], send_sem=sm_cs.at[1], recv_sem=sm_cr.at[1],
                device_id=partner[:2], device_id_type=MESH)

        first_slot = [0, sizes[0], sizes[0] + sizes[1]]

        def sm_copy(d, k):
            lane = lane_all[d]
            to = lax.rem(lane.i + k, lane.n)
            return pltpu.make_async_remote_copy(
                src_ref=small_land.at[first_slot[d] + lane.i],
                dst_ref=small_land.at[first_slot[d] + lane.i],
                send_sem=sm_s.at[first_slot[d] + k],
                recv_sem=sm_r.at[first_slot[d] + lane.i],
                device_id=lane.peer(to - lane.i), device_id_type=MESH)

        def sm_wait(d, k):
            lane = lane_all[d]
            source = lax.rem(lane.i + k, lane.n)
            pltpu.make_async_remote_copy(
                src_ref=small_land.at[first_slot[d] + source],
                dst_ref=small_land.at[first_slot[d] + source],
                send_sem=sm_s.at[first_slot[d] + k],
                recv_sem=sm_r.at[first_slot[d] + source],
                device_id=lane.peer(source - lane.i), device_id_type=MESH).wait_recv()

        def sm_start(d, value):
            lane = lane_all[d]
            small_land[first_slot[d] + lane.i] = value
            for k in range(1, lane.n):
                sm_copy(d, k).start()

        def sm_finish(d):
            lane = lane_all[d]
            for k in range(1, lane.n):
                sm_wait(d, k)
            value = small_land[first_slot[d]]
            for j in range(1, lane.n):
                value = value + small_land[first_slot[d] + j]
            return value

        def sm0():
            sm_core().wait_recv()
            sm_start(0, small_ref[group] + small_core[...])

        def sm1():
            sm_start(1, sm_finish(0))

        def sm2():
            sm_start(2, sm_finish(1))

        def sm3():
            small_out[group] = sm_finish(2)
            sm_back().start()

        def sm4():
            sm_back().wait_recv()

        def back(k):
            return pltpu.make_async_remote_copy(
                src_ref=(tail_a, tail_b)[k], dst_ref=(back_a, back_b)[k], send_sem=bk_s.at[k], recv_sem=bk_r.at[k],
                device_id=partner[:2], device_id_type=MESH)

        sm_core().start()
        made = [tasks_for(p, env) for p in range(pieces)]
        for core_copy, _ in made:
            core_copy().start()
        for k in range(2):
            back(k).start()
        table = {}
        length = max(len(t) for _, t in made)
        for p, (_, ticks) in enumerate(made):
            for k, tick in enumerate(ticks):
                table.setdefault(int(delta * (p // 2)) + k, []).append((p, tick))
        for k, task in enumerate((sm0, sm1, sm2, sm3, sm4)):
            table.setdefault(1 + 2 * k, []).append((-1, [task]))
        for when in sorted(table):
            for p, tick in sorted(table[when], key=lambda e: e[0]):
                for task in tick:
                    task()
        for task in ends:
            task()
        for k in range(2):
            back(k).wait()
        sm_core().wait_send()
        sm_back().wait_send()
        for d in range(3):
            for k in range(1, sizes[d]):
                sm_copy(d, k).wait_send()

    def call(grads, small, tail_a, tail_b, delta=1.0):
        dma = pltpu.SemaphoreType.DMA
        vmem = pl.BlockSpec(memory_space=pltpu.VMEM)
        return pl.pallas_call(
            functools.partial(kernel, delta=delta),
            out_shape=(
                jax.ShapeDtypeStruct((HALF, BLK, BLK), jnp.bfloat16),
                jax.ShapeDtypeStruct((2, SMALL, 128), jnp.float32),
                jax.ShapeDtypeStruct(tail_a.shape, tail_a.dtype),
                jax.ShapeDtypeStruct(tail_b.shape, tail_b.dtype),
            ),
            in_specs=[vmem, vmem, vmem, vmem],
            out_specs=[vmem, vmem, vmem, vmem],
            scratch_shapes=[
                pltpu.VMEM((HALF, BLK, BLK), jnp.bfloat16),
                pltpu.VMEM((HALF, BLK, BLK), jnp.bfloat16),
                pltpu.VMEM((plan.rows, BLK), jnp.bfloat16),
                pltpu.VMEM((SMALL, 128), jnp.float32),
                pltpu.VMEM((sum(sizes), SMALL, 128), jnp.float32),
                dma((plan.rs.count,)),
                dma((plan.rs.count,)),
                dma((plan.ag.count,)),
                dma((plan.ag.count,)),
                dma((plan.ag.count,)),
                dma((pieces,)),
                dma((pieces,)),
                dma((2,)),
                dma((2,)),
                dma((sum(sizes),)),
                dma((sum(sizes),)),
                dma((2,)),
                dma((2,)),
            ],
            compiler_params=pltpu.CompilerParams(
                collective_id=1, has_side_effects=True, vmem_limit_bytes=56 * 2**20
            ),
            name="reduce_gradients",
        )(grads, small, tail_a, tail_b)

    return call


MOMENTUM = 0.9
MATRIX_RATE = 0.4
NEWTON_ONE = 3.4445
NEWTON_TWO = -4.775
NEWTON_THREE = 2.0315
STEP = 32


def muon_kernel(g_hbm, sw_hbm, ww_hbm, sm_hbm, wm_hbm, row_a, row_b, back_a, back_b,
                gs_out, gw_out, ns_out, nw_out, nsm_out, nwm_out, out_a, out_b,
                g, sw, ww, sm, wm, gs, gw, xs, xw, gram, mix, own, back, sem_in, sem_out, sem_row):
    ff = ww.shape[2]
    cols = ff // D

    def load(src, dst, k):
        return pltpu.make_async_copy(src, dst, sem_in.at[k])

    loads = [load(g_hbm.at[pl.ds(0, 2)], g.at[pl.ds(0, 2)], 0), load(sm_hbm, sm, 1),
             load(g_hbm.at[pl.ds(2, cols)], g.at[pl.ds(2, cols)], 2), load(wm_hbm, wm, 3),
             load(sw_hbm, sw, 4), load(ww_hbm, ww, 5)]
    for c in loads:
        c.start()
    first, rows = row_a.shape[0] - back.shape[1], back.shape[1]
    fetch, put = [], []
    for k, (mine, theirs, out) in enumerate(((row_a, back_a, out_a), (row_b, back_b, out_b))):
        fetch.append(pltpu.make_async_copy(mine.at[pl.ds(first, rows)], own.at[k], sem_row.at[k]))
        fetch.append(pltpu.make_async_copy(theirs, back.at[k], sem_row.at[2 + k]))
        put.append(pltpu.make_async_copy(own.at[k], out.at[pl.ds(first, rows)], sem_row.at[4 + k]))
    for c in fetch:
        c.start()
    stores = [pltpu.make_async_copy(a, b, sem_out.at[k]) for k, (a, b) in enumerate(
        ((gs, gs_out), (sm, nsm_out), (gw, gw_out), (wm, nwm_out), (sw, ns_out), (ww, nw_out)))]

    def scan(moment, grad, pick):
        def body(k, total):
            r = pl.multiple_of(k * STEP, STEP)
            new = None
            part = jnp.zeros((STEP, D), jnp.float32)
            for c, block in enumerate(pick):
                cs = pl.ds(c * D, D)
                add = g[block, pl.ds(r, STEP)].astype(jnp.float32)
                grad[pl.ds(r, STEP), cs] = add
                new = MOMENTUM * moment[pl.ds(r, STEP), cs] + add
                moment[pl.ds(r, STEP), cs] = new
                part = part + new * new
            return total + part
        total = lax.fori_loop(0, D // STEP, body, jnp.zeros((STEP, D), jnp.float32))
        return jnp.sum(total)

    def scale(moment, x, total, width):
        size = jnp.sqrt(jnp.full((1, D), total, jnp.float32)) + 1e-07

        def body(k, carry):
            r = pl.multiple_of(k * STEP, STEP)
            for c in range(width // D):
                cs = pl.ds(c * D, D)
                x[pl.ds(r, STEP), cs] = (moment[pl.ds(r, STEP), cs] / size).astype(jnp.bfloat16)
            return carry
        lax.fori_loop(0, D // STEP, body, 0)

    dot_t = functools.partial(lax.dot_general, dimension_numbers=(((1,), (1,)), ((), ())),
                              preferred_element_type=jnp.float32)

    def newton(many, width):
        def body(k, carry):
            for m in range(len(many)):
                x = many[m]
                gram[m] = dot_t(x[...], x[...]).astype(jnp.bfloat16)
            for m in range(len(many)):
                a = gram[m]
                square = jnp.dot(a, a, preferred_element_type=jnp.float32)
                mix[m] = (NEWTON_TWO * a.astype(jnp.float32) + NEWTON_THREE * square).astype(jnp.bfloat16)
            for m in range(len(many)):
                x = many[m]
                for c in range(width // D):
                    cs = pl.ds(c * D, D)
                    old = x[:, cs]
                    x[:, cs] = (NEWTON_ONE * old.astype(jnp.float32)
                                + jnp.dot(mix[m], old, preferred_element_type=jnp.float32)).astype(jnp.bfloat16)
            return carry
        lax.fori_loop(0, 5, body, 0)

    def finish(weight, x, width):
        def body(k, carry):
            r = pl.multiple_of(k * STEP, STEP)
            for c in range(width // D):
                cs = pl.ds(c * D, D)
                weight[pl.ds(r, STEP), cs] = weight[pl.ds(r, STEP), cs] - MATRIX_RATE * x[pl.ds(r, STEP), cs].astype(jnp.float32)
            return carry
        lax.fori_loop(0, D // STEP, body, 0)

    loads[0].wait()
    loads[1].wait()
    for m in range(2):
        total = scan(sm.at[m], gs.at[m], (m,))
        scale(sm.at[m], xs.at[m], total, D)
    stores[0].start()
    stores[1].start()
    loads[2].wait()
    loads[3].wait()
    total = scan(wm.at[0], gw.at[0], tuple(range(2, 2 + cols)))
    scale(wm.at[0], xw, total, ff)
    stores[2].start()
    stores[3].start()
    for c in fetch:
        c.wait()
    for k in range(2):
        def join(i, carry):
            r = pl.ds(pl.multiple_of(i * 16, 16), 16)
            own[k, r] = own[k, r] + back[k, r]
            return carry
        lax.fori_loop(0, rows // 16, join, 0)
        put[k].start()
    newton([xs.at[0], xs.at[1]], D)
    loads[4].wait()
    for m in range(2):
        finish(sw.at[m], xs.at[m], D)
    stores[4].start()
    newton([xw], ff)
    loads[5].wait()
    finish(ww.at[0], xw, ff)
    stores[5].start()
    for c in stores + put:
        c.wait()


def muon(g, sw, ww, sm, wm, row_a, row_b, back_a, back_b):
    any_ = pl.BlockSpec(memory_space=pl.ANY)
    shapes = [sw, ww, sw, ww, sm, wm]
    f32 = jnp.float32
    return pl.pallas_call(
        muon_kernel,
        out_shape=tuple(jax.ShapeDtypeStruct(a.shape, f32) for a in shapes)
        + tuple(jax.ShapeDtypeStruct(a.shape, a.dtype) for a in (row_a, row_b)),
        in_specs=[any_] * 9,
        out_specs=(any_,) * 8,
        input_output_aliases={5: 6, 6: 7},
        scratch_shapes=[
            pltpu.VMEM(g.shape, jnp.bfloat16),
            pltpu.VMEM(sw.shape, f32), pltpu.VMEM(ww.shape, f32),
            pltpu.VMEM(sm.shape, f32), pltpu.VMEM(wm.shape, f32),
            pltpu.VMEM(sw.shape, f32), pltpu.VMEM(ww.shape, f32),
            pltpu.VMEM((2, D, D), jnp.bfloat16), pltpu.VMEM((D, ww.shape[2]), jnp.bfloat16),
            pltpu.VMEM((2, D, D), jnp.bfloat16), pltpu.VMEM((2, D, D), jnp.bfloat16),
            pltpu.VMEM((2,) + back_a.shape, jnp.bfloat16), pltpu.VMEM((2,) + back_a.shape, jnp.bfloat16),
            pltpu.SemaphoreType.DMA((6,)), pltpu.SemaphoreType.DMA((6,)), pltpu.SemaphoreType.DMA((6,)),
        ],
        compiler_params=pltpu.CompilerParams(vmem_limit_bytes=58 * 2**20),
        name="muon_step",
    )(g, sw, ww, sm, wm, row_a, row_b, back_a, back_b)


def shards(
    tokens,
    cotangent,
    counts,
    regions,
    square_weights,
    wide_weights,
    vectors,
    bias_table,
    square_moment,
    wide_moment,
    vector_moment,
    table_moment,
):
    meta = jnp.concatenate([counts, regions[::TOKW]])
    meta = jnp.pad(meta[None], ((0, 7), (0, 128 - meta.shape[0])))
    square_low, wide_low, tok_tail, cot_tail, meta_theirs = exchange(
        square_weights, wide_weights, tokens, cotangent, meta
    )
    hot = relative_onehot_t()
    bias = jnp.dot(hot.reshape(-1, TABLE_ROWS), bias_table, precision=HIGHEST)
    bias = bias.reshape(TOKW, IR, HEADS).transpose(0, 2, 1).reshape(TOKW, HEADS * IR)
    bias = jnp.pad(bias, ((0, JR - TOKW), (0, 0)))
    out, out_tail, gtok, gtok_tail, grads, grad_vectors, pair_sum = block(
        meta, meta_theirs, tokens, cotangent, tok_tail, cot_tail, square_low, wide_low, vectors, bias
    )
    pair_sum = pair_sum[:TOKW].reshape(TOKW, HEADS, IR)
    grad_table = jnp.einsum("jir,jhi->rh", hot, pair_sum, precision=HIGHEST)
    small = jnp.concatenate([grad_vectors.reshape(-1), grad_table.reshape(-1)])
    small = jnp.pad(small, (0, 2 * SMALL * 128 - small.shape[0])).reshape(2, SMALL, 128)
    summed, small_sum, out_back, gtok_back = make_comm(chip_grid(lax.axis_size("dp")))(
        grads, small, out_tail, gtok_tail
    )
    small_sum = small_sum.reshape(-1)
    vec_size = grad_vectors.size
    summed_vectors = small_sum[:vec_size].reshape(grad_vectors.shape)
    summed_table = small_sum[vec_size : vec_size + grad_table.size].reshape(grad_table.shape)
    owned_square, owned_wide, new_square, new_wide, new_square_moment, new_wide_moment, block_out, grad_tokens = muon(
        summed, square_weights, wide_weights, square_moment, wide_moment, out, gtok, out_back, gtok_back
    )
    slots_total = WIN_DEV * lax.axis_size("dp") * lax.axis_size("group")
    slot_root = jnp.sqrt(jnp.float32(slots_total))
    new_vector_moment = MOMENTUM * vector_moment + summed_vectors
    new_vectors = vectors - VECTOR_RATE / slot_root * new_vector_moment
    new_table_moment = MOMENTUM * table_moment + summed_table
    new_table = bias_table - TABLE_RATE / slot_root * new_table_moment
    return (
        block_out,
        grad_tokens,
        owned_square,
        owned_wide,
        summed_vectors,
        summed_table,
        new_square,
        new_wide,
        new_vectors,
        new_table,
        new_square_moment,
        new_wide_moment,
        new_vector_moment,
        new_table_moment,
    )


def solution(mesh):
    in_specs = (
        P(("dp", "group"), None),
        P(("dp", "group"), None),
        P(("dp", "group")),
        P(("dp", "group")),
        P("group", None, None),
        P("group", None, None),
        P(),
        P(),
        P("group", None, None),
        P("group", None, None),
        P(),
        P(),
    )
    out_specs = (
        P(("dp", "group"), None),
        P(("dp", "group"), None),
        P("group", None, None),
        P("group", None, None),
        P(),
        P(),
        P("group", None, None),
        P("group", None, None),
        P(),
        P(),
        P("group", None, None),
        P("group", None, None),
        P(),
        P(),
    )
    return jax.shard_map(shards, mesh=mesh, in_specs=in_specs, out_specs=out_specs, check_vma=False)
```

```python
import functools
import math

import jax
import jax.numpy as jnp
import numpy as np
from jax import lax
from jax.experimental import pallas as pl
from jax.experimental.pallas import tpu as pltpu
from jax.sharding import PartitionSpec as P

HIGHEST = lax.Precision.HIGHEST
D = 512
HEADS = 16
HEAD_DIM = 32
WIN = 7
WIN_DEV = 16
TOKW = 49
TABLE_ROWS = 169
MASKED = -1e30
EPSILON = 1e-05
MESH = pl.DeviceIdType.MESH

SLOTS_RUN = 10
TALL = 512
PADR = 528
TAIL0 = 480
TAIL = WIN_DEV * TOKW - TAIL0
SMALL = 40
JR = 56
IR = 64
GH = 8
GC = GH * HEAD_DIM
GL = GH * IR

f32, bf16 = jnp.float32, jnp.bfloat16


def nn(a, b):
    return jnp.dot(a, b, preferred_element_type=f32)


def pair_codes(shape, query_axis, entry_axis):
    i = lax.broadcasted_iota(jnp.int32, shape, query_axis)
    r = lax.broadcasted_iota(jnp.int32, shape, entry_axis)
    return jnp.where(i < TOKW, i + 6 * ((i * 37) >> 8) - r, -1000), i


def exchange_kernel(sq_hbm, wide_hbm, tok_hbm, cot_hbm, counts, regions, table,
                    sq_out, wide_out, tok_out, cot_out, counts_out, regions_out, bias,
                    sq_in, wide_in, sq_low, wide_low, parts, heads_first, sem_in, sem_out, send, recv):
    dp, group = lax.axis_index("dp"), lax.axis_index("group")
    partner = (dp, 1 - group)
    loads = [pltpu.make_async_copy(sq_hbm.at[m], sq_in.at[m], sem_in.at[m]) for m in range(2)]
    loads += [pltpu.make_async_copy(wide_hbm.at[0, pl.ds(128 * c, 128)], wide_in.at[pl.ds(128 * c, 128)], sem_in.at[2 + c])
              for c in range(4)]
    for c in loads:
        c.start()
    barrier = pltpu.get_barrier_semaphore()
    pl.semaphore_signal(barrier, inc=1, device_id=partner, device_id_type=MESH)
    pl.semaphore_wait(barrier, 1)

    def remote(src, dst, k):
        return pltpu.make_async_remote_copy(src_ref=src, dst_ref=dst, send_sem=send.at[k], recv_sem=recv.at[k],
                                            device_id=partner, device_id_type=MESH)

    copies = [remote(counts, counts_out, 6), remote(regions, regions_out, 9),
              remote(tok_hbm.at[pl.ds(TAIL0, TAIL)], tok_out, 7),
              remote(cot_hbm.at[pl.ds(TAIL0, TAIL)], cot_out, 8)]
    for c in copies:
        c.start()
    for m in range(2):
        loads[m].wait()

        def body(k, carry):
            r = pl.multiple_of(k * 32, 32)
            sq_low[m, pl.ds(r, 32)] = sq_in[m, pl.ds(r, 32)].astype(bf16)
            return carry
        lax.fori_loop(0, D // 32, body, 0)
        copies.append(remote(sq_low.at[m], sq_out.at[group, m], m))
        copies[-1].start()
        copies.append(pltpu.make_async_copy(sq_low.at[m], sq_out.at[group, m], sem_out.at[m]))
        copies[-1].start()
    for q in range(4):
        loads[2 + q].wait()

        def body(k, carry):
            r = pl.multiple_of(q * 128 + k * 16, 16)
            wide_low[pl.ds(r, 16)] = wide_in[pl.ds(r, 16)].astype(bf16)
            return carry
        lax.fori_loop(0, 8, body, 0)
        piece = pl.ds(128 * q, 128)
        copies.append(remote(wide_low.at[piece], wide_out.at[group, piece], 2 + q))
        copies[-1].start()
        copies.append(pltpu.make_async_copy(wide_low.at[piece], wide_out.at[group, piece], sem_out.at[2 + q]))
        copies[-1].start()

    heads, entries = table.shape
    parts[...] = jnp.zeros(parts.shape, f32)
    rest = table[...]
    for k in range(3):
        part = rest.astype(bf16).astype(f32)
        parts[pl.ds(heads * k, heads), pl.ds(0, entries)] = part
        rest = rest - part
    heads_first[...] = jnp.zeros(heads_first.shape, f32)
    spot, _ = pair_codes((256, IR), 1, 0)

    def one_key(j, carry):
        hot = (spot == j + 6 * ((j * 37) >> 8) - 84).astype(f32).astype(bf16)
        row = nn(parts[...].astype(bf16), hot)
        row = row[:heads] + row[heads : 2 * heads] + row[2 * heads :]
        heads_first[:, pl.ds(j, 1), :] = row[:, None, :]
        return carry
    lax.fori_loop(0, TOKW, one_key, 0)
    for c in range(heads // 2):
        bias[:, pl.ds(128 * c, 128)] = jnp.concatenate([heads_first[2 * c], heads_first[2 * c + 1]], axis=1)
    for c in copies:
        c.wait()


def exchange(sq, wide, tok, cot, counts, regions, table):
    vmem, any_ = pl.BlockSpec(memory_space=pltpu.VMEM), pl.BlockSpec(memory_space=pl.ANY)
    ff = wide.shape[2]
    return pl.pallas_call(
        exchange_kernel,
        out_shape=(
            jax.ShapeDtypeStruct((2, 2, D, D), bf16),
            jax.ShapeDtypeStruct((2, D, ff), bf16),
            jax.ShapeDtypeStruct((TAIL, D), bf16),
            jax.ShapeDtypeStruct((TAIL, D), bf16),
            jax.ShapeDtypeStruct(counts.shape, jnp.int32),
            jax.ShapeDtypeStruct(regions.shape, jnp.int32),
            jax.ShapeDtypeStruct((JR, HEADS * IR), f32),
        ),
        in_specs=[any_] * 6 + [vmem],
        out_specs=(any_,) * 6 + (vmem,),
        scratch_shapes=[pltpu.VMEM((2, D, D), f32), pltpu.VMEM((D, ff), f32),
                        pltpu.VMEM((2, D, D), bf16), pltpu.VMEM((D, ff), bf16),
                        pltpu.VMEM((3 * HEADS, 256), f32), pltpu.VMEM((HEADS, JR, IR), f32),
                        pltpu.SemaphoreType.DMA((6,)), pltpu.SemaphoreType.DMA((6,)),
                        pltpu.SemaphoreType.DMA((10,)), pltpu.SemaphoreType.DMA((10,))],
        compiler_params=pltpu.CompilerParams(collective_id=0, has_side_effects=True, vmem_limit_bytes=60 * 2**20),
        name="exchange_weights",
    )(sq, wide, tok, cot, counts, regions, table)


def nt(a, b):
    return lax.dot_general(a, b, (((1,), (1,)), ((), ())), preferred_element_type=f32)


def tn(a, b):
    return lax.dot_general(a, b, (((0,), (0,)), ((), ())), preferred_element_type=f32)


def loop_rows(fn, total=TALL, step=64):
    def body(k, carry):
        fn(pl.ds(pl.multiple_of(k * step, step), step))
        return carry
    lax.fori_loop(0, total // step, body, 0)


def block_kernel(count_ref, regions, count_other, regions_other, tok_hbm, cot_hbm, tok_tail_hbm, cot_tail_hbm, sq_hbm, wide_hbm, vec, bias,
                 out_hbm, out_tail_hbm, gtok_hbm, gtok_tail_hbm, grads_hbm, small,
                 tok, cot, tok_tail, cot_tail, sq, wide, out, out_tail, grads, gvec, gtab, sem_in, sem_out,
                 x, e, norm, inv, h1, hT, qkv, mask_bias, probs, o, h2, eb, act, dact, u_s, y, dh, dx, dO, wins, dwin, tail_f, heads_first):
    count = jnp.minimum(count_ref[0], SLOTS_RUN)
    extra = jnp.maximum(count_other[0] - SLOTS_RUN, 0)
    ff = wide.shape[2]
    chunks = ff // D
    scale = HEAD_DIM ** (-0.5)
    loads = [pltpu.make_async_copy(a, b, sem_in.at[k]) for k, (a, b) in enumerate((
        (tok_hbm, tok), (tok_tail_hbm, tok_tail), (sq_hbm, sq), (cot_hbm, cot), (cot_tail_hbm, cot_tail), (wide_hbm, wide)))]
    for c in loads:
        c.start()

    def store(src, dst, k):
        return pltpu.make_async_copy(src, dst, sem_out.at[k])

    stores = []

    def fill(src, src_tail, dst, masked):
        def body(rows, own):
            v = own.astype(f32)
            if masked:
                index = rows.start + lax.broadcasted_iota(jnp.int32, (rows.size, 1), 0)
                v = jnp.where(index < count * TOKW, v, 0.0)
            dst[rows] = v
        loop_rows(lambda rows: body(rows, src[rows]), 512, 64)
        dst[pl.ds(SLOTS_RUN * TOKW, PADR - SLOTS_RUN * TOKW)] = jnp.zeros((PADR - SLOTS_RUN * TOKW, D), f32)
        loop_rows(lambda rows: tail_f.__setitem__(rows, src_tail[rows].astype(f32)), TAIL, 16)

        for k in range(WIN_DEV - SLOTS_RUN):
            @pl.when(k < extra)
            def _():
                dst[pl.ds((SLOTS_RUN - 1 - k) * TOKW, TOKW)] = tail_f[pl.ds(SLOTS_RUN * TOKW - TAIL0 + k * TOKW, TOKW)]

    loads[0].wait()
    loads[1].wait()
    fill(tok, tok_tail, x, False)

    def bias_body(c, carry):
        cs = pl.ds(pl.multiple_of(c * 128, 128), 128)
        j = lax.broadcasted_iota(jnp.int32, (JR, 128), 0)
        i = lax.broadcasted_iota(jnp.int32, (JR, 128), 1) & (IR - 1)
        aj, ai = (j * 37) >> 8, (i * 37) >> 8
        bj, bi = j - 7 * aj, i - 7 * ai
        inside = j < TOKW
        same_row = (aj >= 4) == (ai >= 4)
        same_col = (bj >= 4) == (bi >= 4)
        pad = i >= TOKW
        base = bias[:, cs]
        mask_bias[0, :, cs] = jnp.where(inside, base, MASKED)
        mask_bias[1, :, cs] = jnp.where(inside & (same_col | pad), base, MASKED)
        mask_bias[2, :, cs] = jnp.where(inside & (same_row | pad), base, MASKED)
        mask_bias[3, :, cs] = jnp.where(inside & ((same_row & same_col) | pad), base, MASKED)
        return carry
    lax.fori_loop(0, HEADS * IR // 128, bias_body, 0)

    def norm_rows(src, gain, shift, low, k):
        def body(rows):
            v = src[rows]
            center = v - jnp.mean(v, axis=1, keepdims=True)
            r = lax.rsqrt(jnp.mean(center * center, axis=1, keepdims=True) + EPSILON)
            n = center * r
            norm[k, rows] = n
            inv[k, rows] = jnp.broadcast_to(r, (rows.size, 128))
            low[rows] = (n * gain + shift).astype(bf16)
        loop_rows(body)

    norm_rows(x, vec[0:1], vec[2:3], h1, 0)

    loads[2].wait()
    def project(m, carry):
        shift = jnp.where(m == 0, vec[4:5], jnp.where(m == 2, vec[5:6], jnp.zeros((1, D), f32)))
        qkv[m, pl.ds(0, TALL)] = nn(h1[...], sq[m]) + shift
        return carry
    lax.fori_loop(0, 3, project, 0)
    o[pl.ds(TALL - 24, PADR - TALL + 24)] = jnp.zeros((PADR - TALL + 24, D), f32)
    live_i = lax.broadcasted_iota(jnp.int32, (IR, 1), 0) < TOKW

    def spread_windows(src, dst):
        for w in range(SLOTS_RUN):
            def body(c, carry):
                cs = pl.ds(pl.multiple_of(c * 128, 128), 128)
                dst[pl.ds(w * IR, IR), cs] = jnp.where(live_i, src[pl.ds(w * TOKW, IR), cs], 0.0).astype(bf16)
                return carry
            lax.fori_loop(0, D // 128, body, 0)

    def pack_windows(src, dst):
        for w in range(SLOTS_RUN):
            def body(c, carry):
                cs = pl.ds(pl.multiple_of(c * 128, 128), 128)
                dst[pl.ds(w * TOKW, TOKW), cs] = src[pl.ds(w * IR, TOKW), cs]
                return carry
            lax.fori_loop(0, D // 128, body, 0)

    for m in range(3):
        spread_windows(qkv.at[m], wins.at[m])

    lane_head = lax.broadcasted_iota(jnp.int32, (GH, 1, GC), 2) >> 5
    row_head = lax.broadcasted_iota(jnp.int32, (GH, 1, GC), 0)
    pick = lane_head == row_head
    pick_f = pick.astype(f32)
    pick_b = pick_f.astype(bf16)

    def spread(b):
        return (b[None] * pick_b).reshape(GL, GC)

    def gather(result):
        return jnp.sum(result.reshape(GH, IR, GC) * pick_f, axis=0)

    def place(t):
        w, hg = lax.div(t, 2), lax.rem(t, 2)
        return w, pl.multiple_of(w * IR, IR), pl.ds(pl.multiple_of(hg * GC, 128), GC), pl.ds(pl.multiple_of(hg * GL, 128), GL)

    def kind_of(w):
        own = regions[w * TOKW]
        other = regions_other[jnp.clip(2 * SLOTS_RUN - 1 - w, SLOTS_RUN, WIN_DEV - 1) * TOKW]
        region = jnp.where(w >= SLOTS_RUN - extra, other, own)
        return jnp.where(region == 1, 1, jnp.where(region == 3, 2, jnp.where(region == 4, 3, 0)))

    def attend(t, carry):
        w, row, cs, ls = place(t)
        qd = spread(wins[0, pl.ds(row, IR), cs])
        kb = wins[1, pl.ds(row, JR), cs]
        vb = wins[2, pl.ds(row, JR), cs]
        s = nt(kb, qd) * scale + mask_bias[kind_of(w), :, ls]
        top = jnp.max(s, axis=0, keepdims=True)
        p = jnp.exp(s - top)
        p = p * (1.0 / jnp.sum(p, axis=0, keepdims=True))
        probs[t] = p
        dwin[0, pl.ds(row, IR), cs] = gather(tn(p.astype(bf16), vb))
        return carry
    lax.fori_loop(0, 2 * SLOTS_RUN, attend, 0)

    pack_windows(dwin.at[0], o)

    loads[3].wait()
    loads[4].wait()
    fill(cot, cot_tail, e, True)

    ob = h2
    loop_rows(lambda rows: ob.__setitem__(rows, o[rows].astype(bf16)))
    y[...] = x[pl.ds(0, TALL)] + (nn(ob[...], sq[3]) + vec[6:7])
    hT[0] = o[pl.ds(0, TALL)].T.astype(bf16)
    norm_rows(y, vec[1:2], vec[3:4], h2, 1)
    hT[1] = h2[...].astype(f32).T.astype(bf16)
    hT[2] = e[pl.ds(0, TALL)].T.astype(bf16)
    loop_rows(lambda rows: eb.__setitem__(rows, e[rows].astype(bf16)))
    dh[...] = jnp.zeros((TALL, D), f32)

    def feed(c, carry):
        cs = pl.ds(pl.multiple_of(c * D, 128), D)
        u_s[...] = nn(h2[...], wide[0, :, cs]) + vec[pl.ds(8 + c, 1)]
        dh_c = nn(eb[...], wide[1, :, cs])
        dO[pl.ds(0, TALL)] = dh_c

        def body(rows):
            u = u_s[rows]
            cdf = 0.5 * (1.0 + lax.erf(u * 0.7071067811865476))
            density = jnp.exp(-0.5 * u * u) * 0.3989422804014327
            act[rows] = (u * cdf).astype(bf16)
            dact[rows] = (dO[rows] * (cdf + u * density)).astype(bf16)
        loop_rows(body, TALL, 16)
        y[...] += nt(act[...], wide[1, :, cs])
        dh[...] += nt(dact[...], wide[0, :, cs])
        grads[1, 2 + c] = nn(hT[2], act[...]).astype(bf16)
        grads[0, 2 + c] = nn(hT[1], dact[...]).astype(bf16)
        gvec[pl.ds(8 + c, 1)] = jnp.sum(dact[...].astype(f32), axis=0, keepdims=True)
        return carry
    loads[5].wait()
    lax.fori_loop(0, chunks, feed, 0)
    for g in range(2):
        stores.append(store(grads.at[g, pl.ds(2, chunks)], grads_hbm.at[g, pl.ds(2, chunks)], g))
        stores[-1].start()

    def norm_back(grad, gain, k, add, dst):
        zero = jnp.zeros((1, D), f32)

        def body(i, carry):
            rows = pl.ds(pl.multiple_of(i * 64, 64), 64)
            g_gain, g_shift = carry
            g = grad[rows]
            n = norm[k, rows]
            dn = g * gain
            r = inv[k, rows][:, :1]
            dst[rows] = add[rows] + r * (dn - jnp.mean(dn, axis=1, keepdims=True)
                                         - n * jnp.mean(dn * n, axis=1, keepdims=True))
            return (g_gain + jnp.sum(g * n, axis=0, keepdims=True), g_shift + jnp.sum(g, axis=0, keepdims=True))
        return lax.fori_loop(0, TALL // 64, body, (zero, zero))

    gvec[1:2], gvec[3:4] = norm_back(dh, vec[1:2], 1, e, dx)
    gvec[7:8] = jnp.sum(e[pl.ds(0, TALL)], axis=0, keepdims=True)

    def put(src, dst, dst_tail):
        def own(rows):
            index = rows.start + lax.broadcasted_iota(jnp.int32, (rows.size, 1), 0)
            dst[rows] = jnp.where(index < count * TOKW, src[rows], 0.0).astype(bf16)
        loop_rows(own, 512, 64)
        dst[pl.ds(512, WIN_DEV * TOKW - 512)] = jnp.zeros((WIN_DEV * TOKW - 512, D), bf16)
        tail_f[...] = jnp.zeros((TAIL + 16, D), f32)

        for k in range(WIN_DEV - SLOTS_RUN):
            @pl.when(k < extra)
            def _():
                tail_f[pl.ds(SLOTS_RUN * TOKW - TAIL0 + k * TOKW, TOKW)] = src[pl.ds((SLOTS_RUN - 1 - k) * TOKW, TOKW)]
        loop_rows(lambda rows: dst_tail.__setitem__(rows, tail_f[rows].astype(bf16)), TAIL, 16)

    y[...] += vec[7:8]
    put(y, out, out_tail)
    stores += [store(out, out_hbm, 2), store(out_tail, out_tail_hbm, 3)]
    stores[-2].start()
    stores[-1].start()

    loop_rows(lambda rows: eb.__setitem__(rows, dx[rows].astype(bf16)))
    gvec[6:7] = jnp.sum(eb[...].astype(f32), axis=0, keepdims=True)
    grads[1, 1] = nn(hT[0], eb[...]).astype(bf16)
    dO[pl.ds(0, TALL)] = nt(eb[...], sq[3])
    spread_windows(dO, wins.at[3])
    gtab[...] = jnp.zeros((JR, HEADS * IR), f32)

    def attend_back(t, carry):
        w, row, cs, ls = place(t)
        dd = spread(wins[3, pl.ds(row, IR), cs])
        qd = spread(wins[0, pl.ds(row, IR), cs])
        kb = wins[1, pl.ds(row, JR), cs]
        vb = wins[2, pl.ds(row, JR), cs]
        p = probs[t]
        dp = nt(vb, dd)
        dwin[2, pl.ds(row, JR), cs] = nn(p.astype(bf16), dd)
        ds = p * (dp - jnp.sum(p * dp, axis=0, keepdims=True))
        dsb = ds.astype(bf16)
        gtab[:, ls] += dsb.astype(f32)
        dwin[1, pl.ds(row, JR), cs] = nn(dsb, qd) * scale
        dwin[0, pl.ds(row, IR), cs] = gather(tn(dsb, kb)) * scale
        return carry
    lax.fori_loop(0, 2 * SLOTS_RUN, attend_back, 0)

    for m in range(3):
        qkv[m, pl.ds(TALL - 24, PADR - TALL + 24)] = jnp.zeros((PADR - TALL + 24, D), f32)
        pack_windows(dwin.at[m], qkv.at[m])
    hT[0] = h1[...].astype(f32).T.astype(bf16)
    dh[...] = jnp.zeros((TALL, D), f32)

    def input_grads(m, carry):
        loop_rows(lambda rows: eb.__setitem__(rows, qkv[m, rows].astype(bf16)))
        total = jnp.sum(eb[...].astype(f32), axis=0, keepdims=True)

        @pl.when(m == 0)
        def _():
            gvec[4:5] = total

        @pl.when(m == 2)
        def _():
            gvec[5:6] = total
        dh[...] += nt(eb[...], sq[m])
        grads[lax.div(m, 2), lax.rem(m, 2)] = nn(hT[0], eb[...]).astype(bf16)
        return carry
    lax.fori_loop(0, 3, input_grads, 0)
    gvec[0:1], gvec[2:3] = norm_back(dh, vec[0:1], 0, dx, y)
    stores.append(store(grads.at[0, pl.ds(0, 2)], grads_hbm.at[0, pl.ds(0, 2)], 4))
    stores.append(store(grads.at[1, pl.ds(0, 2)], grads_hbm.at[1, pl.ds(0, 2)], 5))
    stores[-2].start()
    stores[-1].start()
    put(y, cot, cot_tail)
    stores += [store(cot, gtok_hbm, 6), store(cot_tail, gtok_tail_hbm, 7)]
    stores[-2].start()
    stores[-1].start()

    half = small.shape[1]
    for r in range(vec.shape[0]):
        for c in range(D // 128):
            k = r * (D // 128) + c
            small[k // half, pl.ds(k % half, 1)] = gvec[pl.ds(r, 1), pl.ds(128 * c, 128)]
    for h in range(HEADS):
        heads_first[h] = gtab[:, pl.ds(IR * h, IR)]
    spot, _ = pair_codes((IR, 256), 0, 1)

    def diagonal(j, total):
        row = heads_first[:, j]
        high = row.astype(bf16)
        low = (row - high.astype(f32)).astype(bf16)
        hot = (spot == j + 6 * ((j * 37) >> 8) - 84).astype(f32).astype(bf16)
        return total + nn(high, hot) + nn(low, hot)
    table = jnp.zeros((HEADS, 256), f32)
    for j in range(TOKW):
        table = diagonal(j, table)
    first = vec.shape[0] * (D // 128)
    for h in range(HEADS):
        for c in range(2):
            k = first + 2 * h + c
            small[k // half, pl.ds(k % half, 1)] = table[h : h + 1, 128 * c : 128 * c + 128]
    for c in stores:
        c.wait()


def block(count, regions, count_other, regions_other, tok, cot, tok_tail, cot_tail, sq, wide, vec, bias):
    vmem, smem = pl.BlockSpec(memory_space=pltpu.VMEM), pl.BlockSpec(memory_space=pltpu.SMEM)
    any_ = pl.BlockSpec(memory_space=pl.ANY)
    ff = wide.shape[2]
    V = pltpu.VMEM
    shape = jax.ShapeDtypeStruct
    blocks = (2, 2 + ff // D, D, D)
    return pl.pallas_call(
        block_kernel,
        out_shape=(shape(tok.shape, bf16), shape((TAIL, D), bf16), shape(tok.shape, bf16), shape((TAIL, D), bf16),
                   shape(blocks, bf16), shape((2, SMALL, 128), f32)),
        in_specs=[smem] * 4 + [any_] * 6 + [vmem] * 2,
        out_specs=(any_,) * 5 + (vmem,),
        scratch_shapes=[
            V(tok.shape, bf16), V(cot.shape, bf16), V((TAIL, D), bf16), V((TAIL, D), bf16), V((4, D, D), bf16),
            V(wide.shape, bf16), V(tok.shape, bf16), V((TAIL, D), bf16), V(blocks, bf16), V(vec.shape, f32),
            V((JR, HEADS * IR), f32), pltpu.SemaphoreType.DMA((6,)), pltpu.SemaphoreType.DMA((8,)),
            V((PADR, D), f32), V((PADR, D), f32), V((2, TALL, D), f32), V((2, TALL, 128), f32),
            V((TALL, D), bf16), V((3, D, TALL), bf16), V((3, PADR, D), f32), V((4, JR, HEADS * IR), f32),
            V((2 * SLOTS_RUN, JR, GL), f32), V((PADR, D), f32), V((TALL, D), bf16), V((TALL, D), bf16),
            V((TALL, D), bf16), V((TALL, D), bf16), V((TALL, D), f32), V((TALL, D), f32), V((TALL, D), f32),
            V((TALL, D), f32), V((PADR, D), f32), V((4, SLOTS_RUN * IR, D), bf16), V((3, SLOTS_RUN * IR, D), f32),
            V((TAIL + 16, D), f32), V((HEADS, JR, IR), f32),
        ],
        compiler_params=pltpu.CompilerParams(vmem_limit_bytes=60 * 2**20),
        name="window_block",
    )(count, regions, count_other, regions_other, tok, cot, tok_tail, cot_tail, sq.reshape(4, D, D), wide, vec, bias)


BLK = 512
HALF = 6
ORDER = (2, 3, 4, 5, 0, 1)
SMALL = 40


PER = 9


def own_copy(grads_ref, acc, own_sem, group, piece):
    block, rows = ORDER[piece // 2], pl.ds((piece % 2) * (BLK // 2), BLK // 2)
    return pltpu.make_async_copy(grads_ref.at[group, block, rows], acc.at[block, rows], own_sem.at[piece])


def chip_grid(dp):
    side = max(1, math.isqrt(dp // 4))
    if side * side * 4 == dp:
        return (side, side, 4)
    return (1, 1, dp)


class Lane:
    def __init__(self, size, pos, stride, dp, group):
        self.n, self.i, self.stride, self.dp, self.group = size, pos, stride, dp, group

    def peer(self, delta):
        return (self.dp + delta * self.stride, self.group)


class Ids:
    def __init__(self):
        self.count = 0

    def take(self, number=1):
        first = self.count
        self.count += number
        return first


def lanes(sizes):
    dp, group = lax.axis_index("dp"), lax.axis_index("group")
    nx, ny, nz = sizes
    x, y, z = lax.rem(dp, nx), lax.rem(lax.div(dp, nx), ny), lax.div(dp, nx * ny)
    return (
        Lane(nx, x, 1, dp, group),
        Lane(ny, y, nx, dp, group),
        Lane(nz, z, nx * ny, dp, group),
    )


class Plan:
    def __init__(self, sizes, pieces):
        self.orders = ((0, 2, 1), (1, 2, 0))
        self.rs, self.ag, self.agr = Ids(), Ids(), Ids()
        self.rows = 0
        self.slots = {}
        for piece in range(pieces):
            rows = BLK // 2
            for stage, dim in enumerate(self.orders[piece % 2]):
                n = sizes[dim]
                if stage < 2:
                    rows = rows // n
                one = n == 2
                first = self.rs.take(1 if one else 2)
                send = self.ag.take(1 if one else 2)
                land = self.rows
                self.rows += rows * (1 if one else 2 * (n - 1))
                self.slots[piece, stage] = dict(
                    rs={"R": first, "L": first if one else first + 1},
                    land={"R": land, "L": land if one else land + rows * (n - 1)},
                    ag={1: send, -1: send if one else send + 1},
                    agr=self.agr.take(n),
                )


def make_comm(sizes):
    if sizes == (2, 2, 4):
        return make_pairs(sizes)
    pieces = 2 * HALF
    plan = Plan(sizes, pieces)

    def tasks_for(piece, env):
        (lane_all, core_land, acc, out_ref, land_ref, rs_send, rs_recv, ag_send, ag_recv,
         core_send_sem, core_recv_sem, partner, ends, grads_ref, own_sem) = env
        block = ORDER[piece // 2]
        half = BLK // 2
        base = (piece % 2) * half
        dims = [lane_all[d] for d in plan.orders[piece % 2]]
        size = [half // dims[0].n, half // dims[0].n // dims[1].n]
        start1 = base + dims[0].i * size[0]
        start2 = start1 + dims[1].i * size[1]
        cols = BLK // dims[2].n

        def view(stage, j, many=1):
            if stage < 2:
                return pl.multiple_of((base, start1)[stage] + j * size[stage], 16), many * size[stage], 0, BLK
            begin = j * cols if isinstance(j, int) else pl.multiple_of(j * cols, 128)
            return pl.multiple_of(start2, 16), size[1], begin, many * cols

        def landing(stage, way, j, many):
            land = plan.slots[piece, stage]["land"][way]
            n = dims[stage].n
            k = 0 if n == 2 else (j - 1 if way == "R" else j)
            if stage < 2:
                return land + k * size[stage], many * size[stage], 0, BLK
            return land + k * size[1], size[1], 0, many * cols

        def rs_copy(stage, way, j, many):
            slot = plan.slots[piece, stage]
            r, rows, c, width = view(stage, j, many)
            lr, lrows, lc, lwidth = landing(stage, way, j, many)
            return pltpu.make_async_remote_copy(
                src_ref=acc.at[block, pl.ds(r, rows), pl.ds(c, width)],
                dst_ref=land_ref.at[pl.ds(lr, lrows), pl.ds(lc, lwidth)],
                send_sem=rs_send.at[slot["rs"][way]],
                recv_sem=rs_recv.at[slot["rs"][way]],
                device_id=dims[stage].peer(1 if way == "R" else -1),
                device_id_type=MESH,
            )

        def add_landed(stage, way, j, many):
            r, rows, c, width = view(stage, j, many)
            lr, lrows, _, lwidth = landing(stage, way, j, many)
            step = min(rows, 32)

            def body(k, carry):
                here = pl.ds(pl.multiple_of(r + k * step, 16), step)
                there = pl.ds(pl.multiple_of(lr + k * step, 16), step)
                acc[block, here, pl.ds(c, width)] += land_ref[there, pl.ds(0, lwidth)]
                return carry

            if rows == step:
                body(0, 0)
            else:
                lax.fori_loop(0, rows // step, body, 0)

        def parts(stage, first, many):
            if many == 0:
                return []
            if stage < 2:
                return [(first, many)]
            return [(first, many)]

        def rs_tick(stage, h):
            lane = dims[stage]
            n = lane.n

            @pl.when(lane.i == h)
            def _():
                if h > 0:
                    rs_copy(stage, "R", h, n - h).wait_recv()
                if h < n - 1:
                    if h > 0:
                        add_landed(stage, "R", h + 1, n - 1 - h)
                    rs_copy(stage, "R", h + 1, n - 1 - h).start()
                if h > 0:
                    add_landed(stage, "R", h, 1)

            g = n - 1 - h

            @pl.when(lane.i == g)
            def _():
                if h > 0:
                    rs_copy(stage, "L", 0, g + 1).wait_recv()
                if g > 0:
                    if h > 0:
                        add_landed(stage, "L", 0, g)
                    rs_copy(stage, "L", 0, g).start()
                if h > 0:
                    add_landed(stage, "L", g, 1)

        def rs_end(stage):
            lane = dims[stage]
            n = lane.n
            for h in range(n):
                @pl.when(lane.i == h)
                def _():
                    if h < n - 1:
                        rs_copy(stage, "R", h + 1, n - 1 - h).wait_send()
                    if h > 0:
                        rs_copy(stage, "L", 0, h).wait_send()

        def ag_copy(stage, j, way):
            slot = plan.slots[piece, stage]
            r, rows, c, width = view(stage, j)
            piece_ref = out_ref.at[block, pl.ds(r, rows), pl.ds(c, width)]
            return pltpu.make_async_remote_copy(
                src_ref=piece_ref,
                dst_ref=piece_ref,
                send_sem=ag_send.at[slot["ag"][way]],
                recv_sem=ag_recv.at[slot["agr"] + j],
                device_id=dims[stage].peer(way),
                device_id_type=MESH,
            )

        def ag_tick(stage, h):
            lane = dims[stage]
            n, i = lane.n, lane.i
            if h == 0:
                @pl.when(i < n - 1)
                def _():
                    ag_copy(stage, i, 1).start()

                @pl.when(i > 0)
                def _():
                    ag_copy(stage, i, -1).start()
                return

            @pl.when(i >= h)
            def _():
                ag_copy(stage, i - h, -1).wait_recv()

                if n > 2:
                    @pl.when(i < n - 1)
                    def _():
                        ag_copy(stage, i - h + 1, 1).wait_send()
                        ag_copy(stage, i - h, 1).start()

            @pl.when(i + h <= n - 1)
            def _():
                ag_copy(stage, i + h, 1).wait_recv()

                if n > 2:
                    @pl.when(i > 0)
                    def _():
                        ag_copy(stage, i + h - 1, -1).wait_send()
                        ag_copy(stage, i + h, -1).start()

        def ag_end(stage):
            lane = dims[stage]
            n, i = lane.n, lane.i

            @pl.when(i < n - 1)
            def _():
                ag_copy(stage, 0 if n > 2 else i, 1).wait_send()

            @pl.when(i > 0)
            def _():
                ag_copy(stage, n - 1 if n > 2 else i, -1).wait_send()

        def core_copy():
            return pltpu.make_async_remote_copy(
                src_ref=grads_ref.at[1 - partner[2], block, pl.ds(base, half)],
                dst_ref=core_land.at[block, pl.ds(base, half)],
                send_sem=core_send_sem.at[piece],
                recv_sem=core_recv_sem.at[piece],
                device_id=partner[:2],
                device_id_type=MESH,
            )

        def first():
            own_copy(grads_ref, acc, own_sem, partner[2], piece).wait()
            core_copy().wait_recv()

            def body(k, carry):
                r = pl.ds(pl.multiple_of(base + k * 32, 16), 32)
                acc[block, r] += core_land[block, r]
                return carry

            lax.fori_loop(0, half // 32, body, 0)

        def copy_out():
            r, rows, c, width = view(2, dims[2].i)
            out_ref[block, pl.ds(r, rows), pl.ds(c, width)] = acc[block, pl.ds(r, rows), pl.ds(c, width)]

        ticks = [[first]]
        for stage in range(3):
            ticks[-1].append(functools.partial(rs_tick, stage, 0))
            ticks.extend([functools.partial(rs_tick, stage, h)] for h in range(1, dims[stage].n))
        ticks[-1].append(copy_out)
        for stage in (2, 1, 0):
            ticks[-1].append(functools.partial(ag_tick, stage, 0))
            ticks.extend([functools.partial(ag_tick, stage, h)] for h in range(1, dims[stage].n))
        for stage in range(3):
            ends.append(functools.partial(rs_end, stage))
            ends.append(functools.partial(ag_end, stage))
        ends.append(lambda: core_copy().wait_send())
        return core_copy, ticks

    def kernel(grads_ref, small_ref, tail_a, tail_b, out_ref, small_out, back_a, back_b, core_land, acc, land_ref, small_core, small_land,
               rs_send, rs_recv, ag_send, ag_recv, core_s, core_r, sm_cs, sm_cr, sm_s, sm_r, bk_s, bk_r, own_sem, *, delta):
        lane_all = lanes(sizes)
        dp, group = lax.axis_index("dp"), lax.axis_index("group")
        partner = (dp, 1 - group, group)

        for p in range(pieces):
            own_copy(grads_ref, acc, own_sem, group, p).start()
        barrier = pltpu.get_barrier_semaphore()
        total = 1
        pl.semaphore_signal(barrier, inc=1, device_id=partner[:2], device_id_type=MESH)
        for lane in lane_all:
            for k in range(1, lane.n):
                to = lax.rem(lane.i + k, lane.n)
                pl.semaphore_signal(barrier, inc=1, device_id=lane.peer(to - lane.i), device_id_type=MESH)
                total += 1
        pl.semaphore_wait(barrier, total)

        ends = []
        env = (lane_all, core_land, acc, out_ref, land_ref, rs_send, rs_recv, ag_send, ag_recv,
               core_s, core_r, partner, ends, grads_ref, own_sem)

        def sm_core():
            return pltpu.make_async_remote_copy(
                src_ref=small_ref.at[1 - group], dst_ref=small_core, send_sem=sm_cs.at[0], recv_sem=sm_cr.at[0],
                device_id=partner[:2], device_id_type=MESH)

        def sm_back():
            return pltpu.make_async_remote_copy(
                src_ref=small_out.at[group], dst_ref=small_out.at[group], send_sem=sm_cs.at[1], recv_sem=sm_cr.at[1],
                device_id=partner[:2], device_id_type=MESH)

        first_slot = [0, sizes[0], sizes[0] + sizes[1]]

        def sm_copy(d, k):
            lane = lane_all[d]
            to = lax.rem(lane.i + k, lane.n)
            return pltpu.make_async_remote_copy(
                src_ref=small_land.at[first_slot[d] + lane.i],
                dst_ref=small_land.at[first_slot[d] + lane.i],
                send_sem=sm_s.at[first_slot[d] + k],
                recv_sem=sm_r.at[first_slot[d] + lane.i],
                device_id=lane.peer(to - lane.i), device_id_type=MESH)

        def sm_wait(d, k):
            lane = lane_all[d]
            source = lax.rem(lane.i + k, lane.n)
            pltpu.make_async_remote_copy(
                src_ref=small_land.at[first_slot[d] + source],
                dst_ref=small_land.at[first_slot[d] + source],
                send_sem=sm_s.at[first_slot[d] + k],
                recv_sem=sm_r.at[first_slot[d] + source],
                device_id=lane.peer(source - lane.i), device_id_type=MESH).wait_recv()

        def sm_start(d, value):
            lane = lane_all[d]
            small_land[first_slot[d] + lane.i] = value
            for k in range(1, lane.n):
                sm_copy(d, k).start()

        def sm_finish(d):
            lane = lane_all[d]
            for k in range(1, lane.n):
                sm_wait(d, k)
            value = small_land[first_slot[d]]
            for j in range(1, lane.n):
                value = value + small_land[first_slot[d] + j]
            return value

        def sm0():
            sm_core().wait_recv()
            sm_start(0, small_ref[group] + small_core[...])

        def sm1():
            sm_start(1, sm_finish(0))

        def sm2():
            sm_start(2, sm_finish(1))

        def sm3():
            small_out[group] = sm_finish(2)
            sm_back().start()

        def sm4():
            sm_back().wait_recv()

        def back(k):
            return pltpu.make_async_remote_copy(
                src_ref=(tail_a, tail_b)[k], dst_ref=(back_a, back_b)[k], send_sem=bk_s.at[k], recv_sem=bk_r.at[k],
                device_id=partner[:2], device_id_type=MESH)

        sm_core().start()
        made = [tasks_for(p, env) for p in range(pieces)]
        for core_copy, _ in made:
            core_copy().start()
        for k in range(2):
            back(k).start()
        for _, ticks in made:
            for task in ticks[0]:
                task()
        sm0()
        table = {}
        for p, (_, ticks) in enumerate(made):
            for k, tick in enumerate(ticks[1:]):
                table.setdefault(int(delta * (p // 2)) + k, []).append((p, tick))
        for k, task in enumerate((sm1, sm2, sm3, sm4)):
            table.setdefault(2 + 2 * k, []).append((pieces, [task]))
        for when in sorted(table):
            for p, tick in sorted(table[when], key=lambda e: e[0]):
                for task in tick:
                    task()
        for task in ends:
            task()
        for k in range(2):
            back(k).wait()
        sm_core().wait_send()
        sm_back().wait_send()
        for d in range(3):
            for k in range(1, sizes[d]):
                sm_copy(d, k).wait_send()

    def call(grads, small, tail_a, tail_b, delta=1.0):
        dma = pltpu.SemaphoreType.DMA
        vmem = pl.BlockSpec(memory_space=pltpu.VMEM)
        return pl.pallas_call(
            functools.partial(kernel, delta=delta),
            out_shape=(
                jax.ShapeDtypeStruct((HALF, BLK, BLK), jnp.bfloat16),
                jax.ShapeDtypeStruct((2, SMALL, 128), jnp.float32),
                jax.ShapeDtypeStruct(tail_a.shape, tail_a.dtype),
                jax.ShapeDtypeStruct(tail_b.shape, tail_b.dtype),
            ),
            in_specs=[pl.BlockSpec(memory_space=pl.ANY), vmem, pl.BlockSpec(memory_space=pl.ANY), pl.BlockSpec(memory_space=pl.ANY)],
            out_specs=[vmem, vmem, pl.BlockSpec(memory_space=pl.ANY), pl.BlockSpec(memory_space=pl.ANY)],
            scratch_shapes=[
                pltpu.VMEM((HALF, BLK, BLK), jnp.bfloat16),
                pltpu.VMEM((HALF, BLK, BLK), jnp.bfloat16),
                pltpu.VMEM((plan.rows, BLK), jnp.bfloat16),
                pltpu.VMEM((SMALL, 128), jnp.float32),
                pltpu.VMEM((sum(sizes), SMALL, 128), jnp.float32),
                dma((plan.rs.count,)),
                dma((plan.rs.count,)),
                dma((plan.ag.count,)),
                dma((plan.agr.count,)),
                dma((pieces,)),
                dma((pieces,)),
                dma((2,)),
                dma((2,)),
                dma((sum(sizes),)),
                dma((sum(sizes),)),
                dma((2,)),
                dma((2,)),
                dma((pieces,)),
            ],
            compiler_params=pltpu.CompilerParams(
                collective_id=1, has_side_effects=True, vmem_limit_bytes=60 * 2**20
            ),
            name="reduce_gradients",
        )(grads, small, tail_a, tail_b)

    return call


STEPS_END = (
    0, 8, 16, 24, 32, 40, 48, 56, 64, 72, 80, 88, 1, 9, 17, 25, 33, 41, 49, 57, 65, 2, 73, 10, 81, 18, 89, 3,
    26, 11, 34, 19, 4, 42, 27, 12, 50, 35, 20, 58, 66, 43, 28, 51, 74, 36, 82, 59, 67, 44, 90, 75, 52, 83, 60,
    5, 68, 91, 76, 13, 84, 21, 6, 29, 92, 14, 37, 45, 22, 30, 53, 38, 61, 46, 69, 54, 77, 62, 85, 70, 93, 78,
    86, 94,
)
STEPS_INNER = (
    0, 8, 16, 24, 32, 40, 48, 56, 64, 72, 80, 88, 1, 9, 17, 25, 2, 10, 33, 41, 18, 3, 26, 49, 57, 11, 34, 19,
    42, 65, 73, 27, 50, 35, 58, 81, 89, 43, 66, 51, 74, 59, 82, 67, 90, 75, 83, 4, 91, 12, 20, 5, 13, 28, 21,
    36, 44, 6, 14, 29, 52, 22, 37, 60, 45, 68, 30, 53, 76, 61, 38, 84, 69, 46, 92, 54, 77, 85, 62, 70, 93, 78,
    86, 94,
)


def make_pairs(sizes):
    pieces = 2 * HALF
    half, quarter, eighth = BLK // 2 // 2, BLK // 2 // 4, BLK // 2
    land_rows = half + 2 * quarter + quarter

    def steps_for(piece, env):
        (lane_all, core_land, acc, out_ref, land_ref, sends, recvs, partner, grads_ref, own_sem) = env
        block = ORDER[piece // 2]
        base = (piece % 2) * (BLK // 2)
        first_lane, last_lane = (lane_all[0], lane_all[1]) if piece % 2 == 0 else (lane_all[1], lane_all[0])
        z = lane_all[2]
        side = lax.div(z.i, 2)
        onward = 1 - 2 * side
        land = piece * land_rows
        keep = base + first_lane.i * half
        give = base + (1 - first_lane.i) * half
        mine_z, other_z = keep + side * quarter, keep + (1 - side) * quarter
        c_keep, c_give = last_lane.i * eighth, (1 - last_lane.i) * eighth
        all_cols = pl.ds(0, BLK)
        other_x = 1 - 2 * first_lane.i
        other_y = 1 - 2 * last_lane.i

        def rows_of(start, count):
            return pl.ds(pl.multiple_of(start, 16), count)

        def cols_of(start):
            return pl.ds(pl.multiple_of(start, 128), eighth)

        def send(src, dst, k, to, leave=None):
            leave = k if leave is None else leave
            return pltpu.make_async_remote_copy(
                src_ref=src, dst_ref=dst, send_sem=sends.at[piece * PER + leave], recv_sem=recvs.at[piece * PER + k],
                device_id=to, device_id_type=MESH)

        def landing(row, count):
            return land_ref.at[pl.ds(land + row, count)]

        def add(start, count, row):
            def body(k, carry):
                here = rows_of(start + k * 32, 32)
                acc[block, here] += land_ref[pl.ds(pl.multiple_of(land + row + k * 32, 16), 32)]
                return carry
            lax.fori_loop(0, count // 32, body, 0)

        def out_rows(start):
            return out_ref.at[block, rows_of(start, quarter)]

        def r1():
            return send(acc.at[block, rows_of(give, half)], landing(0, half), 0, first_lane.peer(other_x))

        def near():
            return send(acc.at[block, rows_of(other_z, quarter)], landing(half, quarter), 1, z.peer(onward))

        def near_in():
            return send(acc.at[block, rows_of(other_z, quarter)], landing(half, quarter), 1, z.peer(-onward))

        def cross():
            return send(acc.at[block, rows_of(other_z, quarter)], landing(half + quarter, quarter), 2, z.peer(onward), 1)

        def back():
            return send(acc.at[block, rows_of(mine_z, quarter)], landing(half + quarter, quarter), 2, z.peer(-onward))

        def last_half(c):
            return land_ref.at[pl.ds(land + half + 2 * quarter, quarter), pl.ds(0, eighth)]

        def r3():
            return send(acc.at[block, rows_of(mine_z, quarter), cols_of(c_give)], last_half(0), 3, last_lane.peer(other_y))

        def a3(c):
            ref = out_ref.at[block, rows_of(mine_z, quarter), cols_of(c)]
            return send(ref, ref, 4, last_lane.peer(other_y))

        def a_near(to):
            return send(out_rows(mine_z), out_rows(mine_z), 5, z.peer(to))

        def a_cross():
            return send(out_rows(mine_z), out_rows(mine_z), 6, z.peer(onward), 5)

        def a_far_in():
            return send(out_rows(other_z), out_rows(other_z), 6, z.peer(onward))

        def a_back():
            return send(out_rows(other_z), out_rows(other_z), 6, z.peer(-onward))

        def a1(start, k):
            return send(out_rows(start), out_rows(start), k, first_lane.peer(other_x))

        x_mine, x_other = give + side * quarter, give + (1 - side) * quarter

        def core_copy():
            return pltpu.make_async_remote_copy(
                src_ref=grads_ref.at[1 - partner[2], block, pl.ds(base, BLK // 2)],
                dst_ref=core_land.at[block, pl.ds(base, BLK // 2)],
                send_sem=sends.at[PER * pieces + piece], recv_sem=recvs.at[PER * pieces + piece],
                device_id=partner[:2], device_id_type=MESH)

        def begin():
            own_copy(grads_ref, acc, own_sem, partner[2], piece).wait()
            core_copy().wait_recv()

            def body(k, carry):
                r = pl.ds(pl.multiple_of(base + k * 32, 16), 32)
                acc[block, r] += core_land[block, r]
                return carry
            lax.fori_loop(0, BLK // 2 // 32, body, 0)
            r1().start()

        def x_sum():
            r1().wait_recv()
            add(keep, half, 0)

        def x_done():
            a1(x_mine, 7).wait_recv()
            a1(x_other, 8).wait_recv()

        def e1():
            x_sum()
            near().start()

        def e2():
            cross().wait_recv()
            add(mine_z, quarter, half + quarter)
            r3().start()

        def e3():
            r3().wait_recv()
            r, cs = rows_of(mine_z, quarter), cols_of(c_keep)
            out_ref[block, r, cs] = acc[block, r, cs] + last_half(0)[...]
            a3(c_keep).start()

        def e4():
            a3(c_give).wait_recv()
            a_near(onward).start()
            a1(mine_z, 7).start()

        def e5():
            a_far_in().wait_recv()
            a1(other_z, 8).start()

        def i2():
            near_in().wait_recv()
            add(other_z, quarter, half)
            cross().start()

        def i3():
            cross().wait_recv()
            add(mine_z, quarter, half + quarter)
            back().start()

        def i4():
            a_near(-onward).wait_recv()
            a_cross().start()
            a1(mine_z, 7).start()

        def i5():
            a_far_in().wait_recv()
            a_back().start()
            a1(other_z, 8).start()

        ends_sent = (r1, near, r3, lambda: a3(c_keep), lambda: a_near(onward), lambda: a1(mine_z, 7), lambda: a1(other_z, 8), core_copy)
        inner_sent = (r1, cross, back, a_cross, a_back, lambda: a1(mine_z, 7), lambda: a1(other_z, 8), core_copy)
        return (core_copy, (begin, e1, e2, e3, e4, e5, x_done), (begin, x_sum, i2, i3, i4, i5, x_done), ends_sent, inner_sent)

    def kernel(grads_ref, small_ref, tail_a, tail_b, out_ref, small_out, back_a, back_b, core_land, acc, land_ref, small_core, small_land,
               sends, recvs, sm_cs, sm_cr, sm_s, sm_r, bk_s, bk_r, own_sem):
        lane_all = lanes(sizes)
        dp, group = lax.axis_index("dp"), lax.axis_index("group")
        partner = (dp, 1 - group, group)

        for p in range(pieces):
            own_copy(grads_ref, acc, own_sem, group, p).start()
        barrier = pltpu.get_barrier_semaphore()
        total = 1
        pl.semaphore_signal(barrier, inc=1, device_id=partner[:2], device_id_type=MESH)
        for lane in lane_all:
            for k in range(1, lane.n):
                to = lax.rem(lane.i + k, lane.n)
                pl.semaphore_signal(barrier, inc=1, device_id=lane.peer(to - lane.i), device_id_type=MESH)
                total += 1
        pl.semaphore_wait(barrier, total)

        env = (lane_all, core_land, acc, out_ref, land_ref, sends, recvs, partner, grads_ref, own_sem)

        def sm_core():
            return pltpu.make_async_remote_copy(
                src_ref=small_ref.at[1 - group], dst_ref=small_core, send_sem=sm_cs.at[0], recv_sem=sm_cr.at[0],
                device_id=partner[:2], device_id_type=MESH)

        def sm_back():
            return pltpu.make_async_remote_copy(
                src_ref=small_out.at[group], dst_ref=small_out.at[group], send_sem=sm_cs.at[1], recv_sem=sm_cr.at[1],
                device_id=partner[:2], device_id_type=MESH)

        first_slot = [0, sizes[0], sizes[0] + sizes[1]]

        def sm_copy(d, k):
            lane = lane_all[d]
            to = lax.rem(lane.i + k, lane.n)
            return pltpu.make_async_remote_copy(
                src_ref=small_land.at[first_slot[d] + lane.i],
                dst_ref=small_land.at[first_slot[d] + lane.i],
                send_sem=sm_s.at[first_slot[d] + k],
                recv_sem=sm_r.at[first_slot[d] + lane.i],
                device_id=lane.peer(to - lane.i), device_id_type=MESH)

        def sm_wait(d, k):
            lane = lane_all[d]
            source = lax.rem(lane.i + k, lane.n)
            pltpu.make_async_remote_copy(
                src_ref=small_land.at[first_slot[d] + source],
                dst_ref=small_land.at[first_slot[d] + source],
                send_sem=sm_s.at[first_slot[d] + k],
                recv_sem=sm_r.at[first_slot[d] + source],
                device_id=lane.peer(source - lane.i), device_id_type=MESH).wait_recv()

        def sm_start(d, value):
            lane = lane_all[d]
            small_land[first_slot[d] + lane.i] = value
            for k in range(1, lane.n):
                sm_copy(d, k).start()

        def sm_finish(d):
            lane = lane_all[d]
            for k in range(1, lane.n):
                sm_wait(d, k)
            value = small_land[first_slot[d]]
            for j in range(1, lane.n):
                value = value + small_land[first_slot[d] + j]
            return value

        def sm0():
            sm_core().wait_recv()
            sm_start(0, small_ref[group] + small_core[...])

        def sm1():
            sm_start(1, sm_finish(0))

        def sm2():
            sm_start(2, sm_finish(1))

        def sm3():
            small_out[group] = sm_finish(2)
            sm_back().start()

        def sm4():
            sm_back().wait_recv()

        def back(k):
            return pltpu.make_async_remote_copy(
                src_ref=(tail_a, tail_b)[k], dst_ref=(back_a, back_b)[k], send_sem=bk_s.at[k], recv_sem=bk_r.at[k],
                device_id=partner[:2], device_id_type=MESH)

        sm_core().start()
        made = [steps_for(p, env) for p in range(pieces)]
        for steps in made:
            steps[0]().start()
        for k in range(2):
            back(k).start()
        small_steps = (sm0, sm1, sm2, sm3, sm4)

        def run(order, kind):
            every = len(order) // len(small_steps)
            for index, code in enumerate(order):
                made[code // 8][1 + kind][code % 8]()
                if index % every == every - 1 and index // every < len(small_steps):
                    small_steps[index // every]()
            for steps in made:
                for sent in steps[3 + kind]:
                    sent().wait_send()

        z = lane_all[2].i
        at_end = (z == 0) | (z == 3)

        @pl.when(at_end)
        def _():
            run(STEPS_END, 0)

        @pl.when(jnp.logical_not(at_end))
        def _():
            run(STEPS_INNER, 1)

        for k in range(2):
            back(k).wait()
        sm_core().wait_send()
        sm_back().wait_send()
        for d in range(3):
            for k in range(1, sizes[d]):
                sm_copy(d, k).wait_send()

    def call(grads, small, tail_a, tail_b):
        dma = pltpu.SemaphoreType.DMA
        vmem = pl.BlockSpec(memory_space=pltpu.VMEM)
        return pl.pallas_call(
            kernel,
            out_shape=(
                jax.ShapeDtypeStruct((HALF, BLK, BLK), jnp.bfloat16),
                jax.ShapeDtypeStruct((2, SMALL, 128), jnp.float32),
                jax.ShapeDtypeStruct(tail_a.shape, tail_a.dtype),
                jax.ShapeDtypeStruct(tail_b.shape, tail_b.dtype),
            ),
            in_specs=[pl.BlockSpec(memory_space=pl.ANY), vmem, pl.BlockSpec(memory_space=pl.ANY), pl.BlockSpec(memory_space=pl.ANY)],
            out_specs=[vmem, vmem, pl.BlockSpec(memory_space=pl.ANY), pl.BlockSpec(memory_space=pl.ANY)],
            scratch_shapes=[
                pltpu.VMEM((HALF, BLK, BLK), jnp.bfloat16),
                pltpu.VMEM((HALF, BLK, BLK), jnp.bfloat16),
                pltpu.VMEM((pieces * land_rows, BLK), jnp.bfloat16),
                pltpu.VMEM((SMALL, 128), jnp.float32),
                pltpu.VMEM((sum(sizes), SMALL, 128), jnp.float32),
                dma(((PER + 1) * pieces,)),
                dma(((PER + 1) * pieces,)),
                dma((2,)),
                dma((2,)),
                dma((sum(sizes),)),
                dma((sum(sizes),)),
                dma((2,)),
                dma((2,)),
                dma((pieces,)),
            ],
            compiler_params=pltpu.CompilerParams(
                collective_id=1, has_side_effects=True, vmem_limit_bytes=60 * 2**20
            ),
            name="reduce_gradients",
        )(grads, small, tail_a, tail_b)

    return call


MOMENTUM = 0.9
MATRIX_RATE = 0.4
NEWTON_ONE = 3.4445
NEWTON_TWO = -4.775
NEWTON_THREE = 2.0315
STEP = 32
VECTOR_RATE = 0.05
TABLE_RATE = 1.0


def muon_kernel(g_hbm, sw_hbm, ww_hbm, sm_hbm, wm_hbm, row_a, row_b, back_a, back_b,
                small, vec, tab, vec_m, tab_m,
                gs_out, gw_out, ns_out, nw_out, nsm_out, nwm_out, out_a, out_b, gv_out, gt_out, nv_out, nt_out, nvm_out, ntm_out,
                g, sw, ww, sm, wm, gs, gw, xs, xw, gram, mix, own, back, sem_in, sem_out, sem_row, *, slot_root):
    ff = ww.shape[2]
    cols = ff // D

    def load(src, dst, k):
        return pltpu.make_async_copy(src, dst, sem_in.at[k])

    loads = [load(g_hbm.at[pl.ds(0, 2)], g.at[pl.ds(0, 2)], 0), load(sm_hbm, sm, 1),
             load(g_hbm.at[pl.ds(2, cols)], g.at[pl.ds(2, cols)], 2), load(wm_hbm, wm, 3),
             load(sw_hbm, sw, 4), load(ww_hbm, ww, 5)]
    for c in loads:
        c.start()
    first, rows = row_a.shape[0] - back.shape[1], back.shape[1]
    fetch, put = [], []
    for k, (mine, theirs, out) in enumerate(((row_a, back_a, out_a), (row_b, back_b, out_b))):
        fetch.append(pltpu.make_async_copy(mine.at[pl.ds(first, rows)], own.at[k], sem_row.at[k]))
        fetch.append(pltpu.make_async_copy(theirs, back.at[k], sem_row.at[2 + k]))
        put.append(pltpu.make_async_copy(own.at[k], out.at[pl.ds(first, rows)], sem_row.at[4 + k]))
    for c in fetch:
        c.start()
    stores = [pltpu.make_async_copy(a, b, sem_out.at[k]) for k, (a, b) in enumerate(
        ((gs, gs_out), (sm, nsm_out), (gw, gw_out), (wm, nwm_out), (sw, ns_out), (ww, nw_out)))]

    def scan(moment, grad, pick):
        def body(k, total):
            r = pl.multiple_of(k * STEP, STEP)
            new = None
            part = jnp.zeros((STEP, D), jnp.float32)
            for c, block in enumerate(pick):
                cs = pl.ds(c * D, D)
                add = g[block, pl.ds(r, STEP)].astype(jnp.float32)
                grad[pl.ds(r, STEP), cs] = add
                new = MOMENTUM * moment[pl.ds(r, STEP), cs] + add
                moment[pl.ds(r, STEP), cs] = new
                part = part + new * new
            return total + part
        total = lax.fori_loop(0, D // STEP, body, jnp.zeros((STEP, D), jnp.float32))
        return jnp.sum(total)

    def scale(moment, x, total, width):
        size = jnp.sqrt(jnp.full((1, D), total, jnp.float32)) + 1e-07

        def body(k, carry):
            r = pl.multiple_of(k * STEP, STEP)
            for c in range(width // D):
                cs = pl.ds(c * D, D)
                x[pl.ds(r, STEP), cs] = (moment[pl.ds(r, STEP), cs] / size).astype(jnp.bfloat16)
            return carry
        lax.fori_loop(0, D // STEP, body, 0)

    dot_t = functools.partial(lax.dot_general, dimension_numbers=(((1,), (1,)), ((), ())),
                              preferred_element_type=jnp.float32)

    def newton(many, width):
        def body(k, carry):
            for m in range(len(many)):
                x = many[m]
                gram[m] = dot_t(x[...], x[...]).astype(jnp.bfloat16)
            for m in range(len(many)):
                a = gram[m]
                square = jnp.dot(a, a, preferred_element_type=jnp.float32)
                mix[m] = (NEWTON_TWO * a.astype(jnp.float32) + NEWTON_THREE * square).astype(jnp.bfloat16)
            for m in range(len(many)):
                x = many[m]
                for c in range(width // D):
                    cs = pl.ds(c * D, D)
                    old = x[:, cs]
                    x[:, cs] = (NEWTON_ONE * old.astype(jnp.float32)
                                + jnp.dot(mix[m], old, preferred_element_type=jnp.float32)).astype(jnp.bfloat16)
            return carry
        lax.fori_loop(0, 5, body, 0)

    def finish(weight, x, width):
        def body(k, carry):
            r = pl.multiple_of(k * STEP, STEP)
            for c in range(width // D):
                cs = pl.ds(c * D, D)
                weight[pl.ds(r, STEP), cs] = weight[pl.ds(r, STEP), cs] - MATRIX_RATE * x[pl.ds(r, STEP), cs].astype(jnp.float32)
            return carry
        lax.fori_loop(0, D // STEP, body, 0)

    loads[0].wait()
    loads[1].wait()
    for m in range(2):
        total = scan(sm.at[m], gs.at[m], (m,))
        scale(sm.at[m], xs.at[m], total, D)
    stores[0].start()
    stores[1].start()
    loads[2].wait()
    loads[3].wait()
    total = scan(wm.at[0], gw.at[0], tuple(range(2, 2 + cols)))
    scale(wm.at[0], xw, total, ff)
    stores[2].start()
    stores[3].start()
    for c in fetch:
        c.wait()
    for k in range(2):
        def join(i, carry):
            r = pl.ds(pl.multiple_of(i * 16, 16), 16)
            own[k, r] = own[k, r] + back[k, r]
            return carry
        lax.fori_loop(0, rows // 16, join, 0)
        put[k].start()
    half = small.shape[1]

    def small_row(k):
        return small[k // half, pl.ds(k % half, 1)]

    lines = D // 128
    for r in range(vec.shape[0]):
        for c in range(lines):
            gv_out[pl.ds(r, 1), pl.ds(128 * c, 128)] = small_row(r * lines + c)
    nvm_out[...] = MOMENTUM * vec_m[...] + gv_out[...]
    nv_out[...] = vec[...] - (VECTOR_RATE / slot_root) * nvm_out[...]
    first = vec.shape[0] * lines
    heads, entries = tab.shape
    gt_out[:, pl.ds(0, 128)] = jnp.concatenate([small_row(first + 2 * h) for h in range(heads)], axis=0)
    gt_out[:, pl.ds(128, entries - 128)] = jnp.concatenate(
        [small_row(first + 2 * h + 1)[:, : entries - 128] for h in range(heads)], axis=0)
    ntm_out[...] = MOMENTUM * tab_m[...] + gt_out[...]
    nt_out[...] = tab[...] - (TABLE_RATE / slot_root) * ntm_out[...]
    newton([xs.at[0], xs.at[1]], D)
    loads[4].wait()
    for m in range(2):
        finish(sw.at[m], xs.at[m], D)
    stores[4].start()
    newton([xw], ff)
    loads[5].wait()
    finish(ww.at[0], xw, ff)
    stores[5].start()
    for c in stores + put:
        c.wait()


def muon(g, sw, ww, sm, wm, row_a, row_b, back_a, back_b, small, vec, tab, vec_m, tab_m, slots):
    any_, vmem = pl.BlockSpec(memory_space=pl.ANY), pl.BlockSpec(memory_space=pltpu.VMEM)
    slot_root = float(np.sqrt(np.float32(slots)))
    shapes = [sw, ww, sw, ww, sm, wm]
    f32 = jnp.float32
    return pl.pallas_call(
        functools.partial(muon_kernel, slot_root=slot_root),
        out_shape=tuple(jax.ShapeDtypeStruct(a.shape, f32) for a in shapes)
        + tuple(jax.ShapeDtypeStruct(a.shape, a.dtype) for a in (row_a, row_b))
        + tuple(jax.ShapeDtypeStruct(a.shape, f32) for a in (vec, tab, vec, tab, vec, tab)),
        in_specs=[any_] * 9 + [vmem] * 5,
        out_specs=(any_,) * 8 + (vmem,) * 6,
        input_output_aliases={5: 6, 6: 7},
        scratch_shapes=[
            pltpu.VMEM(g.shape, jnp.bfloat16),
            pltpu.VMEM(sw.shape, f32), pltpu.VMEM(ww.shape, f32),
            pltpu.VMEM(sm.shape, f32), pltpu.VMEM(wm.shape, f32),
            pltpu.VMEM(sw.shape, f32), pltpu.VMEM(ww.shape, f32),
            pltpu.VMEM((2, D, D), jnp.bfloat16), pltpu.VMEM((D, ww.shape[2]), jnp.bfloat16),
            pltpu.VMEM((2, D, D), jnp.bfloat16), pltpu.VMEM((2, D, D), jnp.bfloat16),
            pltpu.VMEM((2,) + back_a.shape, jnp.bfloat16), pltpu.VMEM((2,) + back_a.shape, jnp.bfloat16),
            pltpu.SemaphoreType.DMA((6,)), pltpu.SemaphoreType.DMA((6,)), pltpu.SemaphoreType.DMA((6,)),
        ],
        compiler_params=pltpu.CompilerParams(vmem_limit_bytes=58 * 2**20),
        name="muon_step",
    )(g, sw, ww, sm, wm, row_a, row_b, back_a, back_b, small, vec, tab, vec_m, tab_m)


def shards(
    tokens,
    cotangent,
    counts,
    regions,
    square_weights,
    wide_weights,
    vectors,
    bias_table,
    square_moment,
    wide_moment,
    vector_moment,
    table_moment,
):
    table = bias_table.T
    square_low, wide_low, tok_tail, cot_tail, count_other, regions_other, bias = exchange(
        square_weights, wide_weights, tokens, cotangent, counts, regions, table
    )
    out, out_tail, gtok, gtok_tail, grads, small = block(
        counts, regions, count_other, regions_other, tokens, cotangent, tok_tail, cot_tail, square_low, wide_low, vectors, bias
    )
    dp_size, group_size = lax.axis_size("dp"), lax.axis_size("group")
    summed, small_sum, out_back, gtok_back = make_comm(chip_grid(dp_size))(grads, small, out_tail, gtok_tail)
    (
        owned_square,
        owned_wide,
        new_square,
        new_wide,
        new_square_moment,
        new_wide_moment,
        block_out,
        grad_tokens,
        summed_vectors,
        summed_table,
        new_vectors,
        new_table,
        new_vector_moment,
        new_table_moment,
    ) = muon(
        summed,
        square_weights,
        wide_weights,
        square_moment,
        wide_moment,
        out,
        gtok,
        out_back,
        gtok_back,
        small_sum,
        vectors,
        table,
        vector_moment,
        table_moment.T,
        WIN_DEV * dp_size * group_size,
    )
    return (
        block_out,
        grad_tokens,
        owned_square,
        owned_wide,
        summed_vectors,
        summed_table.T,
        new_square,
        new_wide,
        new_vectors,
        new_table.T,
        new_square_moment,
        new_wide_moment,
        new_vector_moment,
        new_table_moment.T,
    )


def solution(mesh):
    in_specs = (
        P(("dp", "group"), None),
        P(("dp", "group"), None),
        P(("dp", "group")),
        P(("dp", "group")),
        P("group", None, None),
        P("group", None, None),
        P(),
        P(),
        P("group", None, None),
        P("group", None, None),
        P(),
        P(),
    )
    out_specs = (
        P(("dp", "group"), None),
        P(("dp", "group"), None),
        P("group", None, None),
        P("group", None, None),
        P(),
        P(),
        P("group", None, None),
        P("group", None, None),
        P(),
        P(),
        P("group", None, None),
        P("group", None, None),
        P(),
        P(),
    )
    return jax.shard_map(shards, mesh=mesh, in_specs=in_specs, out_specs=out_specs, check_vma=False)
```

```python
import functools
import math

import jax
import jax.numpy as jnp
import numpy as np
from jax import lax
from jax.experimental import pallas as pl
from jax.experimental.pallas import tpu as pltpu
from jax.sharding import PartitionSpec as P

HIGHEST = lax.Precision.HIGHEST
D = 512
HEADS = 16
HEAD_DIM = 32
WIN = 7
WIN_DEV = 16
TOKW = 49
TABLE_ROWS = 169
MASKED = -1e30
EPSILON = 1e-05
MESH = pl.DeviceIdType.MESH

SLOTS_RUN = 10
TALL = 512
PADR = 528
TAIL0 = 480
TAIL = WIN_DEV * TOKW - TAIL0
SMALL = 40
JR = 56
IR = 64
GH = 8
GC = GH * HEAD_DIM
GL = GH * IR

f32, bf16 = jnp.float32, jnp.bfloat16


def nn(a, b):
    return jnp.dot(a, b, preferred_element_type=f32)


def pair_codes(shape, query_axis, entry_axis):
    i = lax.broadcasted_iota(jnp.int32, shape, query_axis)
    r = lax.broadcasted_iota(jnp.int32, shape, entry_axis)
    return jnp.where(i < TOKW, i + 6 * ((i * 37) >> 8) - r, -1000), i


def exchange_kernel(sq_hbm, wide_hbm, tok_hbm, cot_hbm, counts, regions, table,
                    sq_out, wide_out, tok_out, cot_out, counts_out, regions_out, bias,
                    sq_in, wide_in, sq_low, wide_low, parts, heads_first, sem_in, sem_out, send, recv):
    dp, group = lax.axis_index("dp"), lax.axis_index("group")
    partner = (dp, 1 - group)
    loads = [pltpu.make_async_copy(sq_hbm.at[m], sq_in.at[m], sem_in.at[m]) for m in range(2)]
    loads += [pltpu.make_async_copy(wide_hbm.at[0, pl.ds(128 * c, 128)], wide_in.at[pl.ds(128 * c, 128)], sem_in.at[2 + c])
              for c in range(4)]
    for c in loads:
        c.start()
    barrier = pltpu.get_barrier_semaphore()
    pl.semaphore_signal(barrier, inc=1, device_id=partner, device_id_type=MESH)
    pl.semaphore_wait(barrier, 1)

    def remote(src, dst, k):
        return pltpu.make_async_remote_copy(src_ref=src, dst_ref=dst, send_sem=send.at[k], recv_sem=recv.at[k],
                                            device_id=partner, device_id_type=MESH)

    copies = [remote(counts, counts_out, 6), remote(regions, regions_out, 9),
              remote(tok_hbm.at[pl.ds(TAIL0, TAIL)], tok_out, 7),
              remote(cot_hbm.at[pl.ds(TAIL0, TAIL)], cot_out, 8)]
    for c in copies:
        c.start()
    for m in range(2):
        loads[m].wait()

        def body(k, carry):
            r = pl.multiple_of(k * 32, 32)
            sq_low[m, pl.ds(r, 32)] = sq_in[m, pl.ds(r, 32)].astype(bf16)
            return carry
        lax.fori_loop(0, D // 32, body, 0)
        copies.append(remote(sq_low.at[m], sq_out.at[group, m], m))
        copies[-1].start()
        copies.append(pltpu.make_async_copy(sq_low.at[m], sq_out.at[group, m], sem_out.at[m]))
        copies[-1].start()
    for q in range(4):
        loads[2 + q].wait()

        def body(k, carry):
            r = pl.multiple_of(q * 128 + k * 16, 16)
            wide_low[pl.ds(r, 16)] = wide_in[pl.ds(r, 16)].astype(bf16)
            return carry
        lax.fori_loop(0, 8, body, 0)
        piece = pl.ds(128 * q, 128)
        copies.append(remote(wide_low.at[piece], wide_out.at[group, piece], 2 + q))
        copies[-1].start()
        copies.append(pltpu.make_async_copy(wide_low.at[piece], wide_out.at[group, piece], sem_out.at[2 + q]))
        copies[-1].start()

    heads, entries = table.shape
    parts[...] = jnp.zeros(parts.shape, f32)
    rest = table[...]
    for k in range(3):
        part = rest.astype(bf16).astype(f32)
        parts[pl.ds(heads * k, heads), pl.ds(0, entries)] = part
        rest = rest - part
    heads_first[...] = jnp.zeros(heads_first.shape, f32)
    spot, _ = pair_codes((256, IR), 1, 0)
    parts_low = parts[...].astype(bf16)

    def one_key(j, carry):
        hot = (spot == j + 6 * ((j * 37) >> 8) - 84).astype(f32).astype(bf16)
        row = nn(parts_low, hot)
        row = row[:heads] + row[heads : 2 * heads] + row[2 * heads :]
        heads_first[:, pl.ds(j, 1), :] = row[:, None, :]
        return carry
    lax.fori_loop(0, TOKW, one_key, 0, unroll=7)
    for c in range(heads // 2):
        bias[:, pl.ds(128 * c, 128)] = jnp.concatenate([heads_first[2 * c], heads_first[2 * c + 1]], axis=1)
    for c in copies:
        c.wait()


def exchange(sq, wide, tok, cot, counts, regions, table):
    vmem, any_ = pl.BlockSpec(memory_space=pltpu.VMEM), pl.BlockSpec(memory_space=pl.ANY)
    ff = wide.shape[2]
    return pl.pallas_call(
        exchange_kernel,
        out_shape=(
            jax.ShapeDtypeStruct((2, 2, D, D), bf16),
            jax.ShapeDtypeStruct((2, D, ff), bf16),
            jax.ShapeDtypeStruct((TAIL, D), bf16),
            jax.ShapeDtypeStruct((TAIL, D), bf16),
            jax.ShapeDtypeStruct(counts.shape, jnp.int32),
            jax.ShapeDtypeStruct(regions.shape, jnp.int32),
            jax.ShapeDtypeStruct((JR, HEADS * IR), f32),
        ),
        in_specs=[any_] * 6 + [vmem],
        out_specs=(any_,) * 6 + (vmem,),
        scratch_shapes=[pltpu.VMEM((2, D, D), f32), pltpu.VMEM((D, ff), f32),
                        pltpu.VMEM((2, D, D), bf16), pltpu.VMEM((D, ff), bf16),
                        pltpu.VMEM((3 * HEADS, 256), f32), pltpu.VMEM((HEADS, JR, IR), f32),
                        pltpu.SemaphoreType.DMA((6,)), pltpu.SemaphoreType.DMA((6,)),
                        pltpu.SemaphoreType.DMA((10,)), pltpu.SemaphoreType.DMA((10,))],
        compiler_params=pltpu.CompilerParams(collective_id=0, has_side_effects=True, vmem_limit_bytes=60 * 2**20),
        name="exchange_weights",
    )(sq, wide, tok, cot, counts, regions, table)


def nt(a, b):
    return lax.dot_general(a, b, (((1,), (1,)), ((), ())), preferred_element_type=f32)


def tn(a, b):
    return lax.dot_general(a, b, (((0,), (0,)), ((), ())), preferred_element_type=f32)


def loop_rows(fn, total=TALL, step=64):
    def body(k, carry):
        fn(pl.ds(pl.multiple_of(k * step, step), step))
        return carry
    lax.fori_loop(0, total // step, body, 0, unroll=4)


def block_kernel(count_ref, regions, count_other, regions_other, tok_hbm, cot_hbm, tok_tail_hbm, cot_tail_hbm, sq_hbm, wide_hbm, vec, bias,
                 out_hbm, out_tail_hbm, gtok_hbm, gtok_tail_hbm, grads_hbm, small,
                 tok, cot, tok_tail, cot_tail, sq, wide, out, out_tail, grads, gvec, gtab, sem_in, sem_out,
                 x, e, norm, inv, h1, hT, qkv, mask_bias, probs, o, h2, eb, act, dact, u_s, y, dh, dx, dO, wins, dwin, tail_f, heads_first):
    count = jnp.minimum(count_ref[0], SLOTS_RUN)
    extra = jnp.maximum(count_other[0] - SLOTS_RUN, 0)
    ff = wide.shape[2]
    chunks = ff // D
    scale = HEAD_DIM ** (-0.5)
    loads = [pltpu.make_async_copy(a, b, sem_in.at[k]) for k, (a, b) in enumerate((
        (tok_hbm, tok), (tok_tail_hbm, tok_tail), (sq_hbm, sq), (cot_hbm, cot), (cot_tail_hbm, cot_tail), (wide_hbm, wide)))]
    for c in loads:
        c.start()

    def store(src, dst, k):
        return pltpu.make_async_copy(src, dst, sem_out.at[k])

    stores = []

    def fill(src, src_tail, dst, masked):
        def body(rows, own):
            v = own.astype(f32)
            if masked:
                index = rows.start + lax.broadcasted_iota(jnp.int32, (rows.size, 1), 0)
                v = jnp.where(index < count * TOKW, v, 0.0)
            dst[rows] = v
        loop_rows(lambda rows: body(rows, src[rows]), 512, 64)
        dst[pl.ds(SLOTS_RUN * TOKW, PADR - SLOTS_RUN * TOKW)] = jnp.zeros((PADR - SLOTS_RUN * TOKW, D), f32)
        loop_rows(lambda rows: tail_f.__setitem__(rows, src_tail[rows].astype(f32)), TAIL, 16)

        for k in range(WIN_DEV - SLOTS_RUN):
            @pl.when(k < extra)
            def _():
                dst[pl.ds((SLOTS_RUN - 1 - k) * TOKW, TOKW)] = tail_f[pl.ds(SLOTS_RUN * TOKW - TAIL0 + k * TOKW, TOKW)]

    loads[0].wait()
    loads[1].wait()
    fill(tok, tok_tail, x, False)

    def bias_body(c, carry):
        cs = pl.ds(pl.multiple_of(c * 128, 128), 128)
        j = lax.broadcasted_iota(jnp.int32, (JR, 128), 0)
        i = lax.broadcasted_iota(jnp.int32, (JR, 128), 1) & (IR - 1)
        aj, ai = (j * 37) >> 8, (i * 37) >> 8
        bj, bi = j - 7 * aj, i - 7 * ai
        inside = j < TOKW
        same_row = (aj >= 4) == (ai >= 4)
        same_col = (bj >= 4) == (bi >= 4)
        pad = i >= TOKW
        base = bias[:, cs]
        mask_bias[0, :, cs] = jnp.where(inside, base, MASKED)
        mask_bias[1, :, cs] = jnp.where(inside & (same_col | pad), base, MASKED)
        mask_bias[2, :, cs] = jnp.where(inside & (same_row | pad), base, MASKED)
        mask_bias[3, :, cs] = jnp.where(inside & ((same_row & same_col) | pad), base, MASKED)
        return carry
    lax.fori_loop(0, HEADS * IR // 128, bias_body, 0)

    def norm_rows(src, gain, shift, low, k):
        def body(rows):
            v = src[rows]
            center = v - jnp.mean(v, axis=1, keepdims=True)
            r = lax.rsqrt(jnp.mean(center * center, axis=1, keepdims=True) + EPSILON)
            n = center * r
            norm[k, rows] = n
            inv[k, rows] = jnp.broadcast_to(r, (rows.size, 128))
            low[rows] = (n * gain + shift).astype(bf16)
        loop_rows(body)

    norm_rows(x, vec[0:1], vec[2:3], h1, 0)

    loads[2].wait()
    def project(m, carry):
        shift = jnp.where(m == 0, vec[4:5], jnp.where(m == 2, vec[5:6], jnp.zeros((1, D), f32)))
        qkv[m, pl.ds(0, TALL)] = nn(h1[...], sq[m]) + shift
        return carry
    lax.fori_loop(0, 3, project, 0)
    o[pl.ds(TALL - 24, PADR - TALL + 24)] = jnp.zeros((PADR - TALL + 24, D), f32)
    live_i = lax.broadcasted_iota(jnp.int32, (IR, 1), 0) < TOKW

    def spread_windows(src, dst):
        def body(c, carry):
            cs = pl.ds(pl.multiple_of(c * 128, 128), 128)
            for w in range(SLOTS_RUN):
                dst[pl.ds(w * IR, IR), cs] = jnp.where(live_i, src[pl.ds(w * TOKW, IR), cs], 0.0).astype(bf16)
            return carry
        lax.fori_loop(0, D // 128, body, 0)

    def pack_windows(src, dst):
        def body(c, carry):
            cs = pl.ds(pl.multiple_of(c * 128, 128), 128)
            for w in range(SLOTS_RUN):
                dst[pl.ds(w * TOKW, TOKW), cs] = src[pl.ds(w * IR, TOKW), cs]
            return carry
        lax.fori_loop(0, D // 128, body, 0)

    for m in range(3):
        spread_windows(qkv.at[m], wins.at[m])

    lane_head = lax.broadcasted_iota(jnp.int32, (GH, 1, GC), 2) >> 5
    row_head = lax.broadcasted_iota(jnp.int32, (GH, 1, GC), 0)
    pick = lane_head == row_head
    pick_f = pick.astype(f32)
    pick_b = pick_f.astype(bf16)

    def spread(b):
        return (b[None] * pick_b).reshape(GL, GC)

    def gather(result):
        return jnp.sum(result.reshape(GH, IR, GC) * pick_f, axis=0)

    def place(t):
        w, hg = lax.div(t, 2), lax.rem(t, 2)
        return w, pl.multiple_of(w * IR, IR), pl.ds(pl.multiple_of(hg * GC, 128), GC), pl.ds(pl.multiple_of(hg * GL, 128), GL)

    def kind_of(w):
        own = regions[w * TOKW]
        other = regions_other[jnp.clip(2 * SLOTS_RUN - 1 - w, SLOTS_RUN, WIN_DEV - 1) * TOKW]
        region = jnp.where(w >= SLOTS_RUN - extra, other, own)
        return jnp.where(region == 1, 1, jnp.where(region == 3, 2, jnp.where(region == 4, 3, 0)))

    def attend(t, carry):
        w, row, cs, ls = place(t)
        qd = spread(wins[0, pl.ds(row, IR), cs])
        kb = wins[1, pl.ds(row, JR), cs]
        vb = wins[2, pl.ds(row, JR), cs]
        s = nt(kb, qd) * scale + mask_bias[kind_of(w), :, ls]
        top = jnp.max(s, axis=0, keepdims=True)
        p = jnp.exp(s - top)
        p = p * (1.0 / jnp.sum(p, axis=0, keepdims=True))
        probs[t] = p
        dwin[0, pl.ds(row, IR), cs] = gather(tn(p.astype(bf16), vb))
        return carry
    lax.fori_loop(0, 2 * SLOTS_RUN, attend, 0, unroll=10)

    pack_windows(dwin.at[0], o)

    loads[3].wait()
    loads[4].wait()
    fill(cot, cot_tail, e, True)

    ob = h2
    loop_rows(lambda rows: ob.__setitem__(rows, o[rows].astype(bf16)))
    y[...] = x[pl.ds(0, TALL)] + (nn(ob[...], sq[3]) + vec[6:7])
    hT[0] = o[pl.ds(0, TALL)].T.astype(bf16)
    norm_rows(y, vec[1:2], vec[3:4], h2, 1)
    hT[1] = h2[...].astype(f32).T.astype(bf16)
    hT[2] = e[pl.ds(0, TALL)].T.astype(bf16)
    loop_rows(lambda rows: eb.__setitem__(rows, e[rows].astype(bf16)))
    dh[...] = jnp.zeros((TALL, D), f32)

    def feed(c, carry):
        cs = pl.ds(pl.multiple_of(c * D, 128), D)
        u_s[...] = nn(h2[...], wide[0, :, cs]) + vec[pl.ds(8 + c, 1)]
        dh_c = nn(eb[...], wide[1, :, cs])
        dO[pl.ds(0, TALL)] = dh_c

        def body(rows):
            u = u_s[rows]
            cdf = 0.5 * (1.0 + lax.erf(u * 0.7071067811865476))
            density = jnp.exp(-0.5 * u * u) * 0.3989422804014327
            act[rows] = (u * cdf).astype(bf16)
            dact[rows] = (dO[rows] * (cdf + u * density)).astype(bf16)
        loop_rows(body, TALL, 64)
        y[...] += nt(act[...], wide[1, :, cs])
        dh[...] += nt(dact[...], wide[0, :, cs])
        grads[1, 2 + c] = nn(hT[2], act[...]).astype(bf16)
        grads[0, 2 + c] = nn(hT[1], dact[...]).astype(bf16)
        gvec[pl.ds(8 + c, 1)] = jnp.sum(dact[...].astype(f32), axis=0, keepdims=True)
        return carry
    loads[5].wait()
    lax.fori_loop(0, chunks, feed, 0)
    for g in range(2):
        stores.append(store(grads.at[g, pl.ds(2, chunks)], grads_hbm.at[g, pl.ds(2, chunks)], g))
        stores[-1].start()

    def norm_back(grad, gain, k, add, dst):
        zero = jnp.zeros((1, D), f32)

        def body(i, carry):
            rows = pl.ds(pl.multiple_of(i * 64, 64), 64)
            g_gain, g_shift = carry
            g = grad[rows]
            n = norm[k, rows]
            dn = g * gain
            r = inv[k, rows][:, :1]
            dst[rows] = add[rows] + r * (dn - jnp.mean(dn, axis=1, keepdims=True)
                                         - n * jnp.mean(dn * n, axis=1, keepdims=True))
            return (g_gain + jnp.sum(g * n, axis=0, keepdims=True), g_shift + jnp.sum(g, axis=0, keepdims=True))
        return lax.fori_loop(0, TALL // 64, body, (zero, zero), unroll=2)

    gvec[1:2], gvec[3:4] = norm_back(dh, vec[1:2], 1, e, dx)
    gvec[7:8] = jnp.sum(e[pl.ds(0, TALL)], axis=0, keepdims=True)

    def put(src, dst, dst_tail):
        def own(rows):
            index = rows.start + lax.broadcasted_iota(jnp.int32, (rows.size, 1), 0)
            dst[rows] = jnp.where(index < count * TOKW, src[rows], 0.0).astype(bf16)
        loop_rows(own, 512, 64)
        dst[pl.ds(512, WIN_DEV * TOKW - 512)] = jnp.zeros((WIN_DEV * TOKW - 512, D), bf16)
        tail_f[...] = jnp.zeros((TAIL + 16, D), f32)

        for k in range(WIN_DEV - SLOTS_RUN):
            @pl.when(k < extra)
            def _():
                tail_f[pl.ds(SLOTS_RUN * TOKW - TAIL0 + k * TOKW, TOKW)] = src[pl.ds((SLOTS_RUN - 1 - k) * TOKW, TOKW)]
        loop_rows(lambda rows: dst_tail.__setitem__(rows, tail_f[rows].astype(bf16)), TAIL, 16)

    y[...] += vec[7:8]
    put(y, out, out_tail)
    stores += [store(out, out_hbm, 2), store(out_tail, out_tail_hbm, 3)]
    stores[-2].start()
    stores[-1].start()

    loop_rows(lambda rows: eb.__setitem__(rows, dx[rows].astype(bf16)))
    gvec[6:7] = jnp.sum(eb[...].astype(f32), axis=0, keepdims=True)
    grads[1, 1] = nn(hT[0], eb[...]).astype(bf16)
    dO[pl.ds(0, TALL)] = nt(eb[...], sq[3])
    spread_windows(dO, wins.at[3])
    gtab[...] = jnp.zeros((JR, HEADS * IR), f32)

    def attend_back(t, carry):
        w, row, cs, ls = place(t)
        dd = spread(wins[3, pl.ds(row, IR), cs])
        qd = spread(wins[0, pl.ds(row, IR), cs])
        kb = wins[1, pl.ds(row, JR), cs]
        vb = wins[2, pl.ds(row, JR), cs]
        p = probs[t]
        dp = nt(vb, dd)
        dwin[2, pl.ds(row, JR), cs] = nn(p.astype(bf16), dd)
        ds = p * (dp - jnp.sum(p * dp, axis=0, keepdims=True))
        dsb = ds.astype(bf16)
        gtab[:, ls] += dsb.astype(f32)
        dwin[1, pl.ds(row, JR), cs] = nn(dsb, qd) * scale
        dwin[0, pl.ds(row, IR), cs] = gather(tn(dsb, kb)) * scale
        return carry
    lax.fori_loop(0, 2 * SLOTS_RUN, attend_back, 0, unroll=10)

    for m in range(3):
        qkv[m, pl.ds(TALL - 24, PADR - TALL + 24)] = jnp.zeros((PADR - TALL + 24, D), f32)
        pack_windows(dwin.at[m], qkv.at[m])
    hT[0] = h1[...].astype(f32).T.astype(bf16)
    dh[...] = jnp.zeros((TALL, D), f32)

    def input_grads(m, carry):
        loop_rows(lambda rows: eb.__setitem__(rows, qkv[m, rows].astype(bf16)))
        total = jnp.sum(eb[...].astype(f32), axis=0, keepdims=True)

        @pl.when(m == 0)
        def _():
            gvec[4:5] = total

        @pl.when(m == 2)
        def _():
            gvec[5:6] = total
        dh[...] += nt(eb[...], sq[m])
        grads[lax.div(m, 2), lax.rem(m, 2)] = nn(hT[0], eb[...]).astype(bf16)
        return carry
    lax.fori_loop(0, 3, input_grads, 0)
    gvec[0:1], gvec[2:3] = norm_back(dh, vec[0:1], 0, dx, y)
    stores.append(store(grads.at[0, pl.ds(0, 2)], grads_hbm.at[0, pl.ds(0, 2)], 4))
    stores.append(store(grads.at[1, pl.ds(0, 2)], grads_hbm.at[1, pl.ds(0, 2)], 5))
    stores[-2].start()
    stores[-1].start()
    put(y, cot, cot_tail)
    stores += [store(cot, gtok_hbm, 6), store(cot_tail, gtok_tail_hbm, 7)]
    stores[-2].start()
    stores[-1].start()

    half = small.shape[1]
    for r in range(vec.shape[0]):
        for c in range(D // 128):
            k = r * (D // 128) + c
            small[k // half, pl.ds(k % half, 1)] = gvec[pl.ds(r, 1), pl.ds(128 * c, 128)]
    for h in range(HEADS):
        heads_first[h] = gtab[:, pl.ds(IR * h, IR)]
    spot, _ = pair_codes((IR, 256), 0, 1)

    def diagonal(j, total):
        row = heads_first[:, j]
        high = row.astype(bf16)
        low = (row - high.astype(f32)).astype(bf16)
        hot = (spot == j + 6 * ((j * 37) >> 8) - 84).astype(f32).astype(bf16)
        return total + nn(high, hot) + nn(low, hot)
    table = jnp.zeros((HEADS, 256), f32)
    for j in range(TOKW):
        table = diagonal(j, table)
    first = vec.shape[0] * (D // 128)
    for h in range(HEADS):
        for c in range(2):
            k = first + 2 * h + c
            small[k // half, pl.ds(k % half, 1)] = table[h : h + 1, 128 * c : 128 * c + 128]
    for c in stores:
        c.wait()


def block(count, regions, count_other, regions_other, tok, cot, tok_tail, cot_tail, sq, wide, vec, bias):
    vmem, smem = pl.BlockSpec(memory_space=pltpu.VMEM), pl.BlockSpec(memory_space=pltpu.SMEM)
    any_ = pl.BlockSpec(memory_space=pl.ANY)
    ff = wide.shape[2]
    V = pltpu.VMEM
    shape = jax.ShapeDtypeStruct
    blocks = (2, 2 + ff // D, D, D)
    return pl.pallas_call(
        block_kernel,
        out_shape=(shape(tok.shape, bf16), shape((TAIL, D), bf16), shape(tok.shape, bf16), shape((TAIL, D), bf16),
                   shape(blocks, bf16), shape((2, SMALL, 128), f32)),
        in_specs=[smem] * 4 + [any_] * 6 + [vmem] * 2,
        out_specs=(any_,) * 5 + (vmem,),
        scratch_shapes=[
            V(tok.shape, bf16), V(cot.shape, bf16), V((TAIL, D), bf16), V((TAIL, D), bf16), V((4, D, D), bf16),
            V(wide.shape, bf16), V(tok.shape, bf16), V((TAIL, D), bf16), V(blocks, bf16), V(vec.shape, f32),
            V((JR, HEADS * IR), f32), pltpu.SemaphoreType.DMA((6,)), pltpu.SemaphoreType.DMA((8,)),
            V((PADR, D), f32), V((PADR, D), f32), V((2, TALL, D), f32), V((2, TALL, 128), f32),
            V((TALL, D), bf16), V((3, D, TALL), bf16), V((3, PADR, D), f32), V((4, JR, HEADS * IR), f32),
            V((2 * SLOTS_RUN, JR, GL), f32), V((PADR, D), f32), V((TALL, D), bf16), V((TALL, D), bf16),
            V((TALL, D), bf16), V((TALL, D), bf16), V((TALL, D), f32), V((TALL, D), f32), V((TALL, D), f32),
            V((TALL, D), f32), V((PADR, D), f32), V((4, SLOTS_RUN * IR, D), bf16), V((3, SLOTS_RUN * IR, D), f32),
            V((TAIL + 16, D), f32), V((HEADS, JR, IR), f32),
        ],
        compiler_params=pltpu.CompilerParams(vmem_limit_bytes=60 * 2**20),
        name="window_block",
    )(count, regions, count_other, regions_other, tok, cot, tok_tail, cot_tail, sq.reshape(4, D, D), wide, vec, bias)


BLK = 512
HALF = 6
ORDER = (2, 3, 4, 5, 0, 1)
SMALL = 40


PER = 9


def own_copy(grads_ref, acc, own_sem, group, piece):
    block, rows = ORDER[piece // 2], pl.ds((piece % 2) * (BLK // 2), BLK // 2)
    return pltpu.make_async_copy(grads_ref.at[group, block, rows], acc.at[block, rows], own_sem.at[piece])


def chip_grid(dp):
    side = max(1, math.isqrt(dp // 4))
    if side * side * 4 == dp:
        return (side, side, 4)
    return (1, 1, dp)


class Lane:
    def __init__(self, size, pos, stride, dp, group):
        self.n, self.i, self.stride, self.dp, self.group = size, pos, stride, dp, group

    def peer(self, delta):
        return (self.dp + delta * self.stride, self.group)


class Ids:
    def __init__(self):
        self.count = 0

    def take(self, number=1):
        first = self.count
        self.count += number
        return first


def lanes(sizes):
    dp, group = lax.axis_index("dp"), lax.axis_index("group")
    nx, ny, nz = sizes
    x, y, z = lax.rem(dp, nx), lax.rem(lax.div(dp, nx), ny), lax.div(dp, nx * ny)
    return (
        Lane(nx, x, 1, dp, group),
        Lane(ny, y, nx, dp, group),
        Lane(nz, z, nx * ny, dp, group),
    )


class Plan:
    def __init__(self, sizes, pieces):
        self.orders = ((0, 2, 1), (1, 2, 0))
        self.rs, self.ag, self.agr = Ids(), Ids(), Ids()
        self.rows = 0
        self.slots = {}
        for piece in range(pieces):
            rows = BLK // 2
            for stage, dim in enumerate(self.orders[piece % 2]):
                n = sizes[dim]
                if stage < 2:
                    rows = rows // n
                one = n == 2
                first = self.rs.take(1 if one else 2)
                send = self.ag.take(1 if one else 2)
                land = self.rows
                self.rows += rows * (1 if one else 2 * (n - 1))
                self.slots[piece, stage] = dict(
                    rs={"R": first, "L": first if one else first + 1},
                    land={"R": land, "L": land if one else land + rows * (n - 1)},
                    ag={1: send, -1: send if one else send + 1},
                    agr=self.agr.take(n),
                )


def make_comm(sizes):
    if sizes == (2, 2, 4):
        return make_pairs(sizes)
    pieces = 2 * HALF
    plan = Plan(sizes, pieces)

    def tasks_for(piece, env):
        (lane_all, core_land, acc, out_ref, land_ref, rs_send, rs_recv, ag_send, ag_recv,
         core_send_sem, core_recv_sem, partner, ends, grads_ref, own_sem) = env
        block = ORDER[piece // 2]
        half = BLK // 2
        base = (piece % 2) * half
        dims = [lane_all[d] for d in plan.orders[piece % 2]]
        size = [half // dims[0].n, half // dims[0].n // dims[1].n]
        start1 = base + dims[0].i * size[0]
        start2 = start1 + dims[1].i * size[1]
        cols = BLK // dims[2].n

        def view(stage, j, many=1):
            if stage < 2:
                return pl.multiple_of((base, start1)[stage] + j * size[stage], 16), many * size[stage], 0, BLK
            begin = j * cols if isinstance(j, int) else pl.multiple_of(j * cols, 128)
            return pl.multiple_of(start2, 16), size[1], begin, many * cols

        def landing(stage, way, j, many):
            land = plan.slots[piece, stage]["land"][way]
            n = dims[stage].n
            k = 0 if n == 2 else (j - 1 if way == "R" else j)
            if stage < 2:
                return land + k * size[stage], many * size[stage], 0, BLK
            return land + k * size[1], size[1], 0, many * cols

        def rs_copy(stage, way, j, many):
            slot = plan.slots[piece, stage]
            r, rows, c, width = view(stage, j, many)
            lr, lrows, lc, lwidth = landing(stage, way, j, many)
            return pltpu.make_async_remote_copy(
                src_ref=acc.at[block, pl.ds(r, rows), pl.ds(c, width)],
                dst_ref=land_ref.at[pl.ds(lr, lrows), pl.ds(lc, lwidth)],
                send_sem=rs_send.at[slot["rs"][way]],
                recv_sem=rs_recv.at[slot["rs"][way]],
                device_id=dims[stage].peer(1 if way == "R" else -1),
                device_id_type=MESH,
            )

        def add_landed(stage, way, j, many):
            r, rows, c, width = view(stage, j, many)
            lr, lrows, _, lwidth = landing(stage, way, j, many)
            step = min(rows, 32)

            def body(k, carry):
                here = pl.ds(pl.multiple_of(r + k * step, 16), step)
                there = pl.ds(pl.multiple_of(lr + k * step, 16), step)
                acc[block, here, pl.ds(c, width)] += land_ref[there, pl.ds(0, lwidth)]
                return carry

            if rows == step:
                body(0, 0)
            else:
                lax.fori_loop(0, rows // step, body, 0)

        def parts(stage, first, many):
            if many == 0:
                return []
            if stage < 2:
                return [(first, many)]
            return [(first, many)]

        def rs_tick(stage, h):
            lane = dims[stage]
            n = lane.n

            @pl.when(lane.i == h)
            def _():
                if h > 0:
                    rs_copy(stage, "R", h, n - h).wait_recv()
                if h < n - 1:
                    if h > 0:
                        add_landed(stage, "R", h + 1, n - 1 - h)
                    rs_copy(stage, "R", h + 1, n - 1 - h).start()
                if h > 0:
                    add_landed(stage, "R", h, 1)

            g = n - 1 - h

            @pl.when(lane.i == g)
            def _():
                if h > 0:
                    rs_copy(stage, "L", 0, g + 1).wait_recv()
                if g > 0:
                    if h > 0:
                        add_landed(stage, "L", 0, g)
                    rs_copy(stage, "L", 0, g).start()
                if h > 0:
                    add_landed(stage, "L", g, 1)

        def rs_end(stage):
            lane = dims[stage]
            n = lane.n
            for h in range(n):
                @pl.when(lane.i == h)
                def _():
                    if h < n - 1:
                        rs_copy(stage, "R", h + 1, n - 1 - h).wait_send()
                    if h > 0:
                        rs_copy(stage, "L", 0, h).wait_send()

        def ag_copy(stage, j, way):
            slot = plan.slots[piece, stage]
            r, rows, c, width = view(stage, j)
            piece_ref = out_ref.at[block, pl.ds(r, rows), pl.ds(c, width)]
            return pltpu.make_async_remote_copy(
                src_ref=piece_ref,
                dst_ref=piece_ref,
                send_sem=ag_send.at[slot["ag"][way]],
                recv_sem=ag_recv.at[slot["agr"] + j],
                device_id=dims[stage].peer(way),
                device_id_type=MESH,
            )

        def ag_tick(stage, h):
            lane = dims[stage]
            n, i = lane.n, lane.i
            if h == 0:
                @pl.when(i < n - 1)
                def _():
                    ag_copy(stage, i, 1).start()

                @pl.when(i > 0)
                def _():
                    ag_copy(stage, i, -1).start()
                return

            @pl.when(i >= h)
            def _():
                ag_copy(stage, i - h, -1).wait_recv()

                if n > 2:
                    @pl.when(i < n - 1)
                    def _():
                        ag_copy(stage, i - h + 1, 1).wait_send()
                        ag_copy(stage, i - h, 1).start()

            @pl.when(i + h <= n - 1)
            def _():
                ag_copy(stage, i + h, 1).wait_recv()

                if n > 2:
                    @pl.when(i > 0)
                    def _():
                        ag_copy(stage, i + h - 1, -1).wait_send()
                        ag_copy(stage, i + h, -1).start()

        def ag_end(stage):
            lane = dims[stage]
            n, i = lane.n, lane.i

            @pl.when(i < n - 1)
            def _():
                ag_copy(stage, 0 if n > 2 else i, 1).wait_send()

            @pl.when(i > 0)
            def _():
                ag_copy(stage, n - 1 if n > 2 else i, -1).wait_send()

        def core_copy():
            return pltpu.make_async_remote_copy(
                src_ref=grads_ref.at[1 - partner[2], block, pl.ds(base, half)],
                dst_ref=core_land.at[block, pl.ds(base, half)],
                send_sem=core_send_sem.at[piece],
                recv_sem=core_recv_sem.at[piece],
                device_id=partner[:2],
                device_id_type=MESH,
            )

        def first():
            own_copy(grads_ref, acc, own_sem, partner[2], piece).wait()
            core_copy().wait_recv()

            def body(k, carry):
                r = pl.ds(pl.multiple_of(base + k * 32, 16), 32)
                acc[block, r] += core_land[block, r]
                return carry

            lax.fori_loop(0, half // 32, body, 0)

        def copy_out():
            r, rows, c, width = view(2, dims[2].i)
            out_ref[block, pl.ds(r, rows), pl.ds(c, width)] = acc[block, pl.ds(r, rows), pl.ds(c, width)]

        ticks = [[first]]
        for stage in range(3):
            ticks[-1].append(functools.partial(rs_tick, stage, 0))
            ticks.extend([functools.partial(rs_tick, stage, h)] for h in range(1, dims[stage].n))
        ticks[-1].append(copy_out)
        for stage in (2, 1, 0):
            ticks[-1].append(functools.partial(ag_tick, stage, 0))
            ticks.extend([functools.partial(ag_tick, stage, h)] for h in range(1, dims[stage].n))
        for stage in range(3):
            ends.append(functools.partial(rs_end, stage))
            ends.append(functools.partial(ag_end, stage))
        ends.append(lambda: core_copy().wait_send())
        return core_copy, ticks

    def kernel(grads_ref, small_ref, tail_a, tail_b, out_ref, small_out, back_a, back_b, core_land, acc, land_ref, small_core, small_land,
               rs_send, rs_recv, ag_send, ag_recv, core_s, core_r, sm_cs, sm_cr, sm_s, sm_r, bk_s, bk_r, own_sem, *, delta):
        lane_all = lanes(sizes)
        dp, group = lax.axis_index("dp"), lax.axis_index("group")
        partner = (dp, 1 - group, group)

        for p in range(pieces):
            own_copy(grads_ref, acc, own_sem, group, p).start()
        barrier = pltpu.get_barrier_semaphore()
        total = 1
        pl.semaphore_signal(barrier, inc=1, device_id=partner[:2], device_id_type=MESH)
        for lane in lane_all:
            for k in range(1, lane.n):
                to = lax.rem(lane.i + k, lane.n)
                pl.semaphore_signal(barrier, inc=1, device_id=lane.peer(to - lane.i), device_id_type=MESH)
                total += 1
        pl.semaphore_wait(barrier, total)

        ends = []
        env = (lane_all, core_land, acc, out_ref, land_ref, rs_send, rs_recv, ag_send, ag_recv,
               core_s, core_r, partner, ends, grads_ref, own_sem)

        def sm_core():
            return pltpu.make_async_remote_copy(
                src_ref=small_ref.at[1 - group], dst_ref=small_core, send_sem=sm_cs.at[0], recv_sem=sm_cr.at[0],
                device_id=partner[:2], device_id_type=MESH)

        def sm_back():
            return pltpu.make_async_remote_copy(
                src_ref=small_out.at[group], dst_ref=small_out.at[group], send_sem=sm_cs.at[1], recv_sem=sm_cr.at[1],
                device_id=partner[:2], device_id_type=MESH)

        first_slot = [0, sizes[0], sizes[0] + sizes[1]]

        def sm_copy(d, k):
            lane = lane_all[d]
            to = lax.rem(lane.i + k, lane.n)
            return pltpu.make_async_remote_copy(
                src_ref=small_land.at[first_slot[d] + lane.i],
                dst_ref=small_land.at[first_slot[d] + lane.i],
                send_sem=sm_s.at[first_slot[d] + k],
                recv_sem=sm_r.at[first_slot[d] + lane.i],
                device_id=lane.peer(to - lane.i), device_id_type=MESH)

        def sm_wait(d, k):
            lane = lane_all[d]
            source = lax.rem(lane.i + k, lane.n)
            pltpu.make_async_remote_copy(
                src_ref=small_land.at[first_slot[d] + source],
                dst_ref=small_land.at[first_slot[d] + source],
                send_sem=sm_s.at[first_slot[d] + k],
                recv_sem=sm_r.at[first_slot[d] + source],
                device_id=lane.peer(source - lane.i), device_id_type=MESH).wait_recv()

        def sm_start(d, value):
            lane = lane_all[d]
            small_land[first_slot[d] + lane.i] = value
            for k in range(1, lane.n):
                sm_copy(d, k).start()

        def sm_finish(d):
            lane = lane_all[d]
            for k in range(1, lane.n):
                sm_wait(d, k)
            value = small_land[first_slot[d]]
            for j in range(1, lane.n):
                value = value + small_land[first_slot[d] + j]
            return value

        def sm0():
            sm_core().wait_recv()
            sm_start(0, small_ref[group] + small_core[...])

        def sm1():
            sm_start(1, sm_finish(0))

        def sm2():
            sm_start(2, sm_finish(1))

        def sm3():
            small_out[group] = sm_finish(2)
            sm_back().start()

        def sm4():
            sm_back().wait_recv()

        def back(k):
            return pltpu.make_async_remote_copy(
                src_ref=(tail_a, tail_b)[k], dst_ref=(back_a, back_b)[k], send_sem=bk_s.at[k], recv_sem=bk_r.at[k],
                device_id=partner[:2], device_id_type=MESH)

        sm_core().start()
        made = [tasks_for(p, env) for p in range(pieces)]
        for core_copy, _ in made:
            core_copy().start()
        for k in range(2):
            back(k).start()
        for _, ticks in made:
            for task in ticks[0]:
                task()
        sm0()
        table = {}
        for p, (_, ticks) in enumerate(made):
            for k, tick in enumerate(ticks[1:]):
                table.setdefault(int(delta * (p // 2)) + k, []).append((p, tick))
        for k, task in enumerate((sm1, sm2, sm3, sm4)):
            table.setdefault(2 + 2 * k, []).append((pieces, [task]))
        for when in sorted(table):
            for p, tick in sorted(table[when], key=lambda e: e[0]):
                for task in tick:
                    task()
        for task in ends:
            task()
        for k in range(2):
            back(k).wait()
        sm_core().wait_send()
        sm_back().wait_send()
        for d in range(3):
            for k in range(1, sizes[d]):
                sm_copy(d, k).wait_send()

    def call(grads, small, tail_a, tail_b, delta=1.0):
        dma = pltpu.SemaphoreType.DMA
        vmem = pl.BlockSpec(memory_space=pltpu.VMEM)
        return pl.pallas_call(
            functools.partial(kernel, delta=delta),
            out_shape=(
                jax.ShapeDtypeStruct((HALF, BLK, BLK), jnp.bfloat16),
                jax.ShapeDtypeStruct((2, SMALL, 128), jnp.float32),
                jax.ShapeDtypeStruct(tail_a.shape, tail_a.dtype),
                jax.ShapeDtypeStruct(tail_b.shape, tail_b.dtype),
            ),
            in_specs=[pl.BlockSpec(memory_space=pl.ANY), vmem, pl.BlockSpec(memory_space=pl.ANY), pl.BlockSpec(memory_space=pl.ANY)],
            out_specs=[vmem, vmem, pl.BlockSpec(memory_space=pl.ANY), pl.BlockSpec(memory_space=pl.ANY)],
            scratch_shapes=[
                pltpu.VMEM((HALF, BLK, BLK), jnp.bfloat16),
                pltpu.VMEM((HALF, BLK, BLK), jnp.bfloat16),
                pltpu.VMEM((plan.rows, BLK), jnp.bfloat16),
                pltpu.VMEM((SMALL, 128), jnp.float32),
                pltpu.VMEM((sum(sizes), SMALL, 128), jnp.float32),
                dma((plan.rs.count,)),
                dma((plan.rs.count,)),
                dma((plan.ag.count,)),
                dma((plan.agr.count,)),
                dma((pieces,)),
                dma((pieces,)),
                dma((2,)),
                dma((2,)),
                dma((sum(sizes),)),
                dma((sum(sizes),)),
                dma((2,)),
                dma((2,)),
                dma((pieces,)),
            ],
            compiler_params=pltpu.CompilerParams(
                collective_id=1, has_side_effects=True, vmem_limit_bytes=60 * 2**20
            ),
            name="reduce_gradients",
        )(grads, small, tail_a, tail_b)

    return call


STEPS_END = (
    0, 8, 16, 24, 32, 40, 48, 56, 64, 72, 80, 88, 1, 9, 17, 25, 33, 41, 49, 57, 65, 2, 73, 10, 81, 18, 89, 3,
    26, 11, 34, 19, 4, 42, 27, 12, 50, 35, 20, 58, 66, 43, 28, 51, 74, 36, 82, 59, 67, 44, 90, 75, 52, 83, 60,
    5, 68, 91, 76, 13, 84, 21, 6, 29, 92, 14, 37, 45, 22, 30, 53, 38, 61, 46, 69, 54, 77, 62, 85, 70, 93, 78,
    86, 94,
)
STEPS_INNER = (
    0, 8, 16, 24, 32, 40, 48, 56, 64, 72, 80, 88, 1, 9, 17, 25, 2, 10, 33, 41, 18, 3, 26, 49, 57, 11, 34, 19,
    42, 65, 73, 27, 50, 35, 58, 81, 89, 43, 66, 51, 74, 59, 82, 67, 90, 75, 83, 4, 91, 12, 20, 5, 13, 28, 21,
    36, 44, 6, 14, 29, 52, 22, 37, 60, 45, 68, 30, 53, 76, 61, 38, 84, 69, 46, 92, 54, 77, 85, 62, 70, 93, 78,
    86, 94,
)


def make_pairs(sizes):
    pieces = 2 * HALF
    half, quarter, eighth = BLK // 2 // 2, BLK // 2 // 4, BLK // 2
    land_rows = half + 2 * quarter + quarter

    def steps_for(piece, env):
        (lane_all, core_land, acc, out_ref, land_ref, sends, recvs, partner, grads_ref, own_sem) = env
        block = ORDER[piece // 2]
        base = (piece % 2) * (BLK // 2)
        first_lane, last_lane = (lane_all[0], lane_all[1]) if piece % 2 == 0 else (lane_all[1], lane_all[0])
        z = lane_all[2]
        side = lax.div(z.i, 2)
        onward = 1 - 2 * side
        land = piece * land_rows
        keep = base + first_lane.i * half
        give = base + (1 - first_lane.i) * half
        mine_z, other_z = keep + side * quarter, keep + (1 - side) * quarter
        c_keep, c_give = last_lane.i * eighth, (1 - last_lane.i) * eighth
        all_cols = pl.ds(0, BLK)
        other_x = 1 - 2 * first_lane.i
        other_y = 1 - 2 * last_lane.i

        def rows_of(start, count):
            return pl.ds(pl.multiple_of(start, 16), count)

        def cols_of(start):
            return pl.ds(pl.multiple_of(start, 128), eighth)

        def send(src, dst, k, to, leave=None):
            leave = k if leave is None else leave
            return pltpu.make_async_remote_copy(
                src_ref=src, dst_ref=dst, send_sem=sends.at[piece * PER + leave], recv_sem=recvs.at[piece * PER + k],
                device_id=to, device_id_type=MESH)

        def landing(row, count):
            return land_ref.at[pl.ds(land + row, count)]

        def add(start, count, row):
            def body(k, carry):
                here = rows_of(start + k * 32, 32)
                acc[block, here] += land_ref[pl.ds(pl.multiple_of(land + row + k * 32, 16), 32)]
                return carry
            lax.fori_loop(0, count // 32, body, 0)

        def out_rows(start):
            return out_ref.at[block, rows_of(start, quarter)]

        def r1():
            return send(acc.at[block, rows_of(give, half)], landing(0, half), 0, first_lane.peer(other_x))

        def near():
            return send(acc.at[block, rows_of(other_z, quarter)], landing(half, quarter), 1, z.peer(onward))

        def near_in():
            return send(acc.at[block, rows_of(other_z, quarter)], landing(half, quarter), 1, z.peer(-onward))

        def cross():
            return send(acc.at[block, rows_of(other_z, quarter)], landing(half + quarter, quarter), 2, z.peer(onward), 1)

        def back():
            return send(acc.at[block, rows_of(mine_z, quarter)], landing(half + quarter, quarter), 2, z.peer(-onward))

        def last_half(c):
            return land_ref.at[pl.ds(land + half + 2 * quarter, quarter), pl.ds(0, eighth)]

        def r3():
            return send(acc.at[block, rows_of(mine_z, quarter), cols_of(c_give)], last_half(0), 3, last_lane.peer(other_y))

        def a3(c):
            ref = out_ref.at[block, rows_of(mine_z, quarter), cols_of(c)]
            return send(ref, ref, 4, last_lane.peer(other_y))

        def a_near(to):
            return send(out_rows(mine_z), out_rows(mine_z), 5, z.peer(to))

        def a_cross():
            return send(out_rows(mine_z), out_rows(mine_z), 6, z.peer(onward), 5)

        def a_far_in():
            return send(out_rows(other_z), out_rows(other_z), 6, z.peer(onward))

        def a_back():
            return send(out_rows(other_z), out_rows(other_z), 6, z.peer(-onward))

        def a1(start, k):
            return send(out_rows(start), out_rows(start), k, first_lane.peer(other_x))

        x_mine, x_other = give + side * quarter, give + (1 - side) * quarter

        def core_copy():
            return pltpu.make_async_remote_copy(
                src_ref=grads_ref.at[1 - partner[2], block, pl.ds(base, BLK // 2)],
                dst_ref=core_land.at[block, pl.ds(base, BLK // 2)],
                send_sem=sends.at[PER * pieces + piece], recv_sem=recvs.at[PER * pieces + piece],
                device_id=partner[:2], device_id_type=MESH)

        def begin():
            own_copy(grads_ref, acc, own_sem, partner[2], piece).wait()
            core_copy().wait_recv()

            def body(k, carry):
                r = pl.ds(pl.multiple_of(base + k * 32, 16), 32)
                acc[block, r] += core_land[block, r]
                return carry
            lax.fori_loop(0, BLK // 2 // 32, body, 0)
            r1().start()

        def x_sum():
            r1().wait_recv()
            add(keep, half, 0)

        def x_done():
            a1(x_mine, 7).wait_recv()
            a1(x_other, 8).wait_recv()

        def e1():
            x_sum()
            near().start()

        def e2():
            cross().wait_recv()
            add(mine_z, quarter, half + quarter)
            r3().start()

        def e3():
            r3().wait_recv()
            r, cs = rows_of(mine_z, quarter), cols_of(c_keep)
            out_ref[block, r, cs] = acc[block, r, cs] + last_half(0)[...]
            a3(c_keep).start()

        def e4():
            a3(c_give).wait_recv()
            a_near(onward).start()
            a1(mine_z, 7).start()

        def e5():
            a_far_in().wait_recv()
            a1(other_z, 8).start()

        def i2():
            near_in().wait_recv()
            add(other_z, quarter, half)
            cross().start()

        def i3():
            cross().wait_recv()
            add(mine_z, quarter, half + quarter)
            back().start()

        def i4():
            a_near(-onward).wait_recv()
            a_cross().start()
            a1(mine_z, 7).start()

        def i5():
            a_far_in().wait_recv()
            a_back().start()
            a1(other_z, 8).start()

        ends_sent = (r1, near, r3, lambda: a3(c_keep), lambda: a_near(onward), lambda: a1(mine_z, 7), lambda: a1(other_z, 8), core_copy)
        inner_sent = (r1, cross, back, a_cross, a_back, lambda: a1(mine_z, 7), lambda: a1(other_z, 8), core_copy)
        return (core_copy, (begin, e1, e2, e3, e4, e5, x_done), (begin, x_sum, i2, i3, i4, i5, x_done), ends_sent, inner_sent)

    def kernel(grads_ref, small_ref, tail_a, tail_b, out_ref, small_out, back_a, back_b, core_land, acc, land_ref, small_core, small_land,
               sends, recvs, sm_cs, sm_cr, sm_s, sm_r, bk_s, bk_r, own_sem):
        lane_all = lanes(sizes)
        dp, group = lax.axis_index("dp"), lax.axis_index("group")
        partner = (dp, 1 - group, group)

        for p in range(pieces):
            own_copy(grads_ref, acc, own_sem, group, p).start()
        barrier = pltpu.get_barrier_semaphore()
        total = 1
        pl.semaphore_signal(barrier, inc=1, device_id=partner[:2], device_id_type=MESH)
        for lane in lane_all:
            for k in range(1, lane.n):
                to = lax.rem(lane.i + k, lane.n)
                pl.semaphore_signal(barrier, inc=1, device_id=lane.peer(to - lane.i), device_id_type=MESH)
                total += 1
        pl.semaphore_wait(barrier, total)

        env = (lane_all, core_land, acc, out_ref, land_ref, sends, recvs, partner, grads_ref, own_sem)

        def sm_core():
            return pltpu.make_async_remote_copy(
                src_ref=small_ref.at[1 - group], dst_ref=small_core, send_sem=sm_cs.at[0], recv_sem=sm_cr.at[0],
                device_id=partner[:2], device_id_type=MESH)

        def sm_back():
            return pltpu.make_async_remote_copy(
                src_ref=small_out.at[group], dst_ref=small_out.at[group], send_sem=sm_cs.at[1], recv_sem=sm_cr.at[1],
                device_id=partner[:2], device_id_type=MESH)

        first_slot = [0, sizes[0], sizes[0] + sizes[1]]

        def sm_copy(d, k):
            lane = lane_all[d]
            to = lax.rem(lane.i + k, lane.n)
            return pltpu.make_async_remote_copy(
                src_ref=small_land.at[first_slot[d] + lane.i],
                dst_ref=small_land.at[first_slot[d] + lane.i],
                send_sem=sm_s.at[first_slot[d] + k],
                recv_sem=sm_r.at[first_slot[d] + lane.i],
                device_id=lane.peer(to - lane.i), device_id_type=MESH)

        def sm_wait(d, k):
            lane = lane_all[d]
            source = lax.rem(lane.i + k, lane.n)
            pltpu.make_async_remote_copy(
                src_ref=small_land.at[first_slot[d] + source],
                dst_ref=small_land.at[first_slot[d] + source],
                send_sem=sm_s.at[first_slot[d] + k],
                recv_sem=sm_r.at[first_slot[d] + source],
                device_id=lane.peer(source - lane.i), device_id_type=MESH).wait_recv()

        def sm_start(d, value):
            lane = lane_all[d]
            small_land[first_slot[d] + lane.i] = value
            for k in range(1, lane.n):
                sm_copy(d, k).start()

        def sm_finish(d):
            lane = lane_all[d]
            for k in range(1, lane.n):
                sm_wait(d, k)
            value = small_land[first_slot[d]]
            for j in range(1, lane.n):
                value = value + small_land[first_slot[d] + j]
            return value

        def sm0():
            sm_core().wait_recv()
            sm_start(0, small_ref[group] + small_core[...])

        def sm1():
            sm_start(1, sm_finish(0))

        def sm2():
            sm_start(2, sm_finish(1))

        def sm3():
            small_out[group] = sm_finish(2)
            sm_back().start()

        def sm4():
            sm_back().wait_recv()

        def back(k):
            return pltpu.make_async_remote_copy(
                src_ref=(tail_a, tail_b)[k], dst_ref=(back_a, back_b)[k], send_sem=bk_s.at[k], recv_sem=bk_r.at[k],
                device_id=partner[:2], device_id_type=MESH)

        sm_core().start()
        made = [steps_for(p, env) for p in range(pieces)]
        for steps in made:
            steps[0]().start()
        for k in range(2):
            back(k).start()
        small_steps = (sm0, sm1, sm2, sm3, sm4)

        def run(order, kind):
            every = len(order) // len(small_steps)
            for index, code in enumerate(order):
                made[code // 8][1 + kind][code % 8]()
                if index % every == every - 1 and index // every < len(small_steps):
                    small_steps[index // every]()
            for steps in made:
                for sent in steps[3 + kind]:
                    sent().wait_send()

        z = lane_all[2].i
        at_end = (z == 0) | (z == 3)

        @pl.when(at_end)
        def _():
            run(STEPS_END, 0)

        @pl.when(jnp.logical_not(at_end))
        def _():
            run(STEPS_INNER, 1)

        for k in range(2):
            back(k).wait()
        sm_core().wait_send()
        sm_back().wait_send()
        for d in range(3):
            for k in range(1, sizes[d]):
                sm_copy(d, k).wait_send()

    def call(grads, small, tail_a, tail_b):
        dma = pltpu.SemaphoreType.DMA
        vmem = pl.BlockSpec(memory_space=pltpu.VMEM)
        return pl.pallas_call(
            kernel,
            out_shape=(
                jax.ShapeDtypeStruct((HALF, BLK, BLK), jnp.bfloat16),
                jax.ShapeDtypeStruct((2, SMALL, 128), jnp.float32),
                jax.ShapeDtypeStruct(tail_a.shape, tail_a.dtype),
                jax.ShapeDtypeStruct(tail_b.shape, tail_b.dtype),
            ),
            in_specs=[pl.BlockSpec(memory_space=pl.ANY), vmem, pl.BlockSpec(memory_space=pl.ANY), pl.BlockSpec(memory_space=pl.ANY)],
            out_specs=[vmem, vmem, pl.BlockSpec(memory_space=pl.ANY), pl.BlockSpec(memory_space=pl.ANY)],
            scratch_shapes=[
                pltpu.VMEM((HALF, BLK, BLK), jnp.bfloat16),
                pltpu.VMEM((HALF, BLK, BLK), jnp.bfloat16),
                pltpu.VMEM((pieces * land_rows, BLK), jnp.bfloat16),
                pltpu.VMEM((SMALL, 128), jnp.float32),
                pltpu.VMEM((sum(sizes), SMALL, 128), jnp.float32),
                dma(((PER + 1) * pieces,)),
                dma(((PER + 1) * pieces,)),
                dma((2,)),
                dma((2,)),
                dma((sum(sizes),)),
                dma((sum(sizes),)),
                dma((2,)),
                dma((2,)),
                dma((pieces,)),
            ],
            compiler_params=pltpu.CompilerParams(
                collective_id=1, has_side_effects=True, vmem_limit_bytes=60 * 2**20
            ),
            name="reduce_gradients",
        )(grads, small, tail_a, tail_b)

    return call


MOMENTUM = 0.9
MATRIX_RATE = 0.4
NEWTON_ONE = 3.4445
NEWTON_TWO = -4.775
NEWTON_THREE = 2.0315
STEP = 32
H = 256
VECTOR_RATE = 0.05
TABLE_RATE = 1.0


def muon_kernel(g_hbm, sw_hbm, ww_hbm, sm_hbm, wm_hbm, row_a, row_b, back_a, back_b,
                small, vec, tab, vec_m, tab_m,
                gs_out, gw_out, ns_out, nw_out, nsm_out, nwm_out, out_a, out_b, gv_out, gt_out, nv_out, nt_out, nvm_out, ntm_out,
                g, sw, ww, sm, wm, gs, gw, xs, xw, gram, mix, own, back, sem_in, sem_out, sem_row, *, slot_root):
    ff = ww.shape[2]
    cols = ff // D

    def load(src, dst, k):
        return pltpu.make_async_copy(src, dst, sem_in.at[k])

    loads = [load(g_hbm.at[pl.ds(0, 2)], g.at[pl.ds(0, 2)], 0), load(sm_hbm, sm, 1),
             load(g_hbm.at[pl.ds(2, cols)], g.at[pl.ds(2, cols)], 2), load(wm_hbm, wm, 3),
             load(sw_hbm, sw, 4), load(ww_hbm, ww, 5)]
    for c in loads:
        c.start()
    first, rows = row_a.shape[0] - back.shape[1], back.shape[1]
    fetch, put = [], []
    for k, (mine, theirs, out) in enumerate(((row_a, back_a, out_a), (row_b, back_b, out_b))):
        fetch.append(pltpu.make_async_copy(mine.at[pl.ds(first, rows)], own.at[k], sem_row.at[k]))
        fetch.append(pltpu.make_async_copy(theirs, back.at[k], sem_row.at[2 + k]))
        put.append(pltpu.make_async_copy(own.at[k], out.at[pl.ds(first, rows)], sem_row.at[4 + k]))
    for c in fetch:
        c.start()
    stores = [pltpu.make_async_copy(a, b, sem_out.at[k]) for k, (a, b) in enumerate(
        ((gs, gs_out), (sm, nsm_out), (gw, gw_out), (wm, nwm_out), (sw, ns_out), (ww, nw_out)))]

    def scan(moment, grad, pick):
        def body(k, total):
            r = pl.multiple_of(k * STEP, STEP)
            new = None
            part = jnp.zeros((STEP, D), jnp.float32)
            for c, block in enumerate(pick):
                cs = pl.ds(c * D, D)
                add = g[block, pl.ds(r, STEP)].astype(jnp.float32)
                grad[pl.ds(r, STEP), cs] = add
                new = MOMENTUM * moment[pl.ds(r, STEP), cs] + add
                moment[pl.ds(r, STEP), cs] = new
                part = part + new * new
            return total + part
        total = lax.fori_loop(0, D // STEP, body, jnp.zeros((STEP, D), jnp.float32))
        return jnp.sum(total)

    def scale(moment, x, total, width):
        size = jnp.sqrt(jnp.full((1, D), total, jnp.float32)) + 1e-07

        def body(k, carry):
            r = pl.multiple_of(k * STEP, STEP)
            for c in range(width // D):
                cs = pl.ds(c * D, D)
                x[pl.ds(r, STEP), cs] = (moment[pl.ds(r, STEP), cs] / size).astype(jnp.bfloat16)
            return carry
        lax.fori_loop(0, D // STEP, body, 0)

    dot_t = functools.partial(lax.dot_general, dimension_numbers=(((1,), (1,)), ((), ())),
                              preferred_element_type=jnp.float32)

    def newton(many):
        def body(k, carry):
            for m in range(len(many)):
                x = many[m]
                top, low = x[pl.ds(0, H)], x[pl.ds(H, H)]
                gram[m, pl.ds(0, H), :] = dot_t(top, x[...]).astype(jnp.bfloat16)
                gram[m, pl.ds(H, H), pl.ds(H, H)] = dot_t(low, low).astype(jnp.bfloat16)
                gram[m, pl.ds(H, H), pl.ds(0, H)] = gram[m, pl.ds(0, H), pl.ds(H, H)].T
            for m in range(len(many)):
                a = gram[m]

                def poly(r, c):
                    square = jnp.dot(a[r], a[:, c], preferred_element_type=jnp.float32)
                    return (NEWTON_TWO * a[r, c].astype(jnp.float32) + NEWTON_THREE * square).astype(jnp.bfloat16)
                up, down = slice(0, H), slice(H, D)
                mix[m, pl.ds(0, H), :] = poly(up, slice(0, D))
                mix[m, pl.ds(H, H), pl.ds(H, H)] = poly(down, down)
                mix[m, pl.ds(H, H), pl.ds(0, H)] = mix[m, pl.ds(0, H), pl.ds(H, H)].T
            for m in range(len(many)):
                x, width = many[m], many[m].shape[1]
                for c in range(width // D):
                    cs = pl.ds(c * D, D)
                    old = x[:, cs]
                    x[:, cs] = (NEWTON_ONE * old.astype(jnp.float32)
                                + jnp.dot(mix[m], old, preferred_element_type=jnp.float32)).astype(jnp.bfloat16)
            return carry
        lax.fori_loop(0, 5, body, 0)

    def finish(weight, x, width):
        def body(k, carry):
            r = pl.multiple_of(k * STEP, STEP)
            for c in range(width // D):
                cs = pl.ds(c * D, D)
                weight[pl.ds(r, STEP), cs] = weight[pl.ds(r, STEP), cs] - MATRIX_RATE * x[pl.ds(r, STEP), cs].astype(jnp.float32)
            return carry
        lax.fori_loop(0, D // STEP, body, 0)

    loads[0].wait()
    loads[1].wait()
    for m in range(2):
        total = scan(sm.at[m], gs.at[m], (m,))
        scale(sm.at[m], xs.at[m], total, D)
    stores[0].start()
    stores[1].start()
    loads[2].wait()
    loads[3].wait()
    total = scan(wm.at[0], gw.at[0], tuple(range(2, 2 + cols)))
    scale(wm.at[0], xw, total, ff)
    stores[2].start()
    stores[3].start()
    for c in fetch:
        c.wait()
    for k in range(2):
        def join(i, carry):
            r = pl.ds(pl.multiple_of(i * 16, 16), 16)
            own[k, r] = own[k, r] + back[k, r]
            return carry
        lax.fori_loop(0, rows // 16, join, 0)
        put[k].start()
    half = small.shape[1]

    def small_row(k):
        return small[k // half, pl.ds(k % half, 1)]

    lines = D // 128
    for r in range(vec.shape[0]):
        for c in range(lines):
            gv_out[pl.ds(r, 1), pl.ds(128 * c, 128)] = small_row(r * lines + c)
    nvm_out[...] = MOMENTUM * vec_m[...] + gv_out[...]
    nv_out[...] = vec[...] - (VECTOR_RATE / slot_root) * nvm_out[...]
    first = vec.shape[0] * lines
    heads, entries = tab.shape
    gt_out[:, pl.ds(0, 128)] = jnp.concatenate([small_row(first + 2 * h) for h in range(heads)], axis=0)
    gt_out[:, pl.ds(128, entries - 128)] = jnp.concatenate(
        [small_row(first + 2 * h + 1)[:, : entries - 128] for h in range(heads)], axis=0)
    ntm_out[...] = MOMENTUM * tab_m[...] + gt_out[...]
    nt_out[...] = tab[...] - (TABLE_RATE / slot_root) * ntm_out[...]
    newton([xw, xs.at[0], xs.at[1]])
    loads[4].wait()
    for m in range(2):
        finish(sw.at[m], xs.at[m], D)
    stores[4].start()
    loads[5].wait()
    finish(ww.at[0], xw, ff)
    stores[5].start()
    for c in stores + put:
        c.wait()


def muon(g, sw, ww, sm, wm, row_a, row_b, back_a, back_b, small, vec, tab, vec_m, tab_m, slots):
    any_, vmem = pl.BlockSpec(memory_space=pl.ANY), pl.BlockSpec(memory_space=pltpu.VMEM)
    slot_root = float(np.sqrt(np.float32(slots)))
    shapes = [sw, ww, sw, ww, sm, wm]
    f32 = jnp.float32
    return pl.pallas_call(
        functools.partial(muon_kernel, slot_root=slot_root),
        out_shape=tuple(jax.ShapeDtypeStruct(a.shape, f32) for a in shapes)
        + tuple(jax.ShapeDtypeStruct(a.shape, a.dtype) for a in (row_a, row_b))
        + tuple(jax.ShapeDtypeStruct(a.shape, f32) for a in (vec, tab, vec, tab, vec, tab)),
        in_specs=[any_] * 9 + [vmem] * 5,
        out_specs=(any_,) * 8 + (vmem,) * 6,
        input_output_aliases={5: 6, 6: 7},
        scratch_shapes=[
            pltpu.VMEM(g.shape, jnp.bfloat16),
            pltpu.VMEM(sw.shape, f32), pltpu.VMEM(ww.shape, f32),
            pltpu.VMEM(sm.shape, f32), pltpu.VMEM(wm.shape, f32),
            pltpu.VMEM(sw.shape, f32), pltpu.VMEM(ww.shape, f32),
            pltpu.VMEM((2, D, D), jnp.bfloat16), pltpu.VMEM((D, ww.shape[2]), jnp.bfloat16),
            pltpu.VMEM((3, D, D), jnp.bfloat16), pltpu.VMEM((3, D, D), jnp.bfloat16),
            pltpu.VMEM((2,) + back_a.shape, jnp.bfloat16), pltpu.VMEM((2,) + back_a.shape, jnp.bfloat16),
            pltpu.SemaphoreType.DMA((6,)), pltpu.SemaphoreType.DMA((6,)), pltpu.SemaphoreType.DMA((6,)),
        ],
        compiler_params=pltpu.CompilerParams(vmem_limit_bytes=58 * 2**20),
        name="muon_step",
    )(g, sw, ww, sm, wm, row_a, row_b, back_a, back_b, small, vec, tab, vec_m, tab_m)


def shards(
    tokens,
    cotangent,
    counts,
    regions,
    square_weights,
    wide_weights,
    vectors,
    bias_table,
    square_moment,
    wide_moment,
    vector_moment,
    table_moment,
):
    table = bias_table.T
    square_low, wide_low, tok_tail, cot_tail, count_other, regions_other, bias = exchange(
        square_weights, wide_weights, tokens, cotangent, counts, regions, table
    )
    out, out_tail, gtok, gtok_tail, grads, small = block(
        counts, regions, count_other, regions_other, tokens, cotangent, tok_tail, cot_tail, square_low, wide_low, vectors, bias
    )
    dp_size, group_size = lax.axis_size("dp"), lax.axis_size("group")
    summed, small_sum, out_back, gtok_back = make_comm(chip_grid(dp_size))(grads, small, out_tail, gtok_tail)
    (
        owned_square,
        owned_wide,
        new_square,
        new_wide,
        new_square_moment,
        new_wide_moment,
        block_out,
        grad_tokens,
        summed_vectors,
        summed_table,
        new_vectors,
        new_table,
        new_vector_moment,
        new_table_moment,
    ) = muon(
        summed,
        square_weights,
        wide_weights,
        square_moment,
        wide_moment,
        out,
        gtok,
        out_back,
        gtok_back,
        small_sum,
        vectors,
        table,
        vector_moment,
        table_moment.T,
        WIN_DEV * dp_size * group_size,
    )
    return (
        block_out,
        grad_tokens,
        owned_square,
        owned_wide,
        summed_vectors,
        summed_table.T,
        new_square,
        new_wide,
        new_vectors,
        new_table.T,
        new_square_moment,
        new_wide_moment,
        new_vector_moment,
        new_table_moment.T,
    )


def solution(mesh):
    in_specs = (
        P(("dp", "group"), None),
        P(("dp", "group"), None),
        P(("dp", "group")),
        P(("dp", "group")),
        P("group", None, None),
        P("group", None, None),
        P(),
        P(),
        P("group", None, None),
        P("group", None, None),
        P(),
        P(),
    )
    out_specs = (
        P(("dp", "group"), None),
        P(("dp", "group"), None),
        P("group", None, None),
        P("group", None, None),
        P(),
        P(),
        P("group", None, None),
        P("group", None, None),
        P(),
        P(),
        P("group", None, None),
        P("group", None, None),
        P(),
        P(),
    )
    return jax.shard_map(shards, mesh=mesh, in_specs=in_specs, out_specs=out_specs, check_vma=False)
```
